128 devices in a mesh: aux: 8 (over z, core), orb: 16 (over x, y).
Axes of the slice: x: 4, y: 4, z: 4, core: 2. Of those that a mesh axis runs over, the one named last changes fastest.
Arguments:
- half: bfloat16 [128, 384, 3072], P('aux', 'orb'), may hold values from -1 to 1
- metric: bfloat16 [128, 128], P('aux'), may hold values from -1 to 2
- survive: int32 [8, 16, 24], P('aux', 'orb'), may hold values 0 or 1
Outputs:
- exchange_k: float32 [3072, 3072], P('orb', 'aux')
The draws below stay inside these ranges and needn't reach their ends.
All inputs are finite; a program needn't handle non-finite values. No bound on the sum of `survive` on one device may be relied on, other than what follows from the above.
Results may differ from the reference program's by a relative error of at most 0.00098.
Values may be sent and summed in bfloat16 or wider, within the bound.
No kernel may reach another device: no remote copies, remote signals or barrier semaphores. Data moves between devices by JAX's collectives and lax.ppermute only.
A program may use at most 128 MiB of HBM per device.

```python
import jax
import jax.numpy as jnp
from jax import lax

NOCC = 384
OCCB = 24
NAO = 3072
AOBLK = 128
NAUX = 128
N_AUX = 8


def draw_metric(key, part):
    first_key = jax.random.fold_in(key, 11)
    second_key = jax.random.fold_in(key, 12)
    spread = jax.random.normal(first_key, (NAUX, NAUX), jnp.float32) * (0.6 / NAUX ** 0.5)
    diagonal_part = jax.random.uniform(second_key, (NAUX,), jnp.float32, 0.9, 1.1)
    return (spread + jnp.diag(diagonal_part)).astype(jnp.bfloat16)


def set_ends(entries, own_key, low, largest):
    shape = entries.shape
    place = [jax.random.randint(jax.random.fold_in(own_key, axis), (), 0, shape[axis]) for axis in range(len(shape))]
    entries = entries.at[tuple(place)].set(low)
    longest = shape.index(max(shape))
    place[longest] = (place[longest] + 1) % shape[longest]
    return entries.at[tuple(place)].set(largest)


def steps_of(key, shape, cuts, low, largest):
    def one(axis_at, shards_of):
        draws = jax.random.uniform(jax.random.fold_in(jax.random.fold_in(key, 6), axis_at), (shards_of,), jnp.float32, low / len(cuts), largest / len(cuts))
        return jnp.repeat(jnp.exp(draws), shape[axis_at] // shards_of).reshape((-1,) + (1,) * (len(shape) - axis_at - 1))

    level = one(*cuts[0])
    for cut in cuts[1:]:
        level = level * one(*cut)
    return level


def bell_draw(key, shape, scale, most, shards=(), kind=jnp.bfloat16):
    factor_of = steps_of(key, shape, shards, -0.22, 0.18) if shards else 1.0
    values = jax.random.normal(key, shape, jnp.float32) * scale * factor_of
    return jnp.minimum(jnp.maximum(values, -most), most).astype(kind)


def setup_inputs(seed: int = 0) -> dict:
    key_of = jax.random.split(jax.random.key(seed), 4)
    half = bell_draw(key_of[0], (NAUX, NOCC, NAO), ((NAUX * NOCC) ** -0.25), 1.0, ((0, 8), (1, 16)))
    metric = draw_metric(jax.random.fold_in(key_of[3], 71), 0)
    survive = set_ends((jax.random.randint(key_of[2], (N_AUX, NOCC // OCCB, NAO // AOBLK), 0, 3) < 2).astype(jnp.int32), jax.random.fold_in(key_of[2], 1), 0, 1)
    return dict(half=half, metric=metric, survive=survive)


def reference(half, metric, survive):
    blocks_aux, blocks_occ, blocks_ao = survive.shape
    aux_count, occ_count, ao_count = half.shape
    gate = survive.astype(jnp.bfloat16)
    shaped = half.reshape(blocks_aux, aux_count // blocks_aux, blocks_occ, occ_count // blocks_occ, blocks_ao, ao_count // blocks_ao)
    masked = (shaped * gate[:, None, :, None, :, None]).reshape(aux_count, occ_count, ao_count)
    occ_width = occ_count // blocks_occ

    def accumulate(totals, block_index):
        occ_rows = lax.dynamic_slice_in_dim(masked, block_index * occ_width, occ_width, 1)
        fitted = jnp.dot(metric, occ_rows.reshape(aux_count, -1), preferred_element_type=jnp.float32)
        fitted = fitted.astype(jnp.bfloat16).reshape(-1, ao_count)
        update = lax.dot_general(fitted, fitted, (((0,), (0,)), ((), ())), preferred_element_type=jnp.float32)
        return totals + update, None

    exchange_k, _ = lax.scan(accumulate, jnp.zeros((ao_count, ao_count), jnp.float32), jnp.arange(blocks_occ, dtype=jnp.int32))
    return exchange_k
```

```python
import functools

import jax
import jax.numpy as jnp
from jax import lax
from jax.experimental import pallas as pl
from jax.experimental.pallas import tpu as pltpu
from jax.sharding import Mesh
from jax.sharding import PartitionSpec as P


AXES = ("z", "c", "x", "y")
BF = jnp.bfloat16
F32 = jnp.float32
I16 = jnp.int16
MIB = 1 << 20
RING = 4
TAIL = 16


def whole():
    return pl.BlockSpec(memory_space=pltpu.VMEM)


def scalars():
    return pl.BlockSpec(memory_space=pltpu.SMEM)


def params(mib):
    return pltpu.CompilerParams(vmem_limit_bytes=mib * MIB)


def cost(flops, moved):
    return pl.CostEstimate(flops=flops, bytes_accessed=moved, transcendentals=0)


def place(z, c, x, y):
    return ((z % 4) * 2 + c) * 16 + (x % 4) * 4 + y % 4


def moves(shift):
    every = [(z, c, x, y) for z in range(4) for c in range(2) for x in range(4) for y in range(4)]
    return [(place(*d), place(*shift(*d))) for d in every]


def send(v, shift):
    return lax.ppermute(v, AXES, moves(shift))


def along_z(k):
    return lambda z, c, x, y: (z + k, c, x, y)


def other_core(z, c, x, y):
    return (z, 1 - c, x, y)


def first_axis(k):
    return lambda z, c, x, y: (z, c, x + k, y) if c == 0 else (z, c, x, y + k)


def second_axis(k):
    return lambda z, c, x, y: (z, c, x, y + k) if c == 0 else (z, c, x + k, y)


def screen_body(at, half, gate, metric, *outs_and_scratch):
    outs, turned = outs_and_scratch[:4], outs_and_scratch[4]
    lanes = 512

    def step(n, carry):
        cut = pl.ds(pl.multiple_of(n * lanes, lanes), lanes)
        kept = half[:, :, cut] * gate[:, cut][None]
        turned[:, :, cut] = jnp.swapaxes(kept.astype(F32), 0, 1).astype(BF)
        return carry

    ao = half.shape[2]
    lax.fori_loop(0, ao // lanes, step, 0)
    group = outs[0].shape[0]
    for k in range(RING):
        first = lax.rem(at[0] + k, RING) * group
        outs[k][:, :, :ao] = turned[pl.ds(first, group)]
        outs[k][:, :, ao:] = jnp.broadcast_to(metric[...][None], (group,) + metric.shape)


def screen(at, half, gate, metric):
    aux, occ, ao = half.shape
    out = jax.ShapeDtypeStruct((occ // RING, aux, ao + metric.shape[1]), BF)
    return pl.pallas_call(
        screen_body,
        out_shape=[out] * RING,
        in_specs=[scalars(), whole(), whole(), whole()],
        out_specs=[whole()] * RING,
        scratch_shapes=[pltpu.VMEM((occ, aux, ao), BF)],
        compiler_params=params(16),
        cost_estimate=cost(half.size, half.size * 4),
    )(at, half, gate, metric)


def fit_body(at, *refs):
    pieces, (rows, turned, mixed) = refs[:8], refs[8:]
    step = pl.program_id(0)
    ao = rows.shape[1]
    aux = mixed.shape[0]
    part = aux // 8

    @pl.when(step == 0)
    def _():
        metric = jnp.concatenate([p[0][:, ao:] for p in pieces], axis=0)
        source = lax.broadcasted_iota(jnp.int32, (aux, aux), 0)
        n = lax.broadcasted_iota(jnp.int32, (aux, aux), 1)
        slot = n // part
        up = lax.rem(at[0] - slot // 2 + RING, RING)
        core = jnp.where(slot % 2 == 0, at[1], 1 - at[1])
        wanted = (up * 2 + core) * part + n % part
        pick = jnp.where(source == wanted, 1.0, 0.0).astype(BF)
        mixed[...] = jnp.dot(metric, pick, preferred_element_type=F32).astype(BF)

    screened = jnp.concatenate([p[0][:, :ao] for p in pieces], axis=0)
    fitted = jnp.dot(mixed[...], screened, preferred_element_type=F32).astype(BF)
    rows[...] = fitted
    turned[:, pl.ds(pl.multiple_of(step * aux, aux), aux)] = fitted.T


def fit(at, pieces):
    group, part, wide = pieces[0].shape
    aux = part * 8
    ao = wide - aux
    piece = pl.BlockSpec((1, part, wide), lambda i: (i, 0, 0))
    return pl.pallas_call(
        fit_body,
        grid=(group,),
        out_shape=[jax.ShapeDtypeStruct((group * aux, ao), BF), jax.ShapeDtypeStruct((ao, group * aux), BF)],
        in_specs=[scalars()] + [piece] * 8,
        out_specs=[pl.BlockSpec((aux, ao), lambda i: (i, 0)), pl.BlockSpec((ao, group * aux), lambda i: (0, 0))],
        scratch_shapes=[pltpu.VMEM((aux, aux), BF)],
        compiler_params=params(28),
        cost_estimate=cost(2 * group * aux * aux * ao, group * aux * ao * 6),
    )(at, *pieces)


def exponent(top):
    return jnp.floor(14.9 - jnp.log2(jnp.maximum(top, 1e-30)))


def coded(v, e):
    return jnp.round(v * jnp.exp2(e)).astype(jnp.int32).astype(I16)


def marked(e):
    return jnp.broadcast_to(e, (TAIL, e.shape[1])).astype(jnp.int32).astype(I16)


def scale_of(tail):
    return jnp.exp2(-tail.astype(jnp.int32).astype(F32)[:1])


def plain(q):
    return q.astype(jnp.int32).astype(F32)


def partial_body(shift, code, at, rows, turned, out, *scratch):
    j = pl.program_id(0)
    high = out.shape[0] // RING if not code else (out.shape[0] - TAIL) // RING
    wide = out.shape[1]
    core = at[1]
    own = jnp.where(core == 0, at[2], at[3])
    g = lax.rem(own + shift, RING)
    target = scratch[0] if code else out
    top = jnp.zeros((1, wide), F32)
    for h in range(RING):
        x = jnp.where(core == 0, g, h)
        y = jnp.where(core == 0, h, g)
        first = pl.multiple_of((x * RING + y) * high, 64)
        column = pl.multiple_of(j * 2 * wide + core * wide, 128)
        block = jnp.dot(
            turned[pl.ds(first, high), :], rows[:, pl.ds(column, wide)], preferred_element_type=F32
        )
        target[h * high:(h + 1) * high, :] = block
        if code:
            top = jnp.maximum(top, jnp.max(jnp.abs(block), axis=0, keepdims=True))
    if code:
        e = exponent(top)
        total = RING * high
        out[:total, :] = coded(target[...], e)
        out[total:, :] = marked(e)


def partial_k(at, rows, turned, shift, wide):
    depth, ao = rows.shape
    high = ao // RING
    code = shift != 0
    columns = ao // 2
    shape = (high + TAIL, columns) if code else (high, columns)
    return pl.pallas_call(
        functools.partial(partial_body, shift, code),
        grid=(columns // wide,),
        out_shape=jax.ShapeDtypeStruct(shape, I16 if code else F32),
        in_specs=[scalars(), whole(), whole()],
        out_specs=pl.BlockSpec((shape[0], wide), lambda j: (0, j)),
        scratch_shapes=[pltpu.VMEM((high, wide), F32)] if code else [],
        compiler_params=params(32),
        cost_estimate=cost(2 * depth * high * columns, high * columns * (2 if code else 4)),
    )(at, rows, turned)


def sum_rows_body(at, own, a, b, d, kept, *outs):
    high = kept.shape[0]
    total = own.shape[0]
    h = jnp.where(at[1] == 0, at[3], at[2])
    scales = [scale_of(m[total:, :]) for m in (a, b, d)]
    for k in range(RING):
        cut = pl.ds(pl.multiple_of(lax.rem(h + k, RING) * high, 64), high)
        v = own[cut, :]
        for m, s in zip((a, b, d), scales):
            v = v + plain(m[cut, :]) * s
        if k == 0:
            kept[...] = v
        else:
            e = exponent(jnp.max(jnp.abs(v), axis=0, keepdims=True))
            outs[k - 1][:high, :] = coded(v, e)
            outs[k - 1][high:, :] = marked(e)


def sum_rows(at, own, arrived, wide):
    total, columns = own.shape
    high = total // RING

    def spec(rows):
        return pl.BlockSpec((rows, wide), lambda j: (0, j))

    return pl.pallas_call(
        sum_rows_body,
        grid=(columns // wide,),
        out_shape=[jax.ShapeDtypeStruct((high, columns), F32)]
        + [jax.ShapeDtypeStruct((high + TAIL, columns), I16)] * 3,
        in_specs=[scalars(), spec(total)] + [spec(total + TAIL)] * 3,
        out_specs=[spec(high)] + [spec(high + TAIL)] * 3,
        compiler_params=params(28),
        cost_estimate=cost(total * columns * 16, total * columns * 10),
    )(at, own, *arrived)


def sum_columns_body(at, own, a, b, d, kept, *outs):
    high, wide = kept.shape
    for k in range(RING):
        cut = pl.ds(pl.multiple_of(lax.rem(at[0] + k, RING) * wide, 128), wide)
        v = own[:, cut]
        for m in (a, b, d):
            v = v + plain(m[:high, cut]) * scale_of(m[high:, cut])
        if k == 0:
            kept[...] = v
        else:
            e = exponent(jnp.max(jnp.abs(v), axis=0, keepdims=True))
            outs[k - 1][:high, :] = coded(v, e)
            outs[k - 1][high:, :] = marked(e)


def sum_columns(at, own, arrived, wide):
    high = own.shape[0]
    return pl.pallas_call(
        sum_columns_body,
        out_shape=[jax.ShapeDtypeStruct((high, wide), F32)]
        + [jax.ShapeDtypeStruct((high + TAIL, wide), I16)] * 3,
        in_specs=[scalars()] + [whole()] * 4,
        out_specs=[whole()] * 4,
        compiler_params=params(16),
        cost_estimate=cost(own.size * 16, own.size * 10),
    )(at, own, *arrived)


def finish_body(own, a, b, d, out):
    high = out.shape[0]
    v = own[...]
    for m in (a, b, d):
        v = v + plain(m[:high, :]) * scale_of(m[high:, :])
    out[...] = v


def finish(own, arrived):
    return pl.pallas_call(
        finish_body,
        out_shape=jax.ShapeDtypeStruct(own.shape, F32),
        in_specs=[whole()] * 4,
        out_specs=whole(),
        compiler_params=params(8),
        cost_estimate=cost(own.size * 8, own.size * 14),
    )(own, *arrived)


def shards(half, metric, survive):
    aux, occ, ao = half.shape
    at = jnp.stack([lax.axis_index(a) for a in AXES]).astype(jnp.int32)
    blocks = survive.shape[2]
    gate = jnp.repeat(survive.reshape(1, blocks).astype(BF), ao // blocks, axis=1)
    wide = ao // 8

    parts = screen(at, half, gate, metric)
    here = [parts[0]] + [None] * 3
    for k in (2, 1, 3):
        here[k] = send(parts[k], along_z(k))
    there = [send(v, other_core) for v in here]
    rows, turned = fit(at, [v for pair in zip(here, there) for v in pair])

    arrived = []
    for k in (2, 1, 3):
        arrived.append(send(partial_k(at, rows, turned, k, wide), first_axis(k)))
    own = partial_k(at, rows, turned, 0, wide)
    own, *out = sum_rows(at, own, arrived, wide)
    arrived = [send(out[k - 1], second_axis(k)) for k in (2, 1, 3)]
    own, *out = sum_columns(at, own, arrived, wide)
    arrived = [send(out[k - 1], along_z(k)) for k in (2, 1, 3)]
    return finish(own, arrived)


def solution(mesh):
    finer = Mesh(mesh.devices.reshape(4, 2, 4, 4), AXES)
    placed = (P(("z", "c"), ("x", "y"), None), P(("z", "c"), None), P(("z", "c"), ("x", "y"), None))
    return jax.shard_map(
        shards, mesh=finer, in_specs=placed, out_specs=P(("x", "y"), ("z", "c")), check_vma=False
    )
```

```python
import functools

import jax
import jax.numpy as jnp
from jax import lax
from jax.experimental import pallas as pl
from jax.experimental.pallas import tpu as pltpu
from jax.sharding import Mesh
from jax.sharding import PartitionSpec as P


AXES = ("z", "c", "x", "y")
BF = jnp.bfloat16
F32 = jnp.float32
I16 = jnp.int16
MIB = 1 << 20
RING = 4
TAIL = 16


def whole():
    return pl.BlockSpec(memory_space=pltpu.VMEM)


def scalars():
    return pl.BlockSpec(memory_space=pltpu.SMEM)


def params(mib):
    return pltpu.CompilerParams(vmem_limit_bytes=mib * MIB)


def cost(flops, moved):
    return pl.CostEstimate(flops=flops, bytes_accessed=moved, transcendentals=0)


def place(z, c, x, y):
    return ((z % 4) * 2 + c) * 16 + (x % 4) * 4 + y % 4


def moves(shift):
    every = [(z, c, x, y) for z in range(4) for c in range(2) for x in range(4) for y in range(4)]
    return [(place(*d), place(*shift(*d))) for d in every]


def send(v, shift):
    return lax.ppermute(v, AXES, moves(shift))


def along_z(k):
    return lambda z, c, x, y: (z + k, c, x, y)


def other_core(z, c, x, y):
    return (z, 1 - c, x, y)


def first_axis(k):
    return lambda z, c, x, y: (z, c, x + k, y) if c == 0 else (z, c, x, y + k)


def second_axis(k):
    return lambda z, c, x, y: (z, c, x, y + k) if c == 0 else (z, c, x + k, y)


def screen_body(at, half, gate, metric, *outs_and_scratch):
    outs, turned = outs_and_scratch[:4], outs_and_scratch[4]
    lanes = 512

    def step(n, carry):
        cut = pl.ds(pl.multiple_of(n * lanes, lanes), lanes)
        kept = half[:, :, cut] * gate[:, cut][None]
        turned[:, :, cut] = jnp.swapaxes(kept.astype(F32), 0, 1).astype(BF)
        return carry

    ao = half.shape[2]
    lax.fori_loop(0, ao // lanes, step, 0)
    group = outs[0].shape[0]
    for k in range(RING):
        first = lax.rem(at[0] + k, RING) * group
        outs[k][:, :, :ao] = turned[pl.ds(first, group)]
        outs[k][:, :, ao:] = jnp.broadcast_to(metric[...][None], (group,) + metric.shape)


def screen(at, half, gate, metric):
    aux, occ, ao = half.shape
    out = jax.ShapeDtypeStruct((occ // RING, aux, ao + metric.shape[1]), BF)
    return pl.pallas_call(
        screen_body,
        out_shape=[out] * RING,
        in_specs=[scalars(), whole(), whole(), whole()],
        out_specs=[whole()] * RING,
        scratch_shapes=[pltpu.VMEM((occ, aux, ao), BF)],
        compiler_params=params(16),
        cost_estimate=cost(half.size, half.size * 4),
    )(at, half, gate, metric)


def fit_body(at, *refs):
    pieces, (rows, turned, mixed) = refs[:8], refs[8:]
    step = pl.program_id(0)
    ao = rows.shape[1]
    aux = mixed.shape[0]
    part = aux // 8

    @pl.when(step == 0)
    def _():
        metric = jnp.concatenate([p[0][:, ao:] for p in pieces], axis=0)
        source = lax.broadcasted_iota(jnp.int32, (aux, aux), 0)
        n = lax.broadcasted_iota(jnp.int32, (aux, aux), 1)
        slot = n // part
        up = lax.rem(at[0] - slot // 2 + RING, RING)
        core = jnp.where(slot % 2 == 0, at[1], 1 - at[1])
        wanted = (up * 2 + core) * part + n % part
        pick = jnp.where(source == wanted, 1.0, 0.0).astype(BF)
        mixed[...] = jnp.dot(metric, pick, preferred_element_type=F32).astype(BF)

    screened = jnp.concatenate([p[0][:, :ao] for p in pieces], axis=0)
    fitted = jnp.dot(mixed[...], screened, preferred_element_type=F32).astype(BF)
    rows[...] = fitted
    flipped = fitted.T
    cut = pl.ds(pl.multiple_of(step * aux, aux), aux)
    high = ao // (RING * RING)
    for x in range(RING):
        for y in range(RING):
            n = x * RING + y
            to = jnp.where(at[1] == 0, n, y * RING + x) * high
            turned[pl.ds(pl.multiple_of(to, 64), high), cut] = flipped[n * high:(n + 1) * high]


def fit(at, pieces):
    group, part, wide = pieces[0].shape
    aux = part * 8
    ao = wide - aux
    piece = pl.BlockSpec((1, part, wide), lambda i: (i, 0, 0))
    return pl.pallas_call(
        fit_body,
        grid=(group,),
        out_shape=[jax.ShapeDtypeStruct((group * aux, ao), BF), jax.ShapeDtypeStruct((ao, group * aux), BF)],
        in_specs=[scalars()] + [piece] * 8,
        out_specs=[pl.BlockSpec((aux, ao), lambda i: (i, 0)), pl.BlockSpec((ao, group * aux), lambda i: (0, 0))],
        scratch_shapes=[pltpu.VMEM((aux, aux), BF)],
        compiler_params=params(28),
        cost_estimate=cost(2 * group * aux * aux * ao, group * aux * ao * 6),
    )(at, *pieces)


def exponent(top):
    return jnp.floor(14.9 - jnp.log2(jnp.maximum(top, 1e-30)))


def coded(v, e):
    return jnp.round(v * jnp.exp2(e)).astype(jnp.int32).astype(I16)


def marked(e):
    return jnp.broadcast_to(e, (TAIL, e.shape[1])).astype(jnp.int32).astype(I16)


def scale_of(tail):
    return jnp.exp2(-tail.astype(jnp.int32).astype(F32)[:1])


def plain(q):
    return q.astype(jnp.int32).astype(F32)


def write(out, first, block):
    if out.dtype == F32:
        out[first:first + block.shape[0], :] = block
    else:
        e = exponent(jnp.max(jnp.abs(block), axis=0, keepdims=True))
        end = first + block.shape[0]
        out[first:end, :] = coded(block, e)
        out[end:end + TAIL, :] = marked(e)


def bulk_body(shift, at, rows, turned, out):
    core = at[1]
    total = rows.shape[1] // RING
    g = lax.rem(jnp.where(core == 0, at[2], at[3]) + shift, RING)
    column = pl.program_id(0) * total + core * (total // 2)
    block = jnp.dot(
        turned[pl.ds(pl.multiple_of(g * total, 256), total), :],
        rows[:, pl.ds(pl.multiple_of(column, 128), out.shape[1])],
        preferred_element_type=F32,
    )
    write(out, 0, block)


def bulk_k(at, rows, turned, shift, wide):
    depth, ao = rows.shape
    total = ao // RING
    shape = (total + (TAIL if shift else 0), RING * wide)
    return pl.pallas_call(
        functools.partial(bulk_body, shift),
        grid=(RING,),
        out_shape=jax.ShapeDtypeStruct(shape, I16 if shift else F32),
        in_specs=[scalars(), whole(), whole()],
        out_specs=pl.BlockSpec((shape[0], wide), lambda j: (0, j)),
        compiler_params=params(28),
        cost_estimate=cost(2 * depth * total * RING * wide, total * RING * wide * 2),
    )(at, rows, turned)


def rest_body(shift, skip, at, rows, turned, out):
    core = at[1]
    total = rows.shape[1] // RING
    column = lax.rem(at[0] + shift, RING) * total + core * (total // 2) + skip
    block = jnp.dot(turned[...], rows[:, pl.ds(pl.multiple_of(column, 128), out.shape[1])], preferred_element_type=F32)
    write(out, 0, block)


def rest_k(at, rows, turned, shift, skip, wide):
    depth, ao = rows.shape
    total = ao // RING
    each = total + (TAIL if shift else 0)
    return pl.pallas_call(
        functools.partial(rest_body, shift, skip),
        grid=(RING,),
        out_shape=jax.ShapeDtypeStruct((RING * each, wide), I16 if shift else F32),
        in_specs=[scalars(), whole(), pl.BlockSpec((total, depth), lambda g: (g, 0))],
        out_specs=pl.BlockSpec((each, wide), lambda g: (g, 0)),
        compiler_params=params(28),
        cost_estimate=cost(2 * depth * ao * wide, ao * wide * 2),
    )(at, rows, turned)


def sum_groups_body(at, own, a, b, d, kept, *outs):
    total = kept.shape[0]
    each = total + TAIL
    g = jnp.where(at[1] == 0, at[2], at[3])
    for k in range(RING):
        n = lax.rem(g + k, RING)
        v = own[pl.ds(pl.multiple_of(n * total, 256), total), :]
        for m in (a, b, d):
            v = v + plain(m[pl.ds(pl.multiple_of(n * each, 16), total), :]) * scale_of(
                m[pl.ds(pl.multiple_of(n * each + total, 16), TAIL), :]
            )
        write(kept if k == 0 else outs[k - 1], 0, v)


def sum_groups(at, own, arrived):
    total, wide = own.shape[0] // RING, own.shape[1]
    return pl.pallas_call(
        sum_groups_body,
        out_shape=[jax.ShapeDtypeStruct((total, wide), F32)]
        + [jax.ShapeDtypeStruct((total + TAIL, wide), I16)] * 3,
        in_specs=[scalars()] + [whole()] * 4,
        out_specs=[whole()] * 4,
        compiler_params=params(16),
        cost_estimate=cost(own.size * 16, own.size * 10),
    )(at, own, *arrived)


def sum_rows_body(at, own, a, b, d, kept, *outs):
    high = kept.shape[0]
    total = own.shape[0]
    h = jnp.where(at[1] == 0, at[3], at[2])
    scales = [scale_of(m[total:, :]) for m in (a, b, d)]
    for k in range(RING):
        cut = pl.ds(pl.multiple_of(lax.rem(h + k, RING) * high, 64), high)
        v = own[cut, :]
        for m, s in zip((a, b, d), scales):
            v = v + plain(m[cut, :]) * s
        if k == 0:
            kept[...] = v
        else:
            e = exponent(jnp.max(jnp.abs(v), axis=0, keepdims=True))
            outs[k - 1][:high, :] = coded(v, e)
            outs[k - 1][high:, :] = marked(e)


def sum_rows(at, own, arrived, wide):
    total, columns = own.shape
    high = total // RING

    def spec(rows):
        return pl.BlockSpec((rows, wide), lambda j: (0, j))

    return pl.pallas_call(
        sum_rows_body,
        grid=(columns // wide,),
        out_shape=[jax.ShapeDtypeStruct((high, columns), F32)]
        + [jax.ShapeDtypeStruct((high + TAIL, columns), I16)] * 3,
        in_specs=[scalars(), spec(total)] + [spec(total + TAIL)] * 3,
        out_specs=[spec(high)] + [spec(high + TAIL)] * 3,
        compiler_params=params(28),
        cost_estimate=cost(total * columns * 16, total * columns * 10),
    )(at, own, *arrived)


def sum_columns_body(at, own, a, b, d, kept, *outs):
    high, wide = kept.shape
    for k in range(RING):
        cut = pl.ds(pl.multiple_of(lax.rem(at[0] + k, RING) * wide, 128), wide)
        v = own[:, cut]
        for m in (a, b, d):
            v = v + plain(m[:high, cut]) * scale_of(m[high:, cut])
        if k == 0:
            kept[...] = v
        else:
            e = exponent(jnp.max(jnp.abs(v), axis=0, keepdims=True))
            outs[k - 1][:high, :] = coded(v, e)
            outs[k - 1][high:, :] = marked(e)


def sum_columns(at, own, arrived, wide):
    high = own.shape[0]
    return pl.pallas_call(
        sum_columns_body,
        out_shape=[jax.ShapeDtypeStruct((high, wide), F32)]
        + [jax.ShapeDtypeStruct((high + TAIL, wide), I16)] * 3,
        in_specs=[scalars()] + [whole()] * 4,
        out_specs=[whole()] * 4,
        compiler_params=params(16),
        cost_estimate=cost(own.size * 16, own.size * 10),
    )(at, own, *arrived)


def finish_body(own, a, b, d, rest, ra, rb, rd, out):
    high, wide = own.shape
    for first, v, arrived in ((0, own[...], (a, b, d)), (wide, rest[...], (ra, rb, rd))):
        for m in arrived:
            v = v + plain(m[:high, :]) * scale_of(m[high:, :])
        out[:, first:first + v.shape[1]] = v


def finish(bulk, rest):
    high = bulk[0].shape[0]
    ao = bulk[0].shape[1] + rest[0].shape[1]
    return pl.pallas_call(
        finish_body,
        out_shape=jax.ShapeDtypeStruct((high, ao), F32),
        in_specs=[whole()] * 8,
        out_specs=whole(),
        compiler_params=params(8),
        cost_estimate=cost(high * ao * 8, high * ao * 14),
    )(*bulk, *rest)


def shards(half, metric, survive):
    _, _, ao = half.shape
    at = jnp.stack([lax.axis_index(a) for a in AXES]).astype(jnp.int32)
    blocks = survive.shape[2]
    gate = jnp.repeat(survive.reshape(1, blocks).astype(BF), ao // blocks, axis=1)
    wide = ao // 8

    parts = screen(at, half, gate, metric)
    here = [parts[0]] + [None] * 3
    for k in (2, 1, 3):
        here[k] = send(parts[k], along_z(k))
    there = [send(v, other_core) for v in here]
    rows, turned = fit(at, [v for pair in zip(here, there) for v in pair])

    bulk, rest, narrow = [None] * 4, [None] * 4, wide // 3
    for k in (2, 1, 3, 0):
        bulk[k] = bulk_k(at, rows, turned, k, wide - narrow)
        if k:
            bulk[k] = send(bulk[k], first_axis(k))
        rest[k] = rest_k(at, rows, turned, k, wide - narrow, narrow)
        if k:
            rest[k] = send(rest[k], along_z(k))
    rest = list(sum_groups(at, rest[0], rest[1:]))
    rest[1:] = [send(rest[k], first_axis(k)) for k in (1, 2, 3)]
    bulk = list(sum_rows(at, bulk[0], bulk[1:], wide - narrow))
    bulk[1:] = [send(bulk[k], second_axis(k)) for k in (1, 2, 3)]
    rest = list(sum_rows(at, rest[0], rest[1:], narrow))
    rest[1:] = [send(rest[k], second_axis(k)) for k in (1, 2, 3)]
    bulk = list(sum_columns(at, bulk[0], bulk[1:], wide - narrow))
    bulk[1:] = [send(bulk[k], along_z(k)) for k in (1, 2, 3)]
    return finish(bulk, rest)


def solution(mesh):
    finer = Mesh(mesh.devices.reshape(4, 2, 4, 4), AXES)
    placed = (P(("z", "c"), ("x", "y"), None), P(("z", "c"), None), P(("z", "c"), ("x", "y"), None))
    return jax.shard_map(
        shards, mesh=finer, in_specs=placed, out_specs=P(("x", "y"), ("z", "c")), check_vma=False
    )
```

```python
import functools

import jax
import jax.numpy as jnp
from jax import lax
from jax.experimental import pallas as pl
from jax.experimental.pallas import tpu as pltpu
from jax.sharding import Mesh
from jax.sharding import PartitionSpec as P


AXES = ("z", "c", "x", "y")
BF = jnp.bfloat16
F32 = jnp.float32
I16 = jnp.int16
MIB = 1 << 20
RING = 4
ORDER = (2, 1, 3, 0)
TAIL = 16


def whole():
    return pl.BlockSpec(memory_space=pltpu.VMEM)


def scalars():
    return pl.BlockSpec(memory_space=pltpu.SMEM)


def params(mib):
    return pltpu.CompilerParams(vmem_limit_bytes=mib * MIB)


def cost(flops, moved):
    return pl.CostEstimate(flops=flops, bytes_accessed=moved, transcendentals=0)


def place(z, c, x, y):
    return ((z % 4) * 2 + c) * 16 + (x % 4) * 4 + y % 4


def moves(shift):
    every = [(z, c, x, y) for z in range(4) for c in range(2) for x in range(4) for y in range(4)]
    return [(place(*d), place(*shift(*d))) for d in every]


def send(v, shift):
    return lax.ppermute(v, AXES, moves(shift))


def along_z(k):
    return lambda z, c, x, y: (z + k, c, x, y)


def other_core(z, c, x, y):
    return (z, 1 - c, x, y)


def first_axis(k):
    return lambda z, c, x, y: (z, c, x + k, y) if c == 0 else (z, c, x, y + k)


def second_axis(k):
    return lambda z, c, x, y: (z, c, x, y + k) if c == 0 else (z, c, x + k, y)


def screen_body(at, half, gate, metric, *outs_and_scratch):
    outs, turned = outs_and_scratch[:4], outs_and_scratch[4]
    lanes = 512

    def step(n, carry):
        cut = pl.ds(pl.multiple_of(n * lanes, lanes), lanes)
        kept = half[:, :, cut] * gate[:, cut][None]
        turned[:, :, cut] = jnp.swapaxes(kept.astype(F32), 0, 1).astype(BF)
        return carry

    ao = half.shape[2]
    lax.fori_loop(0, ao // lanes, step, 0)
    group = outs[0].shape[0]
    for k in range(RING):
        first = lax.rem(at[0] + k, RING) * group
        outs[k][:, :, :ao] = turned[pl.ds(first, group)]
        outs[k][:, :, ao:] = jnp.broadcast_to(metric[...][None], (group,) + metric.shape)


def screen(at, half, gate, metric):
    aux, occ, ao = half.shape
    out = jax.ShapeDtypeStruct((occ // RING, aux, ao + metric.shape[1]), BF)
    return pl.pallas_call(
        screen_body,
        out_shape=[out] * RING,
        in_specs=[scalars(), whole(), whole(), whole()],
        out_specs=[whole()] * RING,
        scratch_shapes=[pltpu.VMEM((occ, aux, ao), BF)],
        compiler_params=params(16),
        cost_estimate=cost(half.size, half.size * 4),
    )(at, half, gate, metric)


def fit_body(at, *refs):
    pieces, (bulk, rest, turned, mixed, fresh) = refs[:8], refs[8:]
    step = pl.program_id(0)
    ao = fresh.shape[1]
    aux = mixed.shape[0]
    part = aux // 8

    @pl.when(step == 0)
    def _():
        metric = jnp.concatenate([p[0][:, ao:] for p in pieces], axis=0)
        source = lax.broadcasted_iota(jnp.int32, (aux, aux), 0)
        n = lax.broadcasted_iota(jnp.int32, (aux, aux), 1)
        slot = n // part
        up = lax.rem(at[0] - slot // 2 + RING, RING)
        core = jnp.where(slot % 2 == 0, at[1], 1 - at[1])
        wanted = (up * 2 + core) * part + n % part
        pick = jnp.where(source == wanted, 1.0, 0.0).astype(BF)
        mixed[...] = jnp.dot(metric, pick, preferred_element_type=F32).astype(BF)

    screened = jnp.concatenate([p[0][:, :ao] for p in pieces], axis=0)
    fitted = jnp.dot(mixed[...], screened, preferred_element_type=F32).astype(BF)
    fresh[...] = fitted
    wide, narrow = bulk.shape[1] // RING, rest.shape[1] // RING
    for n in range(RING):
        column = n * (ao // RING) + at[1] * (wide + narrow)
        bulk[:, n * wide:(n + 1) * wide] = fresh[:, pl.ds(pl.multiple_of(column, 128), wide)]
        column = lax.rem(at[0] + ORDER[n], RING) * (ao // RING) + at[1] * (wide + narrow) + wide
        rest[:, n * narrow:(n + 1) * narrow] = fresh[:, pl.ds(pl.multiple_of(column, 128), narrow)]
    flipped = fitted.T
    cut = pl.ds(pl.multiple_of(step * aux, aux), aux)
    high = ao // (RING * RING)
    for x in range(RING):
        for y in range(RING):
            n = x * RING + y
            to = jnp.where(at[1] == 0, n, y * RING + x) * high
            turned[pl.ds(pl.multiple_of(to, 64), high), cut] = flipped[n * high:(n + 1) * high]


def fit(at, pieces):
    group, part, wide = pieces[0].shape
    aux = part * 8
    ao = wide - aux
    piece = pl.BlockSpec((1, part, wide), lambda i: (i, 0, 0))
    return pl.pallas_call(
        fit_body,
        grid=(group,),
        out_shape=[jax.ShapeDtypeStruct((group * aux, n), BF) for n in (ao // 3, ao // 6)]
        + [jax.ShapeDtypeStruct((ao, group * aux), BF)],
        in_specs=[scalars()] + [piece] * 8,
        out_specs=[pl.BlockSpec((aux, n), lambda i: (i, 0)) for n in (ao // 3, ao // 6)]
        + [pl.BlockSpec((ao, group * aux), lambda i: (0, 0))],
        scratch_shapes=[pltpu.VMEM((aux, aux), BF), pltpu.VMEM((aux, ao), BF)],
        compiler_params=params(28),
        cost_estimate=cost(2 * group * aux * aux * ao, group * aux * ao * 6),
    )(at, *pieces)


def exponent(top):
    return jnp.floor(14.9 - jnp.log2(jnp.maximum(top, 1e-30)))


def coded(v, e):
    return jnp.round(v * jnp.exp2(e)).astype(jnp.int32).astype(I16)


def marked(e):
    return jnp.broadcast_to(e, (TAIL, e.shape[1])).astype(jnp.int32).astype(I16)


def scale_of(tail):
    return jnp.exp2(-tail.astype(jnp.int32).astype(F32)[:1])


def plain(q):
    return q.astype(jnp.int32).astype(F32)


def write(out, first, block):
    if out.dtype == F32:
        out[first:first + block.shape[0], :] = block
    else:
        e = exponent(jnp.max(jnp.abs(block), axis=0, keepdims=True))
        end = first + block.shape[0]
        out[first:end, :] = coded(block, e)
        out[end:end + TAIL, :] = marked(e)


def bulk_body(shift, at, bulk, turned, out):
    total = turned.shape[0] // RING
    g = lax.rem(jnp.where(at[1] == 0, at[2], at[3]) + shift, RING)
    left = turned[pl.ds(pl.multiple_of(g * total, 256), total), :]
    write(out, 0, jnp.dot(left, bulk[...], preferred_element_type=F32))


def bulk_k(at, bulk, turned, shift):
    depth, columns = bulk.shape
    total = turned.shape[0] // RING
    shape = (total + (TAIL if shift else 0), columns)
    half = columns // 2
    return pl.pallas_call(
        functools.partial(bulk_body, shift),
        grid=(2,),
        out_shape=jax.ShapeDtypeStruct(shape, I16 if shift else F32),
        in_specs=[scalars(), pl.BlockSpec((depth, half), lambda j: (0, j)), whole()],
        out_specs=pl.BlockSpec((shape[0], half), lambda j: (0, j)),
        compiler_params=params(28),
        cost_estimate=cost(2 * depth * total * columns, total * columns * 2),
    )(at, bulk, turned)


def rest_body(rest, turned, *outs):
    both = jnp.dot(turned[...], rest[...], preferred_element_type=F32)
    narrow = both.shape[1] // 2
    write(outs[0], 0, both[:, :narrow])
    write(outs[1], 0, both[:, narrow:])


def rest_k(rest, turned, pair):
    depth = rest.shape[0]
    ao = turned.shape[0]
    total, narrow = ao // RING, rest.shape[1] // RING
    each = [total + (TAIL if k else 0) for k in ORDER[2 * pair:2 * pair + 2]]
    return pl.pallas_call(
        rest_body,
        grid=(RING,),
        out_shape=[jax.ShapeDtypeStruct((RING * n, narrow), I16 if n > total else F32) for n in each],
        in_specs=[
            pl.BlockSpec((depth, 2 * narrow), lambda g: (0, pair)),
            pl.BlockSpec((total, depth), lambda g: (g, 0)),
        ],
        out_specs=[pl.BlockSpec((n, narrow), lambda g: (g, 0)) for n in each],
        compiler_params=params(28),
        cost_estimate=cost(4 * depth * ao * narrow, ao * narrow * 4),
    )(rest, turned)


def second_body(at, bulk, ba, bb, bd, rest, ra, rb, rd, kept, *outs):
    high = kept.shape[0]
    wide = kept.shape[1]
    total = bulk.shape[0]
    h = jnp.where(at[1] == 0, at[3], at[2])

    def part(k, own, arrived, first, lanes):
        row = pl.multiple_of(lax.rem(h + k, RING) * high, 64)
        v = own[pl.ds(pl.multiple_of(first * total + row, 64), high), :]
        for m in arrived:
            start = first * (total + TAIL)
            v = v + plain(m[pl.ds(pl.multiple_of(start + row, 16), high), :]) * scale_of(
                m[start + total:start + total + TAIL, :]
            )
        if k == 0:
            kept[:, lanes] = v
        else:
            e = exponent(jnp.max(jnp.abs(v), axis=0, keepdims=True))
            outs[k - 1][:high, lanes] = coded(v, e)
            outs[k - 1][high:, lanes] = marked(e)

    @pl.when(pl.program_id(0) < RING)
    def _():
        for k in range(RING):
            part(k, bulk, (ba, bb, bd), 0, slice(0, wide))

    @pl.when(pl.program_id(0) >= RING)
    def _():
        for k in range(RING):
            for n in range(2):
                part(k, rest, (ra, rb, rd), n, slice(n * wide // 2, (n + 1) * wide // 2))


def second(at, bulk, rest):
    total, columns = bulk[0].shape
    wide, high = columns // RING, total // RING
    narrow = wide // 2
    every = columns + RING * narrow

    def of_bulk(rows):
        return pl.BlockSpec((rows, wide), lambda j: (0, jnp.minimum(j, RING - 1)))

    def of_rest(rows):
        return pl.BlockSpec((2 * rows, narrow), lambda j: (jnp.maximum(j - RING, 0), 0))

    return pl.pallas_call(
        second_body,
        grid=(RING + 2,),
        out_shape=[jax.ShapeDtypeStruct((high, every), F32)]
        + [jax.ShapeDtypeStruct((high + TAIL, every), I16)] * 3,
        in_specs=[scalars(), of_bulk(total)] + [of_bulk(total + TAIL)] * 3
        + [of_rest(total)] + [of_rest(total + TAIL)] * 3,
        out_specs=[pl.BlockSpec((n, wide), lambda j: (0, j)) for n in [high] + [high + TAIL] * 3],
        compiler_params=params(24),
        cost_estimate=cost(total * every * 16, total * every * 10),
        name="second_sum",
    )(at, *bulk, *rest)


def third_body(at, own, a, b, d, bulk, b1, b2, b3, rest, r1, r2, r3):
    high, wide = bulk.shape
    narrow = rest.shape[1]
    g = jnp.where(at[1] == 0, at[2], at[3])
    for base, step, place_at, outs in (
        (0, wide, at[0], (bulk, b1, b2, b3)), (RING * wide, narrow, g, (rest, r1, r2, r3))
    ):
        for k in range(RING):
            cut = pl.ds(pl.multiple_of(base + lax.rem(place_at + k, RING) * step, 128), step)
            v = own[:, cut]
            for m in (a, b, d):
                v = v + plain(m[:high, cut]) * scale_of(m[high:, cut])
            write(outs[k], 0, v)


def third(at, own, arrived, wide, narrow):
    high = own.shape[0]

    def four(lanes):
        return [jax.ShapeDtypeStruct((high, lanes), F32)] + [jax.ShapeDtypeStruct((high + TAIL, lanes), I16)] * 3

    out = pl.pallas_call(
        third_body,
        out_shape=four(wide) + four(narrow),
        in_specs=[scalars()] + [whole()] * 4,
        out_specs=[whole()] * 8,
        compiler_params=params(16),
        cost_estimate=cost(own.size * 16, own.size * 10),
        name="third_sum",
    )(at, own, *arrived)
    return list(out[:4]), list(out[4:])


def finish_body(own, a, b, d, rest, ra, rb, rd, out):
    high, wide = own.shape
    for first, v, arrived in ((0, own[...], (a, b, d)), (wide, rest[...], (ra, rb, rd))):
        for m in arrived:
            v = v + plain(m[:high, :]) * scale_of(m[high:, :])
        out[:, first:first + v.shape[1]] = v


def finish(bulk, rest):
    high = bulk[0].shape[0]
    ao = bulk[0].shape[1] + rest[0].shape[1]
    return pl.pallas_call(
        finish_body,
        out_shape=jax.ShapeDtypeStruct((high, ao), F32),
        in_specs=[whole()] * 8,
        out_specs=whole(),
        compiler_params=params(8),
        cost_estimate=cost(high * ao * 8, high * ao * 14),
    )(*bulk, *rest)


def shards(half, metric, survive):
    _, _, ao = half.shape
    at = jnp.stack([lax.axis_index(a) for a in AXES]).astype(jnp.int32)
    blocks = survive.shape[2]
    gate = jnp.repeat(survive.reshape(1, blocks).astype(BF), ao // blocks, axis=1)
    wide = ao // 8

    parts = screen(at, half, gate, metric)
    here = [parts[0]] + [None] * 3
    for k in (2, 1, 3):
        here[k] = send(parts[k], along_z(k))
    there = [send(v, other_core) for v in here]
    bulk_rows, rest_rows, turned = fit(at, [v for pair in zip(here, there) for v in pair])

    bulk, rest = [None] * 4, [None] * 4

    def bulk_step(k):
        bulk[k] = bulk_k(at, bulk_rows, turned, k)
        if k:
            bulk[k] = send(bulk[k], first_axis(k))

    def rest_step(pair):
        out = rest_k(rest_rows, turned, pair)
        for k, v in zip(ORDER[2 * pair:2 * pair + 2], out):
            rest[k] = send(v, along_z(k)) if k else v

    bulk_step(2)
    rest_step(0)
    bulk_step(1)
    bulk_step(3)
    rest_step(1)
    bulk_step(0)
    own, *out = second(at, bulk, rest)
    arrived = [send(out[k - 1], second_axis(k)) for k in (2, 1, 3)]
    bulk, rest = third(at, own, arrived, wide - wide // 3, wide // 3)
    bulk[1:] = [send(bulk[k], along_z(k)) for k in (1, 2, 3)]
    rest[1:] = [send(rest[k], first_axis(k)) for k in (1, 2, 3)]
    return finish(bulk, rest)


def solution(mesh):
    finer = Mesh(mesh.devices.reshape(4, 2, 4, 4), AXES)
    placed = (P(("z", "c"), ("x", "y"), None), P(("z", "c"), None), P(("z", "c"), ("x", "y"), None))
    return jax.shard_map(
        shards, mesh=finer, in_specs=placed, out_specs=P(("x", "y"), ("z", "c")), check_vma=False
    )
```

```python
import functools

import jax
import jax.numpy as jnp
from jax import lax
from jax.experimental import pallas as pl
from jax.experimental.pallas import tpu as pltpu
from jax.sharding import Mesh
from jax.sharding import PartitionSpec as P


AXES = ("z", "c", "x", "y")
BF = jnp.bfloat16
F32 = jnp.float32
I16 = jnp.int16
MIB = 1 << 20
RING = 4
ORDER = (2, 1, 3, 0)
TAIL = 16


def whole():
    return pl.BlockSpec(memory_space=pltpu.VMEM)


def scalars():
    return pl.BlockSpec(memory_space=pltpu.SMEM)


def params(mib):
    return pltpu.CompilerParams(vmem_limit_bytes=mib * MIB)


def cost(flops, moved):
    return pl.CostEstimate(flops=flops, bytes_accessed=moved, transcendentals=0)


def place(z, c, x, y):
    return ((z % 4) * 2 + c) * 16 + (x % 4) * 4 + y % 4


def moves(shift):
    every = [(z, c, x, y) for z in range(4) for c in range(2) for x in range(4) for y in range(4)]
    return [(place(*d), place(*shift(*d))) for d in every]


def send(v, shift):
    return lax.ppermute(v, AXES, moves(shift))


def along_z(k):
    return lambda z, c, x, y: (z + k, c, x, y)


def other_core(z, c, x, y):
    return (z, 1 - c, x, y)


def first_axis(k):
    return lambda z, c, x, y: (z, c, x + k, y) if c == 0 else (z, c, x, y + k)


def second_axis(k):
    return lambda z, c, x, y: (z, c, x, y + k) if c == 0 else (z, c, x + k, y)


def screen_body(at, half, gate, *outs_and_scratch):
    outs, turned = outs_and_scratch[:4], outs_and_scratch[4]
    kept = half[...] * gate[...][None]
    turned[...] = jnp.swapaxes(kept.astype(F32), 0, 1).astype(BF)
    group = outs[0].shape[0]
    for k in range(RING):
        outs[k][...] = turned[pl.ds(lax.rem(at[0] + k, RING) * group, group)]


def screen(at, half, gate):
    aux, occ, ao = half.shape
    lanes = 512
    group = occ // RING
    return pl.pallas_call(
        screen_body,
        grid=(ao // lanes,),
        out_shape=[jax.ShapeDtypeStruct((group, aux, ao), BF)] * RING,
        in_specs=[
            scalars(),
            pl.BlockSpec((aux, occ, lanes), lambda j: (0, 0, j)),
            pl.BlockSpec((1, lanes), lambda j: (0, j)),
        ],
        out_specs=[pl.BlockSpec((group, aux, lanes), lambda j: (0, 0, j))] * RING,
        scratch_shapes=[pltpu.VMEM((occ, aux, lanes), BF)],
        compiler_params=params(16),
        cost_estimate=cost(half.size, half.size * 4),
        name="screen",
    )(at, half, gate)


def join_body(at, *refs):
    metrics, mixed = refs[:4], refs[4]
    aux = mixed.shape[0]
    part = aux // 8
    metric = jnp.concatenate([m[...] for m in metrics], axis=0)
    source = lax.broadcasted_iota(jnp.int32, (aux, aux), 0)
    n = lax.broadcasted_iota(jnp.int32, (aux, aux), 1)
    slot = n // part
    up = lax.rem(at[0] - slot // 2 + RING, RING)
    core = jnp.where(slot % 2 == 0, at[1], 1 - at[1])
    wanted = (up * 2 + core) * part + n % part
    pick = jnp.where(source == wanted, 1.0, 0.0).astype(BF)
    mixed[...] = jnp.dot(metric, pick, preferred_element_type=F32).astype(BF)


def join(at, metrics):
    aux = metrics[0].shape[1]
    return pl.pallas_call(
        join_body,
        out_shape=jax.ShapeDtypeStruct((aux, aux), BF),
        in_specs=[scalars()] + [whole()] * 4,
        out_specs=whole(),
        compiler_params=params(4),
        cost_estimate=cost(2 * aux**3, aux * aux * 4),
        name="join",
    )(at, *metrics)


def fit_body(at, *refs):
    pieces, mixed, (a1, a2, rest, turned, fresh) = refs[:8], refs[8], refs[9:]
    step = pl.program_id(0)
    ao = fresh.shape[1]
    aux = mixed.shape[0]

    screened = jnp.concatenate([p[0] for p in pieces], axis=0)
    fitted = jnp.dot(mixed[...], screened, preferred_element_type=F32).astype(BF)
    fresh[...] = fitted
    narrow = rest.shape[1] // RING
    for n in range(RING):
        column = n * (ao // RING) + at[1] * 3 * narrow
        cut = slice(n * narrow, (n + 1) * narrow)
        a1[:, cut] = fresh[:, pl.ds(pl.multiple_of(column, 128), narrow)]
        a2[:, cut] = fresh[:, pl.ds(pl.multiple_of(column + narrow, 128), narrow)]
        column = lax.rem(at[0] + ORDER[n], RING) * (ao // RING) + at[1] * 3 * narrow + 2 * narrow
        rest[:, cut] = fresh[:, pl.ds(pl.multiple_of(column, 128), narrow)]
    flipped = fitted.T
    cut = pl.ds(pl.multiple_of(step * aux, aux), aux)
    high = ao // (RING * RING)
    for x in range(RING):
        for y in range(RING):
            n = x * RING + y
            to = jnp.where(at[1] == 0, n, y * RING + x) * high
            turned[pl.ds(pl.multiple_of(to, 64), high), cut] = flipped[n * high:(n + 1) * high]


def fit(at, pieces, mixed):
    group, part, ao = pieces[0].shape
    aux = part * 8
    piece = pl.BlockSpec((1, part, ao), lambda i: (i, 0, 0))
    own = pl.BlockSpec((aux, ao // 6), lambda i: (i, 0))
    return pl.pallas_call(
        fit_body,
        grid=(group,),
        out_shape=[jax.ShapeDtypeStruct((group * aux, ao // 6), BF)] * 3
        + [jax.ShapeDtypeStruct((ao, group * aux), BF)],
        in_specs=[scalars()] + [piece] * 8 + [whole()],
        out_specs=[own] * 3 + [pl.BlockSpec((ao, group * aux), lambda i: (0, 0))],
        scratch_shapes=[pltpu.VMEM((aux, ao), BF)],
        compiler_params=params(28),
        cost_estimate=cost(2 * group * aux * aux * ao, group * aux * ao * 6),
        name="fit",
    )(at, *pieces, mixed)


def exponent(top):
    return jnp.floor(14.9 - jnp.log2(jnp.maximum(top, 1e-30)))


def coded(v, e):
    return jnp.round(v * jnp.exp2(e)).astype(jnp.int32).astype(I16)


def marked(e):
    return jnp.broadcast_to(e, (TAIL, e.shape[1])).astype(jnp.int32).astype(I16)


def scale_of(tail):
    return jnp.exp2(-tail.astype(jnp.int32).astype(F32)[:1])


def plain(q):
    return q.astype(jnp.int32).astype(F32)


def write(out, first, block):
    if out.dtype == F32:
        out[first:first + block.shape[0], :] = block
    else:
        e = exponent(jnp.max(jnp.abs(block), axis=0, keepdims=True))
        end = first + block.shape[0]
        out[first:end, :] = coded(block, e)
        out[end:end + TAIL, :] = marked(e)


def bulk_body(shift, at, bulk, turned, out):
    total = turned.shape[0] // RING
    g = lax.rem(jnp.where(at[1] == 0, at[2], at[3]) + shift, RING)
    left = turned[pl.ds(pl.multiple_of(g * total, 256), total), :]
    write(out, 0, jnp.dot(left, bulk[...], preferred_element_type=F32))


def bulk_k(at, bulk, turned, shift):
    depth, columns = bulk.shape
    total = turned.shape[0] // RING
    shape = (total + (TAIL if shift else 0), columns)
    return pl.pallas_call(
        functools.partial(bulk_body, shift),
        out_shape=jax.ShapeDtypeStruct(shape, I16 if shift else F32),
        in_specs=[scalars(), whole(), whole()],
        out_specs=whole(),
        compiler_params=params(28),
        cost_estimate=cost(2 * depth * total * columns, total * columns * 2),
    )(at, bulk, turned)


def rest_body(rest, turned, *outs):
    both = jnp.dot(turned[...], rest[...], preferred_element_type=F32)
    narrow = both.shape[1] // 2
    write(outs[0], 0, both[:, :narrow])
    write(outs[1], 0, both[:, narrow:])


def rest_k(rest, turned, pair):
    depth = rest.shape[0]
    ao = turned.shape[0]
    total, narrow = ao // RING, rest.shape[1] // RING
    each = [total + (TAIL if k else 0) for k in ORDER[2 * pair:2 * pair + 2]]
    return pl.pallas_call(
        rest_body,
        grid=(RING,),
        out_shape=[jax.ShapeDtypeStruct((RING * n, narrow), I16 if n > total else F32) for n in each],
        in_specs=[
            pl.BlockSpec((depth, 2 * narrow), lambda g: (0, pair)),
            pl.BlockSpec((total, depth), lambda g: (g, 0)),
        ],
        out_specs=[pl.BlockSpec((n, narrow), lambda g: (g, 0)) for n in each],
        compiler_params=params(28),
        cost_estimate=cost(4 * depth * ao * narrow, ao * narrow * 4),
    )(rest, turned)


def second_part(at, own, arrived, kept, outs):
    high = kept.shape[0]
    total = own.shape[0]
    h = jnp.where(at[1] == 0, at[3], at[2])
    scales = [scale_of(m[total:, :]) for m in arrived]
    for k in range(RING):
        row = pl.ds(pl.multiple_of(lax.rem(h + k, RING) * high, 64), high)
        v = own[row, :]
        for m, scale in zip(arrived, scales):
            v = v + plain(m[row, :]) * scale
        write(kept if k == 0 else outs[k - 1], 0, v)


def second_body(at, a, a1, a2, a3, kept, *outs):
    second_part(at, a, (a1, a2, a3), kept, outs)


def second_both_body(at, a, a1, a2, a3, b, b1, b2, b3, kept, *outs):
    @pl.when(pl.program_id(0) < 2)
    def _():
        second_part(at, a, (a1, a2, a3), kept, outs)

    @pl.when(pl.program_id(0) >= 2)
    def _():
        narrow = b.shape[1]
        for n in range(2):
            lanes = slice(n * narrow, (n + 1) * narrow)

            def rows(ref):
                return ref.at[n * (ref.shape[0] // 2):(n + 1) * (ref.shape[0] // 2)]

            second_part(at, rows(b), [rows(m) for m in (b1, b2, b3)], kept.at[:, lanes], [o.at[:, lanes] for o in outs])


def second(at, bulk, rest=()):
    total, columns = bulk[0].shape
    wide, high = columns // 2, total // RING
    steps = 4 if rest else 2
    every = steps * wide

    def of_bulk(rows):
        return pl.BlockSpec((rows, wide), lambda j: (0, jnp.minimum(j, 1)))

    def of_rest(rows):
        return pl.BlockSpec((2 * rows, wide // 2), lambda j: (jnp.maximum(j - 2, 0), 0))

    specs = [of_bulk(total)] + [of_bulk(total + TAIL)] * 3
    if rest:
        specs += [of_rest(total)] + [of_rest(total + TAIL)] * 3
    return pl.pallas_call(
        second_both_body if rest else second_body,
        grid=(steps,),
        out_shape=[jax.ShapeDtypeStruct((high, every), F32)]
        + [jax.ShapeDtypeStruct((high + TAIL, every), I16)] * 3,
        in_specs=[scalars()] + specs,
        out_specs=[pl.BlockSpec((n, wide), lambda j: (0, j)) for n in [high] + [high + TAIL] * 3],
        compiler_params=params(24),
        cost_estimate=cost(total * every * 16, total * every * 10),
        name="second_sum",
    )(at, *bulk, *rest)


def third_body(at, p, p1, p2, p3, q, q1, q2, q3, bulk, b1, b2, b3, rest, r1, r2, r3):
    high, step = rest.shape
    g = jnp.where(at[1] == 0, at[2], at[3])
    for own, arrived, base, start, outs in (
        (p, (p1, p2, p3), 0, at[0], [o.at[:, :step] for o in (bulk, b1, b2, b3)]),
        (q, (q1, q2, q3), 0, at[0], [o.at[:, step:] for o in (bulk, b1, b2, b3)]),
        (q, (q1, q2, q3), RING * step, g, (rest, r1, r2, r3)),
    ):
        for k in range(RING):
            cut = pl.ds(pl.multiple_of(base + lax.rem(start + k, RING) * step, 128), step)
            v = own[:, cut]
            for m in arrived:
                v = v + plain(m[:high, cut]) * scale_of(m[high:, cut])
            write(outs[k], 0, v)


def third(at, first, both):
    high, every = both[0].shape
    narrow = every // 8

    def four(lanes):
        return [jax.ShapeDtypeStruct((high, lanes), F32)] + [jax.ShapeDtypeStruct((high + TAIL, lanes), I16)] * 3

    out = pl.pallas_call(
        third_body,
        out_shape=four(2 * narrow) + four(narrow),
        in_specs=[scalars()] + [whole()] * 8,
        out_specs=[whole()] * 8,
        compiler_params=params(16),
        cost_estimate=cost(high * every * 24, high * every * 15),
        name="third_sum",
    )(at, *first, *both)
    return list(out[:4]), list(out[4:])


def finish_body(own, a, b, d, rest, ra, rb, rd, out):
    high, wide = own.shape
    for first, v, arrived in ((0, own[...], (a, b, d)), (wide, rest[...], (ra, rb, rd))):
        for m in arrived:
            v = v + plain(m[:high, :]) * scale_of(m[high:, :])
        out[:, first:first + v.shape[1]] = v


def finish(bulk, rest):
    high = bulk[0].shape[0]
    ao = bulk[0].shape[1] + rest[0].shape[1]
    return pl.pallas_call(
        finish_body,
        out_shape=jax.ShapeDtypeStruct((high, ao), F32),
        in_specs=[whole()] * 8,
        out_specs=whole(),
        compiler_params=params(8),
        cost_estimate=cost(high * ao * 8, high * ao * 14),
    )(*bulk, *rest)


def shards(half, metric, survive):
    _, _, ao = half.shape
    at = jnp.stack([lax.axis_index(a) for a in AXES]).astype(jnp.int32)
    blocks = survive.shape[2]
    gate = jnp.repeat(survive.reshape(1, blocks).astype(BF), ao // blocks, axis=1)

    pair = jnp.concatenate([metric, send(metric, other_core)], axis=0)
    parts = screen(at, half, gate)
    here, metrics = [parts[0]] + [None] * 3, [pair] + [None] * 3
    for k in ORDER[:3]:
        here[k] = send(parts[k], along_z(k))
    for k in ORDER[:3]:
        metrics[k] = send(pair, along_z(k))
    mixed = join(at, metrics)
    there = [send(v, other_core) for v in here]
    *columns, turned = fit(at, [v for both in zip(here, there) for v in both], mixed)

    moved = {}

    def bulk_step(part, k):
        v = bulk_k(at, columns[part], turned, k)
        if k:
            v = send(v, first_axis(k))
        moved[part, k] = v

    def rest_step(pair):
        out = rest_k(columns[2], turned, pair)
        for k, v in zip(ORDER[2 * pair:2 * pair + 2], out):
            moved[2, k] = send(v, along_z(k)) if k else v

    bulk_step(0, 2)
    rest_step(0)
    bulk_step(0, 1)
    bulk_step(0, 3)
    rest_step(1)
    bulk_step(1, 2)
    bulk_step(1, 1)
    bulk_step(1, 3)
    bulk_step(0, 0)
    bulk_step(1, 0)
    early = list(second(at, [moved[0, k] for k in range(4)]))
    for k in ORDER[:3]:
        early[k] = send(early[k], second_axis(k))
    late = list(second(at, [moved[1, k] for k in range(4)], [moved[2, k] for k in range(4)]))
    for k in ORDER[:3]:
        late[k] = send(late[k], second_axis(k))
    bulk, rest = third(at, early, late)
    bulk[1:] = [send(bulk[k], along_z(k)) for k in (1, 2, 3)]
    rest[1:] = [send(rest[k], first_axis(k)) for k in (1, 2, 3)]
    return finish(bulk, rest)


def solution(mesh):
    finer = Mesh(mesh.devices.reshape(4, 2, 4, 4), AXES)
    placed = (P(("z", "c"), ("x", "y"), None), P(("z", "c"), None), P(("z", "c"), ("x", "y"), None))
    return jax.shard_map(
        shards, mesh=finer, in_specs=placed, out_specs=P(("x", "y"), ("z", "c")), check_vma=False
    )
```

```python
import functools

import jax
import jax.numpy as jnp
from jax import lax
from jax.experimental import pallas as pl
from jax.experimental.pallas import tpu as pltpu
from jax.sharding import Mesh
from jax.sharding import PartitionSpec as P


AXES = ("z", "c", "x", "y")
BF = jnp.bfloat16
F32 = jnp.float32
I16 = jnp.int16
MIB = 1 << 20
RING = 4
ORDER = (2, 1, 3, 0)
TAIL = 16


def whole():
    return pl.BlockSpec(memory_space=pltpu.VMEM)


def scalars():
    return pl.BlockSpec(memory_space=pltpu.SMEM)


def params(mib):
    return pltpu.CompilerParams(vmem_limit_bytes=mib * MIB)


def cost(flops, moved):
    return pl.CostEstimate(flops=flops, bytes_accessed=moved, transcendentals=0)


def place(z, c, x, y):
    return ((z % 4) * 2 + c) * 16 + (x % 4) * 4 + y % 4


def moves(shift):
    every = [(z, c, x, y) for z in range(4) for c in range(2) for x in range(4) for y in range(4)]
    return [(place(*d), place(*shift(*d))) for d in every]


def send(v, shift):
    return lax.ppermute(v, AXES, moves(shift))


def along_z(k):
    return lambda z, c, x, y: (z + k, c, x, y)


def other_core(z, c, x, y):
    return (z, 1 - c, x, y)


def first_axis(k):
    return lambda z, c, x, y: (z, c, x + k, y) if c == 0 else (z, c, x, y + k)


def second_axis(k):
    return lambda z, c, x, y: (z, c, x, y + k) if c == 0 else (z, c, x + k, y)


def screen_body(at, half, gate, metric, *outs_and_scratch):
    outs, turned = outs_and_scratch[:4], outs_and_scratch[4]
    lanes = 512

    def step(n, carry):
        cut = pl.ds(pl.multiple_of(n * lanes, lanes), lanes)
        kept = half[:, :, cut] * gate[:, cut][None]
        turned[:, :, cut] = jnp.swapaxes(kept.astype(F32), 0, 1).astype(BF)
        return carry

    ao = half.shape[2]
    lax.fori_loop(0, ao // lanes, step, 0)
    group = outs[0].shape[0]
    for k in range(RING):
        first = lax.rem(at[0] + k, RING) * group
        outs[k][:, :, :ao] = turned[pl.ds(first, group)]
        outs[k][:, :, ao:] = jnp.broadcast_to(metric[...][None], (group,) + metric.shape)


def screen(at, half, gate, metric):
    aux, occ, ao = half.shape
    out = jax.ShapeDtypeStruct((occ // RING, aux, ao + metric.shape[1]), BF)
    return pl.pallas_call(
        screen_body,
        out_shape=[out] * RING,
        in_specs=[scalars(), whole(), whole(), whole()],
        out_specs=[whole()] * RING,
        scratch_shapes=[pltpu.VMEM((occ, aux, ao), BF)],
        compiler_params=params(16),
        cost_estimate=cost(half.size, half.size * 4),
    )(at, half, gate, metric)


def fit_body(at, *refs):
    pieces, (bulk, rest, turned, mixed, fresh) = refs[:8], refs[8:]
    step = pl.program_id(0)
    ao = fresh.shape[1]
    aux = mixed.shape[0]
    part = aux // 8

    @pl.when(step == 0)
    def _():
        metric = jnp.concatenate([p[0][:, ao:] for p in pieces], axis=0)
        source = lax.broadcasted_iota(jnp.int32, (aux, aux), 0)
        n = lax.broadcasted_iota(jnp.int32, (aux, aux), 1)
        slot = n // part
        up = lax.rem(at[0] - slot // 2 + RING, RING)
        core = jnp.where(slot % 2 == 0, at[1], 1 - at[1])
        wanted = (up * 2 + core) * part + n % part
        pick = jnp.where(source == wanted, 1.0, 0.0).astype(BF)
        mixed[...] = jnp.dot(metric, pick, preferred_element_type=F32).astype(BF)

    screened = jnp.concatenate([p[0][:, :ao] for p in pieces], axis=0)
    fitted = jnp.dot(mixed[...], screened, preferred_element_type=F32).astype(BF)
    fresh[...] = fitted
    wide, narrow = bulk.shape[1] // RING, rest.shape[1] // RING
    for n in range(RING):
        column = n * (ao // RING) + at[1] * (wide + narrow)
        bulk[:, n * wide:(n + 1) * wide] = fresh[:, pl.ds(pl.multiple_of(column, 128), wide)]
        column = lax.rem(at[0] + ORDER[n], RING) * (ao // RING) + at[1] * (wide + narrow) + wide
        rest[:, n * narrow:(n + 1) * narrow] = fresh[:, pl.ds(pl.multiple_of(column, 128), narrow)]
    flipped = fitted.T
    cut = pl.ds(pl.multiple_of(step * aux, aux), aux)
    high = ao // (RING * RING)
    for x in range(RING):
        for y in range(RING):
            n = x * RING + y
            to = jnp.where(at[1] == 0, n, y * RING + x) * high
            turned[pl.ds(pl.multiple_of(to, 64), high), cut] = flipped[n * high:(n + 1) * high]


def fit(at, pieces):
    group, part, wide = pieces[0].shape
    aux = part * 8
    ao = wide - aux
    piece = pl.BlockSpec((1, part, wide), lambda i: (i, 0, 0))
    return pl.pallas_call(
        fit_body,
        grid=(group,),
        out_shape=[jax.ShapeDtypeStruct((group * aux, n), BF) for n in (ao // 3, ao // 6)]
        + [jax.ShapeDtypeStruct((ao, group * aux), BF)],
        in_specs=[scalars()] + [piece] * 8,
        out_specs=[pl.BlockSpec((aux, n), lambda i: (i, 0)) for n in (ao // 3, ao // 6)]
        + [pl.BlockSpec((ao, group * aux), lambda i: (0, 0))],
        scratch_shapes=[pltpu.VMEM((aux, aux), BF), pltpu.VMEM((aux, ao), BF)],
        compiler_params=params(28),
        cost_estimate=cost(2 * group * aux * aux * ao, group * aux * ao * 6),
    )(at, *pieces)


def exponent(top):
    return jnp.floor(14.9 - jnp.log2(jnp.maximum(top, 1e-30)))


def coded(v, e):
    return jnp.round(v * jnp.exp2(e)).astype(jnp.int32).astype(I16)


def marked(e):
    return jnp.broadcast_to(e, (TAIL, e.shape[1])).astype(jnp.int32).astype(I16)


def scale_of(tail):
    return jnp.exp2(-tail.astype(jnp.int32).astype(F32)[:1])


def plain(q):
    return q.astype(jnp.int32).astype(F32)


def write(out, first, block):
    if out.dtype == F32:
        out[first:first + block.shape[0], :] = block
    else:
        e = exponent(jnp.max(jnp.abs(block), axis=0, keepdims=True))
        end = first + block.shape[0]
        out[first:end, :] = coded(block, e)
        out[end:end + TAIL, :] = marked(e)


def bulk_body(shift, at, bulk, turned, out):
    total = turned.shape[0] // RING
    g = lax.rem(jnp.where(at[1] == 0, at[2], at[3]) + shift, RING)
    left = turned[pl.ds(pl.multiple_of(g * total, 256), total), :]
    half = bulk.shape[1] // 2
    for n in range(2):
        lanes = slice(n * half, (n + 1) * half)
        write(out.at[:, lanes], 0, jnp.dot(left, bulk[:, lanes], preferred_element_type=F32))


def bulk_k(at, bulk, turned, shift):
    depth, columns = bulk.shape
    total = turned.shape[0] // RING
    shape = (total + (TAIL if shift else 0), columns)
    return pl.pallas_call(
        functools.partial(bulk_body, shift),
        out_shape=jax.ShapeDtypeStruct(shape, I16 if shift else F32),
        in_specs=[scalars(), whole(), whole()],
        out_specs=whole(),
        compiler_params=params(28),
        cost_estimate=cost(2 * depth * total * columns, total * columns * 2),
    )(at, bulk, turned)


def rest_body(rest, turned, *outs):
    both = jnp.dot(turned[...], rest[...], preferred_element_type=F32)
    narrow = both.shape[1] // 2
    write(outs[0], 0, both[:, :narrow])
    write(outs[1], 0, both[:, narrow:])


def rest_k(rest, turned, pair):
    depth = rest.shape[0]
    ao = turned.shape[0]
    total, narrow = ao // RING, rest.shape[1] // RING
    each = [total + (TAIL if k else 0) for k in ORDER[2 * pair:2 * pair + 2]]
    return pl.pallas_call(
        rest_body,
        grid=(RING,),
        out_shape=[jax.ShapeDtypeStruct((RING * n, narrow), I16 if n > total else F32) for n in each],
        in_specs=[
            pl.BlockSpec((depth, 2 * narrow), lambda g: (0, pair)),
            pl.BlockSpec((total, depth), lambda g: (g, 0)),
        ],
        out_specs=[pl.BlockSpec((n, narrow), lambda g: (g, 0)) for n in each],
        compiler_params=params(28),
        cost_estimate=cost(4 * depth * ao * narrow, ao * narrow * 4),
    )(rest, turned)


def gathered(own, arrived, first, tail, row, lanes):
    v = own[pl.ds(pl.multiple_of(first[0] + row, 64), first[2]), lanes]
    for m in arrived:
        cut = pl.ds(pl.multiple_of(first[1] + row, 16), first[2])
        v = v + plain(m[cut, lanes]) * scale_of(m[tail:tail + TAIL, lanes])
    return v


def second_body(groups, at, own, a, b, d, kept, *outs):
    high = kept.shape[0]
    total = own.shape[0] // groups
    h = jnp.where(at[1] == 0, at[3], at[2])
    step = own.shape[1] if groups > 1 else 256
    for k in range(RING):
        row = lax.rem(h + k, RING) * high
        out = kept if k == 0 else outs[k - 1]
        for n in range(groups):
            start = n * (total + TAIL)
            for lane in range(0, own.shape[1], step):
                v = gathered(
                    own, (a, b, d), (n * total, start, high), start + total, row, slice(lane, lane + step)
                )
                to = n * own.shape[1] + lane
                write(out.at[:, to:to + step], 0, v)


def second(at, parts, groups):
    total, columns = parts[0].shape
    high, every = total // groups // RING, columns * groups
    return list(pl.pallas_call(
        functools.partial(second_body, groups),
        out_shape=[jax.ShapeDtypeStruct((high, every), F32)]
        + [jax.ShapeDtypeStruct((high + TAIL, every), I16)] * 3,
        in_specs=[scalars()] + [whole()] * 4,
        out_specs=[whole()] * 4,
        compiler_params=params(24),
        cost_estimate=cost(total * columns * 16, total * columns * 10),
        name="second_sum",
    )(at, *parts))


def third_body(by_z, at, own, a, b, d, *outs):
    high, step = outs[0].shape
    start = at[0] if by_z else jnp.where(at[1] == 0, at[2], at[3])
    for k in range(RING):
        cut = pl.ds(pl.multiple_of(lax.rem(start + k, RING) * step, 128), step)
        write(outs[k], 0, gathered(own, (a, b, d), (0, 0, high), high, 0, cut))


def third(at, parts, by_z):
    high, every = parts[0].shape
    wide = every // RING
    return list(pl.pallas_call(
        functools.partial(third_body, by_z),
        out_shape=[jax.ShapeDtypeStruct((high, wide), F32)] + [jax.ShapeDtypeStruct((high + TAIL, wide), I16)] * 3,
        in_specs=[scalars()] + [whole()] * 4,
        out_specs=[whole()] * 4,
        compiler_params=params(16),
        cost_estimate=cost(high * every * 16, high * every * 10),
        name="third_sum",
    )(at, *parts))


def tick_body(at, out):
    for n in range(RING):
        out[n] = at[n]


def tick(at):
    return pl.pallas_call(
        tick_body,
        out_shape=jax.ShapeDtypeStruct(at.shape, at.dtype),
        in_specs=[scalars()],
        out_specs=scalars(),
        compiler_params=params(1),
        cost_estimate=cost(1000, 32),
        name="tick",
    )(at)


def finish_body(own, a, b, d, rest, ra, rb, rd, out):
    high, wide = own.shape
    for first, v, arrived in ((0, own[...], (a, b, d)), (wide, rest[...], (ra, rb, rd))):
        for m in arrived:
            v = v + plain(m[:high, :]) * scale_of(m[high:, :])
        out[:, first:first + v.shape[1]] = v


def finish(bulk, rest):
    high = bulk[0].shape[0]
    ao = bulk[0].shape[1] + rest[0].shape[1]
    return pl.pallas_call(
        finish_body,
        out_shape=jax.ShapeDtypeStruct((high, ao), F32),
        in_specs=[whole()] * 8,
        out_specs=whole(),
        compiler_params=params(8),
        cost_estimate=cost(high * ao * 8, high * ao * 14),
    )(*bulk, *rest)


def shards(half, metric, survive):
    _, _, ao = half.shape
    at = jnp.stack([lax.axis_index(a) for a in AXES]).astype(jnp.int32)
    blocks = survive.shape[2]
    gate = jnp.repeat(survive.reshape(1, blocks).astype(BF), ao // blocks, axis=1)

    parts = screen(at, half, gate, metric)
    here = [parts[0]] + [None] * 3
    for k in (2, 1, 3):
        here[k] = send(parts[k], along_z(k))
    there = [send(v, other_core) for v in here]
    bulk_rows, rest_rows, turned = fit(at, [v for pair in zip(here, there) for v in pair])

    bulk, rest = [None] * 4, [None] * 4

    def bulk_step(k):
        bulk[k] = bulk_k(at, bulk_rows, turned, k)
        if k:
            bulk[k] = send(bulk[k], first_axis(k))

    def rest_step(pair):
        out = rest_k(rest_rows, turned, pair)
        for k, v in zip(ORDER[2 * pair:2 * pair + 2], out):
            rest[k] = send(v, along_z(k)) if k else v

    def onward(parts, shift):
        for k in ORDER[:3]:
            parts[k] = send(parts[k], shift(k))

    rest_step(0)
    bulk_step(2)
    rest_step(1)
    bulk_step(1)
    bulk_step(3)
    bulk_step(0)
    rest = second(at, rest, RING)
    onward(rest, second_axis)
    then = tick(at)
    bulk = second(then, bulk, 1)
    onward(bulk, second_axis)
    rest = third(at, rest, False)
    onward(rest, first_axis)
    then = tick(then)
    bulk = third(then, bulk, True)
    onward(bulk, along_z)
    return finish(bulk, rest)


def solution(mesh):
    finer = Mesh(mesh.devices.reshape(4, 2, 4, 4), AXES)
    placed = (P(("z", "c"), ("x", "y"), None), P(("z", "c"), None), P(("z", "c"), ("x", "y"), None))
    return jax.shard_map(
        shards, mesh=finer, in_specs=placed, out_specs=P(("x", "y"), ("z", "c")), check_vma=False
    )
```

```python
import functools

import jax
import jax.numpy as jnp
from jax import lax
from jax.experimental import pallas as pl
from jax.experimental.pallas import tpu as pltpu
from jax.sharding import Mesh
from jax.sharding import PartitionSpec as P


AXES = ("z", "c", "x", "y")
BF = jnp.bfloat16
F32 = jnp.float32
I16 = jnp.int16
MIB = 1 << 20
RING = 4
ORDER = (2, 1, 3, 0)
TAIL = 16


def whole():
    return pl.BlockSpec(memory_space=pltpu.VMEM)


def scalars():
    return pl.BlockSpec(memory_space=pltpu.SMEM)


def position():
    return [lax.axis_index(a) for a in AXES]


def params(mib):
    return pltpu.CompilerParams(vmem_limit_bytes=mib * MIB)


def cost(flops, moved):
    return pl.CostEstimate(flops=flops, bytes_accessed=moved, transcendentals=0)


def place(z, c, x, y):
    return ((z % 4) * 2 + c) * 16 + (x % 4) * 4 + y % 4


def moves(shift):
    every = [(z, c, x, y) for z in range(4) for c in range(2) for x in range(4) for y in range(4)]
    return [(place(*d), place(*shift(*d))) for d in every]


def send(v, shift):
    return lax.ppermute(v, AXES, moves(shift))


def along_z(k):
    return lambda z, c, x, y: (z + k, c, x, y)


def other_core(z, c, x, y):
    return (z, 1 - c, x, y)


def first_axis(k):
    return lambda z, c, x, y: (z, c, x + k, y) if c == 0 else (z, c, x, y + k)


def second_axis(k):
    return lambda z, c, x, y: (z, c, x, y + k) if c == 0 else (z, c, x + k, y)


def screen_body(survive, half, metric, *rest):
    outs, (held, own, turned, sems) = rest[:4], rest[4:]
    at = position()
    ao = half.shape[2]
    block = ao // survive.shape[2]
    chunks = sems.shape[0] - 1
    lanes = ao // chunks
    copies = [
        pltpu.make_async_copy(half.at[:, :, cut], held.at[:, :, cut], sems.at[n])
        for n, cut in enumerate(slice(n * lanes, (n + 1) * lanes) for n in range(chunks))
    ] + [pltpu.make_async_copy(metric, own, sems.at[chunks])]
    for copy in copies:
        copy.start()
    for n in range(chunks):
        copies[n].wait()

        def step(m, carry):
            m = n * (lanes // block) + m
            cut = pl.ds(pl.multiple_of(m * block, block), block)
            keep = survive[0, 0, m].astype(F32)
            turned[:, :, cut] = jnp.swapaxes(held[:, :, cut].astype(F32) * keep, 0, 1).astype(BF)
            return carry

        lax.fori_loop(0, lanes // block, step, 0, unroll=True)
    copies[chunks].wait()
    group = outs[0].shape[0]
    for k in range(RING):
        first = lax.rem(at[0] + k, RING) * group
        outs[k][:, :, :ao] = turned[pl.ds(first, group)]
        outs[k][:, :, ao:] = jnp.broadcast_to(own[...][None], (group,) + metric.shape)


def screen(survive, half, metric):
    aux, occ, ao = half.shape
    out = jax.ShapeDtypeStruct((occ // RING, aux, ao + metric.shape[1]), BF)
    in_hbm = pl.BlockSpec(memory_space=pltpu.HBM)
    return pl.pallas_call(
        screen_body,
        out_shape=[out] * RING,
        in_specs=[scalars(), in_hbm, in_hbm],
        out_specs=[whole()] * RING,
        scratch_shapes=[
            pltpu.VMEM(half.shape, BF),
            pltpu.VMEM(metric.shape, BF),
            pltpu.VMEM((occ, aux, ao), BF),
            pltpu.SemaphoreType.DMA((5,)),
        ],
        compiler_params=params(50),
        cost_estimate=cost(half.size, half.size * 4),
        name="screen",
    )(survive, half, metric)


def fit_body(*refs):
    at = position()
    pieces, (bulk, rest, turned, mixed, fresh) = refs[:8], refs[8:]
    step = pl.program_id(0)
    ao = fresh.shape[1]
    aux = mixed.shape[0]
    part = aux // 8

    @pl.when(step == 0)
    def _():
        metric = jnp.concatenate([p[0][:, ao:] for p in pieces], axis=0)
        source = lax.broadcasted_iota(jnp.int32, (aux, aux), 0)
        n = lax.broadcasted_iota(jnp.int32, (aux, aux), 1)
        slot = n // part
        up = lax.rem(at[0] - slot // 2 + RING, RING)
        core = jnp.where(slot % 2 == 0, at[1], 1 - at[1])
        wanted = (up * 2 + core) * part + n % part
        pick = jnp.where(source == wanted, 1.0, 0.0).astype(BF)
        mixed[...] = jnp.dot(metric, pick, preferred_element_type=F32).astype(BF)

    screened = jnp.concatenate([p[0][:, :ao] for p in pieces], axis=0)
    fitted = jnp.dot(mixed[...], screened, preferred_element_type=F32).astype(BF)
    fresh[...] = fitted
    wide, narrow = bulk.shape[1] // RING, rest.shape[1] // RING
    for n in range(RING):
        column = n * (ao // RING) + at[1] * (wide + narrow)
        bulk[:, n * wide:(n + 1) * wide] = fresh[:, pl.ds(pl.multiple_of(column, 128), wide)]
        column = lax.rem(at[0] + ORDER[n], RING) * (ao // RING) + at[1] * (wide + narrow) + wide
        rest[:, n * narrow:(n + 1) * narrow] = fresh[:, pl.ds(pl.multiple_of(column, 128), narrow)]
    flipped = fitted.T
    cut = pl.ds(pl.multiple_of(step * aux, aux), aux)
    high = ao // (RING * RING)
    for x in range(RING):
        for y in range(RING):
            n = x * RING + y
            to = jnp.where(at[1] == 0, n, y * RING + x) * high
            turned[pl.ds(pl.multiple_of(to, 64), high), cut] = flipped[n * high:(n + 1) * high]


def fit(pieces):
    group, part, wide = pieces[0].shape
    aux = part * 8
    ao = wide - aux
    piece = pl.BlockSpec((1, part, wide), lambda i: (i, 0, 0))
    return pl.pallas_call(
        fit_body,
        grid=(group,),
        out_shape=[jax.ShapeDtypeStruct((group * aux, n), BF) for n in (ao // 3, ao // 6)]
        + [jax.ShapeDtypeStruct((ao, group * aux), BF)],
        in_specs=[piece] * 8,
        out_specs=[pl.BlockSpec((aux, n), lambda i: (i, 0)) for n in (ao // 3, ao // 6)]
        + [pl.BlockSpec((ao, group * aux), lambda i: (0, 0))],
        scratch_shapes=[pltpu.VMEM((aux, aux), BF), pltpu.VMEM((aux, ao), BF)],
        compiler_params=params(28),
        cost_estimate=cost(2 * group * aux * aux * ao, group * aux * ao * 6),
    )(*pieces)


def exponent(top):
    return jnp.floor(14.9 - jnp.log2(jnp.maximum(top, 1e-30)))


def coded(v, e):
    return jnp.round(v * jnp.exp2(e)).astype(jnp.int32).astype(I16)


def marked(e):
    return jnp.broadcast_to(e, (TAIL, e.shape[1])).astype(jnp.int32).astype(I16)


def scale_of(tail):
    return jnp.exp2(-tail.astype(jnp.int32).astype(F32)[:1])


def plain(q):
    return q.astype(jnp.int32).astype(F32)


def write(out, first, block):
    if out.dtype == F32:
        out[first:first + block.shape[0], :] = block
    else:
        e = exponent(jnp.max(jnp.abs(block), axis=0, keepdims=True))
        end = first + block.shape[0]
        out[first:end, :] = coded(block, e)
        out[end:end + TAIL, :] = marked(e)


def bulk_body(shift, bulk, turned, out):
    at = position()
    total = turned.shape[0] // RING
    g = lax.rem(jnp.where(at[1] == 0, at[2], at[3]) + shift, RING)
    left = turned[pl.ds(pl.multiple_of(g * total, 256), total), :]
    half = bulk.shape[1] // 2
    for n in range(2):
        lanes = slice(n * half, (n + 1) * half)
        write(out.at[:, lanes], 0, jnp.dot(left, bulk[:, lanes], preferred_element_type=F32))


def bulk_k(bulk, turned, shift):
    depth, columns = bulk.shape
    total = turned.shape[0] // RING
    shape = (total + (TAIL if shift else 0), columns)
    return pl.pallas_call(
        functools.partial(bulk_body, shift),
        out_shape=jax.ShapeDtypeStruct(shape, I16 if shift else F32),
        in_specs=[whole(), whole()],
        out_specs=whole(),
        compiler_params=params(28),
        cost_estimate=cost(2 * depth * total * columns, total * columns * 2),
    )(bulk, turned)


def rest_body(rest, turned, *outs):
    both = jnp.dot(turned[...], rest[...], preferred_element_type=F32)
    narrow = both.shape[1] // 2
    write(outs[0], 0, both[:, :narrow])
    write(outs[1], 0, both[:, narrow:])


def rest_k(rest, turned, pair):
    depth = rest.shape[0]
    ao = turned.shape[0]
    total, narrow = ao // RING, rest.shape[1] // RING
    each = [total + (TAIL if k else 0) for k in ORDER[2 * pair:2 * pair + 2]]
    return pl.pallas_call(
        rest_body,
        grid=(RING,),
        out_shape=[jax.ShapeDtypeStruct((RING * n, narrow), I16 if n > total else F32) for n in each],
        in_specs=[
            pl.BlockSpec((depth, 2 * narrow), lambda g: (0, pair)),
            pl.BlockSpec((total, depth), lambda g: (g, 0)),
        ],
        out_specs=[pl.BlockSpec((n, narrow), lambda g: (g, 0)) for n in each],
        compiler_params=params(28),
        cost_estimate=cost(4 * depth * ao * narrow, ao * narrow * 4),
    )(rest, turned)


def gathered(own, arrived, first, tail, row, lanes):
    v = own[pl.ds(pl.multiple_of(first[0] + row, 64), first[2]), lanes]
    for m in arrived:
        cut = pl.ds(pl.multiple_of(first[1] + row, 16), first[2])
        v = v + plain(m[cut, lanes]) * scale_of(m[tail:tail + TAIL, lanes])
    return v


def second_body(groups, own, a, b, d, after, kept, *outs):
    at = position()
    high = kept.shape[0]
    total = own.shape[0] // groups
    h = jnp.where(at[1] == 0, at[3], at[2])
    step = own.shape[1] if groups > 1 else 256
    for k in range(RING):
        row = lax.rem(h + k, RING) * high
        out = kept if k == 0 else outs[k - 1]
        for n in range(groups):
            start = n * (total + TAIL)
            for lane in range(0, own.shape[1], step):
                v = gathered(
                    own, (a, b, d), (n * total, start, high), start + total, row, slice(lane, lane + step)
                )
                to = n * own.shape[1] + lane
                write(out.at[:, to:to + step], 0, v)


def second(parts, groups, after):
    total, columns = parts[0].shape
    high, every = total // groups // RING, columns * groups
    return list(pl.pallas_call(
        functools.partial(second_body, groups),
        out_shape=[jax.ShapeDtypeStruct((high, every), F32)]
        + [jax.ShapeDtypeStruct((high + TAIL, every), I16)] * 3,
        in_specs=[whole()] * 5,
        out_specs=[whole()] * 4,
        compiler_params=params(24),
        cost_estimate=cost(total * columns * 16, total * columns * 10),
        name="second_sum",
    )(*parts, after))


def third_body(by_z, own, a, b, d, after, *outs):
    at = position()
    high, step = outs[0].shape
    start = at[0] if by_z else jnp.where(at[1] == 0, at[2], at[3])
    for k in range(RING):
        cut = pl.ds(pl.multiple_of(lax.rem(start + k, RING) * step, 128), step)
        write(outs[k], 0, gathered(own, (a, b, d), (0, 0, high), high, 0, cut))


def third(parts, by_z, after):
    high, every = parts[0].shape
    wide = every // RING
    return list(pl.pallas_call(
        functools.partial(third_body, by_z),
        out_shape=[jax.ShapeDtypeStruct((high, wide), F32)] + [jax.ShapeDtypeStruct((high + TAIL, wide), I16)] * 3,
        in_specs=[whole()] * 5,
        out_specs=[whole()] * 4,
        compiler_params=params(16),
        cost_estimate=cost(high * every * 16, high * every * 10),
        name="third_sum",
    )(*parts, after))


def tick_body(v, out):
    out[...] = v[...]


def tick(v):
    return pl.pallas_call(
        tick_body,
        out_shape=jax.ShapeDtypeStruct(v.shape, v.dtype),
        in_specs=[whole()],
        out_specs=whole(),
        compiler_params=params(1),
        cost_estimate=cost(1000, 32),
        name="tick",
    )(v)


def finish_body(own, a, b, d, rest, ra, rb, rd, out):
    high, wide = own.shape
    for first, v, arrived in ((0, own[...], (a, b, d)), (wide, rest[...], (ra, rb, rd))):
        for m in arrived:
            v = v + plain(m[:high, :]) * scale_of(m[high:, :])
        out[:, first:first + v.shape[1]] = v


def finish(bulk, rest):
    high = bulk[0].shape[0]
    ao = bulk[0].shape[1] + rest[0].shape[1]
    return pl.pallas_call(
        finish_body,
        out_shape=jax.ShapeDtypeStruct((high, ao), F32),
        in_specs=[whole()] * 8,
        out_specs=whole(),
        compiler_params=params(8),
        cost_estimate=cost(high * ao * 8, high * ao * 14),
    )(*bulk, *rest)


def shards(half, metric, survive):
    parts = screen(survive, half, metric)
    here = [parts[0]] + [None] * 3
    for k in (2, 1, 3):
        here[k] = send(parts[k], along_z(k))
    there = [send(v, other_core) for v in here]
    bulk_rows, rest_rows, turned = fit([v for pair in zip(here, there) for v in pair])

    bulk, rest = [None] * 4, [None] * 4

    def bulk_step(k):
        bulk[k] = bulk_k(bulk_rows, turned, k)
        if k:
            bulk[k] = send(bulk[k], first_axis(k))

    def rest_step(pair):
        out = rest_k(rest_rows, turned, pair)
        for k, v in zip(ORDER[2 * pair:2 * pair + 2], out):
            rest[k] = send(v, along_z(k)) if k else v

    def onward(parts, shift):
        for k in ORDER[:3]:
            parts[k] = send(parts[k], shift(k))

    rest_step(0)
    bulk_step(2)
    rest_step(1)
    bulk_step(1)
    bulk_step(3)
    bulk_step(0)
    rest = second(rest, RING, metric)
    onward(rest, second_axis)
    then = tick(metric)
    bulk = second(bulk, 1, then)
    onward(bulk, second_axis)
    rest = third(rest, False, metric)
    onward(rest, first_axis)
    then = tick(then)
    bulk = third(bulk, True, then)
    onward(bulk, along_z)
    return finish(bulk, rest)


def solution(mesh):
    finer = Mesh(mesh.devices.reshape(4, 2, 4, 4), AXES)
    placed = (P(("z", "c"), ("x", "y"), None), P(("z", "c"), None), P(("z", "c"), ("x", "y"), None))
    return jax.shard_map(
        shards, mesh=finer, in_specs=placed, out_specs=P(("x", "y"), ("z", "c")), check_vma=False
    )
```

```python
import functools

import jax
import jax.numpy as jnp
from jax import lax
from jax.experimental import pallas as pl
from jax.experimental.pallas import tpu as pltpu
from jax.sharding import Mesh
from jax.sharding import PartitionSpec as P


AXES = ("z", "c", "x", "y")
BF = jnp.bfloat16
F32 = jnp.float32
I16 = jnp.int16
MIB = 1 << 20
RING = 4
ORDER = (2, 1, 3, 0)
TAIL = 16


def whole():
    return pl.BlockSpec(memory_space=pltpu.VMEM)


def scalars():
    return pl.BlockSpec(memory_space=pltpu.SMEM)


def position():
    return [lax.axis_index(a) for a in AXES]


def params(mib):
    return pltpu.CompilerParams(vmem_limit_bytes=mib * MIB)


def cost(flops, moved):
    return pl.CostEstimate(flops=flops, bytes_accessed=moved, transcendentals=0)


def place(z, c, x, y):
    return ((z % 4) * 2 + c) * 16 + (x % 4) * 4 + y % 4


def moves(shift):
    every = [(z, c, x, y) for z in range(4) for c in range(2) for x in range(4) for y in range(4)]
    return [(place(*d), place(*shift(*d))) for d in every]


def send(v, shift):
    return lax.ppermute(v, AXES, moves(shift))


def along_z(k):
    return lambda z, c, x, y: (z + k, c, x, y)


def other_core(z, c, x, y):
    return (z, 1 - c, x, y)


def first_axis(k):
    return lambda z, c, x, y: (z, c, x + k, y) if c == 0 else (z, c, x, y + k)


def second_axis(k):
    return lambda z, c, x, y: (z, c, x, y + k) if c == 0 else (z, c, x + k, y)


def screen_body(survive, half, *rest):
    outs, (held, turned, sems) = rest[:4], rest[4:]
    at = position()
    ao = half.shape[2]
    block = ao // survive.shape[2]
    chunks = sems.shape[0]
    lanes = ao // chunks
    copies = [
        pltpu.make_async_copy(half.at[:, :, cut], held.at[:, :, cut], sems.at[n])
        for n, cut in enumerate(slice(n * lanes, (n + 1) * lanes) for n in range(chunks))
    ]
    for copy in copies:
        copy.start()
    for n in range(chunks):
        copies[n].wait()

        def step(m, carry):
            m = n * (lanes // block) + m
            cut = pl.ds(pl.multiple_of(m * block, block), block)
            keep = survive[0, 0, m].astype(F32)
            turned[:, :, cut] = jnp.swapaxes(held[:, :, cut].astype(F32) * keep, 0, 1).astype(BF)
            return carry

        lax.fori_loop(0, lanes // block, step, 0, unroll=True)
    group = outs[0].shape[0]
    for k in range(RING):
        first = lax.rem(at[0] + k, RING) * group
        outs[k][...] = turned[pl.ds(first, group)]


def screen(survive, half):
    aux, occ, ao = half.shape
    out = jax.ShapeDtypeStruct((occ // RING, aux, ao), BF)
    in_hbm = pl.BlockSpec(memory_space=pltpu.HBM)
    return pl.pallas_call(
        screen_body,
        out_shape=[out] * RING,
        in_specs=[scalars(), in_hbm],
        out_specs=[whole()] * RING,
        scratch_shapes=[
            pltpu.VMEM(half.shape, BF),
            pltpu.VMEM((occ, aux, ao), BF),
            pltpu.SemaphoreType.DMA((4,)),
        ],
        compiler_params=params(50),
        cost_estimate=cost(half.size, half.size * 4),
        name="screen",
    )(survive, half)


def join_body(*refs):
    metrics, mixed = refs[:4], refs[4]
    at = position()
    aux = mixed.shape[0]
    part = aux // 8
    metric = jnp.concatenate([m[...] for m in metrics], axis=0)
    source = lax.broadcasted_iota(jnp.int32, (aux, aux), 0)
    n = lax.broadcasted_iota(jnp.int32, (aux, aux), 1)
    slot = n // part
    up = lax.rem(at[0] - slot // 2 + RING, RING)
    core = jnp.where(slot % 2 == 0, at[1], 1 - at[1])
    wanted = (up * 2 + core) * part + n % part
    pick = jnp.where(source == wanted, 1.0, 0.0).astype(BF)
    mixed[...] = jnp.dot(metric, pick, preferred_element_type=F32).astype(BF)


def join(metrics):
    aux = metrics[0].shape[1]
    return pl.pallas_call(
        join_body,
        out_shape=jax.ShapeDtypeStruct((aux, aux), BF),
        in_specs=[whole()] * 4,
        out_specs=whole(),
        compiler_params=params(4),
        cost_estimate=cost(2 * aux**3, aux * aux * 4),
        name="join",
    )(*metrics)


def fit_body(*refs):
    pieces, mixed, (bulk, rest, turned, fresh) = refs[:8], refs[8], refs[9:]
    at = position()
    step = pl.program_id(0)
    ao = fresh.shape[1]
    aux = mixed.shape[0]
    screened = jnp.concatenate([p[0] for p in pieces], axis=0)
    fitted = jnp.dot(mixed[...], screened, preferred_element_type=F32).astype(BF)
    fresh[...] = fitted
    wide, narrow = bulk.shape[1] // RING, rest.shape[1] // RING
    for n in range(RING):
        column = n * (ao // RING) + at[1] * (wide + narrow)
        bulk[:, n * wide:(n + 1) * wide] = fresh[:, pl.ds(pl.multiple_of(column, 128), wide)]
        column = lax.rem(at[0] + ORDER[n], RING) * (ao // RING) + at[1] * (wide + narrow) + wide
        rest[:, n * narrow:(n + 1) * narrow] = fresh[:, pl.ds(pl.multiple_of(column, 128), narrow)]
    flipped = fitted.T
    cut = pl.ds(pl.multiple_of(step * aux, aux), aux)
    high = ao // (RING * RING)
    for x in range(RING):
        for y in range(RING):
            n = x * RING + y
            to = jnp.where(at[1] == 0, n, y * RING + x) * high
            turned[pl.ds(pl.multiple_of(to, 64), high), cut] = flipped[n * high:(n + 1) * high]


def fit(pieces, mixed):
    group, part, ao = pieces[0].shape
    aux = part * 8
    piece = pl.BlockSpec((1, part, ao), lambda i: (i, 0, 0))
    return pl.pallas_call(
        fit_body,
        grid=(group,),
        out_shape=[jax.ShapeDtypeStruct((group * aux, n), BF) for n in (ao // 3, ao // 6)]
        + [jax.ShapeDtypeStruct((ao, group * aux), BF)],
        in_specs=[piece] * 8 + [whole()],
        out_specs=[pl.BlockSpec((aux, n), lambda i: (i, 0)) for n in (ao // 3, ao // 6)]
        + [pl.BlockSpec((ao, group * aux), lambda i: (0, 0))],
        scratch_shapes=[pltpu.VMEM((aux, ao), BF)],
        compiler_params=params(28),
        cost_estimate=cost(2 * group * aux * aux * ao, group * aux * ao * 6),
        name="fit",
    )(*pieces, mixed)


def exponent(top):
    return jnp.floor(14.9 - jnp.log2(jnp.maximum(top, 1e-30)))


def coded(v, e):
    return jnp.round(v * jnp.exp2(e)).astype(jnp.int32).astype(I16)


def marked(e):
    return jnp.broadcast_to(e, (TAIL, e.shape[1])).astype(jnp.int32).astype(I16)


def scale_of(tail):
    return jnp.exp2(-tail.astype(jnp.int32).astype(F32)[:1])


def plain(q):
    return q.astype(jnp.int32).astype(F32)


def write(out, first, block):
    if out.dtype == F32:
        out[first:first + block.shape[0], :] = block
    else:
        e = exponent(jnp.max(jnp.abs(block), axis=0, keepdims=True))
        end = first + block.shape[0]
        out[first:end, :] = coded(block, e)
        out[end:end + TAIL, :] = marked(e)


def bulk_body(shift, bulk, turned, out):
    at = position()
    total = turned.shape[0] // RING
    g = lax.rem(jnp.where(at[1] == 0, at[2], at[3]) + shift, RING)
    left = turned[pl.ds(pl.multiple_of(g * total, 256), total), :]
    half = bulk.shape[1] // 2
    for n in range(2):
        lanes = slice(n * half, (n + 1) * half)
        write(out.at[:, lanes], 0, jnp.dot(left, bulk[:, lanes], preferred_element_type=F32))


def bulk_k(bulk, turned, shift):
    depth, columns = bulk.shape
    total = turned.shape[0] // RING
    shape = (total + (TAIL if shift else 0), columns)
    return pl.pallas_call(
        functools.partial(bulk_body, shift),
        out_shape=jax.ShapeDtypeStruct(shape, I16 if shift else F32),
        in_specs=[whole(), whole()],
        out_specs=whole(),
        compiler_params=params(28),
        cost_estimate=cost(2 * depth * total * columns, total * columns * 2),
    )(bulk, turned)


def rest_body(first, rest, turned, *outs):
    narrow = rest.shape[1] // RING
    total = turned.shape[0] // RING
    right = rest[:, first * narrow:(first + len(outs)) * narrow]
    for g in range(RING):
        block = jnp.dot(turned[g * total:(g + 1) * total, :], right, preferred_element_type=F32)
        for n, out in enumerate(outs):
            write(out, g * (out.shape[0] // RING), block[:, n * narrow:(n + 1) * narrow])


def rest_k(rest, turned, first, last):
    depth = rest.shape[0]
    ao = turned.shape[0]
    narrow = rest.shape[1] // RING
    shifts = ORDER[first:last]
    return pl.pallas_call(
        functools.partial(rest_body, first),
        out_shape=[
            jax.ShapeDtypeStruct((ao + (RING * TAIL if k else 0), narrow), I16 if k else F32) for k in shifts
        ],
        in_specs=[whole()] * 2,
        out_specs=[whole()] * len(shifts),
        compiler_params=params(28),
        cost_estimate=cost(2 * len(shifts) * depth * ao * narrow, ao * narrow * 4),
    )(rest, turned)


def gathered(own, arrived, first, tail, row, lanes):
    v = own[pl.ds(pl.multiple_of(first[0] + row, 64), first[2]), lanes]
    for m in arrived:
        cut = pl.ds(pl.multiple_of(first[1] + row, 16), first[2])
        v = v + plain(m[cut, lanes]) * scale_of(m[tail:tail + TAIL, lanes])
    return v


def second_body(groups, own, a, b, d, after, kept, *outs):
    at = position()
    high = kept.shape[0]
    total = own.shape[0] // groups
    h = jnp.where(at[1] == 0, at[3], at[2])
    step = own.shape[1] if groups > 1 else 256
    for k in range(RING):
        row = lax.rem(h + k, RING) * high
        out = kept if k == 0 else outs[k - 1]
        for n in range(groups):
            start = n * (total + TAIL)
            for lane in range(0, own.shape[1], step):
                v = gathered(
                    own, (a, b, d), (n * total, start, high), start + total, row, slice(lane, lane + step)
                )
                to = n * own.shape[1] + lane
                write(out.at[:, to:to + step], 0, v)


def second(parts, groups, after):
    total, columns = parts[0].shape
    high, every = total // groups // RING, columns * groups
    return list(pl.pallas_call(
        functools.partial(second_body, groups),
        out_shape=[jax.ShapeDtypeStruct((high, every), F32)]
        + [jax.ShapeDtypeStruct((high + TAIL, every), I16)] * 3,
        in_specs=[whole()] * 5,
        out_specs=[whole()] * 4,
        compiler_params=params(24),
        cost_estimate=cost(total * columns * 16, total * columns * 10),
        name="second_sum",
    )(*parts, after))


def third_body(by_z, own, a, b, d, after, *outs):
    at = position()
    high, step = outs[0].shape
    start = at[0] if by_z else jnp.where(at[1] == 0, at[2], at[3])
    for k in range(RING):
        cut = pl.ds(pl.multiple_of(lax.rem(start + k, RING) * step, 128), step)
        write(outs[k], 0, gathered(own, (a, b, d), (0, 0, high), high, 0, cut))


def third(parts, by_z, after):
    high, every = parts[0].shape
    wide = every // RING
    return list(pl.pallas_call(
        functools.partial(third_body, by_z),
        out_shape=[jax.ShapeDtypeStruct((high, wide), F32)] + [jax.ShapeDtypeStruct((high + TAIL, wide), I16)] * 3,
        in_specs=[whole()] * 5,
        out_specs=[whole()] * 4,
        compiler_params=params(16),
        cost_estimate=cost(high * every * 16, high * every * 10),
        name="third_sum",
    )(*parts, after))


def tick_body(v, out):
    out[...] = v[...]


def tick(v):
    return pl.pallas_call(
        tick_body,
        out_shape=jax.ShapeDtypeStruct(v.shape, v.dtype),
        in_specs=[whole()],
        out_specs=whole(),
        compiler_params=params(1),
        cost_estimate=cost(1000, 32),
        name="tick",
    )(v)


def finish_body(own, a, b, d, rest, ra, rb, rd, out):
    high, wide = own.shape
    for first, v, arrived in ((0, own[...], (a, b, d)), (wide, rest[...], (ra, rb, rd))):
        for m in arrived:
            v = v + plain(m[:high, :]) * scale_of(m[high:, :])
        out[:, first:first + v.shape[1]] = v


def finish(bulk, rest):
    high = bulk[0].shape[0]
    ao = bulk[0].shape[1] + rest[0].shape[1]
    return pl.pallas_call(
        finish_body,
        out_shape=jax.ShapeDtypeStruct((high, ao), F32),
        in_specs=[whole()] * 8,
        out_specs=whole(),
        compiler_params=params(8),
        cost_estimate=cost(high * ao * 8, high * ao * 14),
    )(*bulk, *rest)


def shards(half, metric, survive):
    parts = screen(survive, half)
    here = [parts[0]] + [None] * 3
    for k in ORDER[:3]:
        here[k] = send(parts[k], along_z(k))
    pair = jnp.concatenate([metric, send(metric, other_core)], axis=0)
    metrics = [pair] + [None] * 3
    for k in ORDER[:3]:
        metrics[k] = send(pair, along_z(k))
    mixed = join(metrics)
    there = [send(v, other_core) for v in here]
    bulk_rows, rest_rows, turned = fit([v for both in zip(here, there) for v in both], mixed)

    bulk, rest = [None] * 4, [None] * 4

    def bulk_step(k):
        bulk[k] = bulk_k(bulk_rows, turned, k)
        if k:
            bulk[k] = send(bulk[k], first_axis(k))

    def rest_step(first, last):
        out = rest_k(rest_rows, turned, first, last)
        for k, v in zip(ORDER[first:last], out):
            rest[k] = send(v, along_z(k)) if k else v

    def onward(parts, shift):
        for k in ORDER[:3]:
            parts[k] = send(parts[k], shift(k))

    rest_step(0, 1)
    bulk_step(2)
    rest_step(1, 3)
    bulk_step(1)
    bulk_step(3)
    rest_step(3, 4)
    bulk_step(0)
    rest = second(rest, RING, metric)
    onward(rest, second_axis)
    then = tick(metric)
    bulk = second(bulk, 1, then)
    onward(bulk, second_axis)
    rest = third(rest, False, metric)
    onward(rest, first_axis)
    then = tick(then)
    bulk = third(bulk, True, then)
    onward(bulk, along_z)
    return finish(bulk, rest)


def solution(mesh):
    finer = Mesh(mesh.devices.reshape(4, 2, 4, 4), AXES)
    placed = (P(("z", "c"), ("x", "y"), None), P(("z", "c"), None), P(("z", "c"), ("x", "y"), None))
    return jax.shard_map(
        shards, mesh=finer, in_specs=placed, out_specs=P(("x", "y"), ("z", "c")), check_vma=False
    )
```

```python
import functools

import jax
import jax.numpy as jnp
from jax import lax
from jax.experimental import pallas as pl
from jax.experimental.pallas import tpu as pltpu
from jax.sharding import Mesh
from jax.sharding import PartitionSpec as P


AXES = ("z", "c", "x", "y")
BF = jnp.bfloat16
F32 = jnp.float32
I16 = jnp.int16
MIB = 1 << 20
RING = 4
ORDER = (2, 1, 3, 0)
TAIL = 16


def whole():
    return pl.BlockSpec(memory_space=pltpu.VMEM)


def scalars():
    return pl.BlockSpec(memory_space=pltpu.SMEM)


def position():
    return [lax.axis_index(a) for a in AXES]


def params(mib):
    return pltpu.CompilerParams(vmem_limit_bytes=mib * MIB)


def cost(flops, moved):
    return pl.CostEstimate(flops=flops, bytes_accessed=moved, transcendentals=0)


def place(z, c, x, y):
    return ((z % 4) * 2 + c) * 16 + (x % 4) * 4 + y % 4


def moves(shift):
    every = [(z, c, x, y) for z in range(4) for c in range(2) for x in range(4) for y in range(4)]
    return [(place(*d), place(*shift(*d))) for d in every]


def send(v, shift):
    return lax.ppermute(v, AXES, moves(shift))


def along_z(k):
    return lambda z, c, x, y: (z + k, c, x, y)


def other_core(z, c, x, y):
    return (z, 1 - c, x, y)


def first_axis(k):
    return lambda z, c, x, y: (z, c, x + k, y) if c == 0 else (z, c, x, y + k)


def second_axis(k):
    return lambda z, c, x, y: (z, c, x, y + k) if c == 0 else (z, c, x + k, y)


def screen_body(survive, half, *rest):
    outs, (held, turned, sems) = rest[:4], rest[4:]
    at = position()
    ao = half.shape[2]
    block = ao // survive.shape[2]
    chunks = sems.shape[0]
    lanes = ao // chunks
    copies = [
        pltpu.make_async_copy(half.at[:, :, cut], held.at[:, :, cut], sems.at[n])
        for n, cut in enumerate(slice(n * lanes, (n + 1) * lanes) for n in range(chunks))
    ]
    for copy in copies:
        copy.start()
    for n in range(chunks):
        copies[n].wait()

        def step(m, carry):
            m = n * (lanes // block) + m
            cut = pl.ds(pl.multiple_of(m * block, block), block)
            keep = survive[0, 0, m].astype(F32)
            turned[:, :, cut] = jnp.swapaxes(held[:, :, cut].astype(F32) * keep, 0, 1).astype(BF)
            return carry

        lax.fori_loop(0, lanes // block, step, 0, unroll=True)
    group = outs[0].shape[0]
    for k in range(RING):
        first = lax.rem(at[0] + k, RING) * group
        outs[k][...] = turned[pl.ds(first, group)]


def screen(survive, half):
    aux, occ, ao = half.shape
    out = jax.ShapeDtypeStruct((occ // RING, aux, ao), BF)
    in_hbm = pl.BlockSpec(memory_space=pltpu.HBM)
    return pl.pallas_call(
        screen_body,
        out_shape=[out] * RING,
        in_specs=[scalars(), in_hbm],
        out_specs=[whole()] * RING,
        scratch_shapes=[
            pltpu.VMEM(half.shape, BF),
            pltpu.VMEM((occ, aux, ao), BF),
            pltpu.SemaphoreType.DMA((4,)),
        ],
        compiler_params=params(50),
        cost_estimate=cost(half.size, half.size * 4),
        name="screen",
    )(survive, half)


def join_body(*refs):
    metrics, mixed = refs[:4], refs[4]
    at = position()
    aux = mixed.shape[0]
    part = aux // 8
    metric = jnp.concatenate([m[...] for m in metrics], axis=0)
    source = lax.broadcasted_iota(jnp.int32, (aux, aux), 0)
    n = lax.broadcasted_iota(jnp.int32, (aux, aux), 1)
    slot = n // part
    up = lax.rem(at[0] - slot // 2 + RING, RING)
    core = jnp.where(slot % 2 == 0, at[1], 1 - at[1])
    wanted = (up * 2 + core) * part + n % part
    pick = jnp.where(source == wanted, 1.0, 0.0).astype(BF)
    mixed[...] = jnp.dot(metric, pick, preferred_element_type=F32).astype(BF)


def join(metrics):
    aux = metrics[0].shape[1]
    return pl.pallas_call(
        join_body,
        out_shape=jax.ShapeDtypeStruct((aux, aux), BF),
        in_specs=[whole()] * 4,
        out_specs=whole(),
        compiler_params=params(4),
        cost_estimate=cost(2 * aux**3, aux * aux * 4),
        name="join",
    )(*metrics)


def fit_body(*refs):
    pieces, mixed, (bulk, rest, turned, fresh) = refs[:8], refs[8], refs[9:]
    at = position()
    step = pl.program_id(0)
    ao = fresh.shape[1]
    aux = mixed.shape[0]
    screened = jnp.concatenate([p[0] for p in pieces], axis=0)
    fitted = jnp.dot(mixed[...], screened, preferred_element_type=F32).astype(BF)
    fresh[...] = fitted
    wide, narrow = bulk.shape[1] // RING, rest.shape[1] // RING
    for n in range(RING):
        column = n * (ao // RING) + at[1] * (wide + narrow)
        bulk[:, n * wide:(n + 1) * wide] = fresh[:, pl.ds(pl.multiple_of(column, 128), wide)]
        column = lax.rem(at[0] + ORDER[n], RING) * (ao // RING) + at[1] * (wide + narrow) + wide
        rest[:, n * narrow:(n + 1) * narrow] = fresh[:, pl.ds(pl.multiple_of(column, 128), narrow)]
    flipped = fitted.T
    cut = pl.ds(pl.multiple_of(step * aux, aux), aux)
    high = ao // (RING * RING)
    for x in range(RING):
        for y in range(RING):
            n = x * RING + y
            to = jnp.where(at[1] == 0, n, y * RING + x) * high
            turned[pl.ds(pl.multiple_of(to, 64), high), cut] = flipped[n * high:(n + 1) * high]


def fit(pieces, mixed):
    group, part, ao = pieces[0].shape
    aux = part * 8
    piece = pl.BlockSpec((1, part, ao), lambda i: (i, 0, 0))
    return pl.pallas_call(
        fit_body,
        grid=(group,),
        out_shape=[jax.ShapeDtypeStruct((group * aux, n), BF) for n in (ao // 3, ao // 6)]
        + [jax.ShapeDtypeStruct((ao, group * aux), BF)],
        in_specs=[piece] * 8 + [whole()],
        out_specs=[pl.BlockSpec((aux, n), lambda i: (i, 0)) for n in (ao // 3, ao // 6)]
        + [pl.BlockSpec((ao, group * aux), lambda i: (0, 0))],
        scratch_shapes=[pltpu.VMEM((aux, ao), BF)],
        compiler_params=params(28),
        cost_estimate=cost(2 * group * aux * aux * ao, group * aux * ao * 6),
        name="fit",
    )(*pieces, mixed)


def exponent(top):
    return jnp.floor(14.9 - jnp.log2(jnp.maximum(top, 1e-30)))


def coded(v, e):
    return jnp.round(v * jnp.exp2(e)).astype(jnp.int32).astype(I16)


def marked(e):
    return jnp.broadcast_to(e, (TAIL, e.shape[1])).astype(jnp.int32).astype(I16)


def scale_of(tail):
    return jnp.exp2(-tail.astype(jnp.int32).astype(F32)[:1])


def plain(q):
    return q.astype(jnp.int32).astype(F32)


def write(out, first, block):
    if out.dtype == F32:
        out[first:first + block.shape[0], :] = block
    else:
        e = exponent(jnp.max(jnp.abs(block), axis=0, keepdims=True))
        end = first + block.shape[0]
        out[first:end, :] = coded(block, e)
        out[end:end + TAIL, :] = marked(e)


def bulk_body(blocks, bulk, turned, *refs):
    at = position()
    total = turned.shape[0] // RING
    own = jnp.where(at[1] == 0, at[2], at[3])
    outs = refs[len(refs) - len(blocks):]
    arrived = iter(refs)
    wide = bulk.shape[1] // 2
    for (shift, half, adds), out in zip(blocks, outs):
        rows = total if half is None else total // 2
        first = lax.rem(own + shift, RING) * total + (0 if half is None else half * rows)
        left = turned[pl.ds(pl.multiple_of(first, 128), rows), :]
        part = next(arrived) if adds else None
        for n in range(2):
            lanes = slice(n * wide, (n + 1) * wide)
            block = jnp.dot(left, bulk[:, lanes], preferred_element_type=F32)
            if adds:
                block = block + plain(part[:rows, lanes]) * scale_of(part[rows:, lanes])
            write(out.at[:, lanes], 0, block)


def bulk_k(bulk, turned, blocks, arrived=()):
    depth, columns = bulk.shape
    total = turned.shape[0] // RING
    sizes = [total if half is None else total // 2 for _, half, _ in blocks]
    return pl.pallas_call(
        functools.partial(bulk_body, blocks),
        out_shape=[
            jax.ShapeDtypeStruct((n + (TAIL if shift else 0), columns), I16 if shift else F32)
            for n, (shift, _, _) in zip(sizes, blocks)
        ],
        in_specs=[whole()] * (2 + len(arrived)),
        out_specs=[whole()] * len(blocks),
        compiler_params=params(28),
        cost_estimate=cost(2 * depth * sum(sizes) * columns, sum(sizes) * columns * 2),
    )(bulk, turned, *arrived)


def rest_body(first, rest, turned, *outs):
    narrow = rest.shape[1] // RING
    total = turned.shape[0] // RING
    right = rest[:, first * narrow:(first + len(outs)) * narrow]
    for g in range(RING):
        block = jnp.dot(turned[g * total:(g + 1) * total, :], right, preferred_element_type=F32)
        for n, out in enumerate(outs):
            write(out, g * (out.shape[0] // RING), block[:, n * narrow:(n + 1) * narrow])


def rest_k(rest, turned, first, last):
    depth = rest.shape[0]
    ao = turned.shape[0]
    narrow = rest.shape[1] // RING
    shifts = ORDER[first:last]
    return pl.pallas_call(
        functools.partial(rest_body, first),
        out_shape=[
            jax.ShapeDtypeStruct((ao + (RING * TAIL if k else 0), narrow), I16 if k else F32) for k in shifts
        ],
        in_specs=[whole()] * 2,
        out_specs=[whole()] * len(shifts),
        compiler_params=params(28),
        cost_estimate=cost(2 * len(shifts) * depth * ao * narrow, ao * narrow * 4),
    )(rest, turned)


def gathered(own, arrived, first, tail, row, lanes):
    v = own[pl.ds(pl.multiple_of(first[0] + row, 64), first[2]), lanes]
    for m in arrived:
        cut = pl.ds(pl.multiple_of(first[1] + row, 16), first[2])
        v = v + plain(m[cut, lanes]) * scale_of(m[tail:tail + TAIL, lanes])
    return v


def second_body(groups, own, a, b, d, after, kept, *outs):
    at = position()
    high = kept.shape[0]
    total = own.shape[0] // groups
    h = jnp.where(at[1] == 0, at[3], at[2])
    step = own.shape[1] if groups > 1 else 256
    for k in range(RING):
        row = lax.rem(h + k, RING) * high
        out = kept if k == 0 else outs[k - 1]
        for n in range(groups):
            start = n * (total + TAIL)
            for lane in range(0, own.shape[1], step):
                v = gathered(
                    own, (a, b, d), (n * total, start, high), start + total, row, slice(lane, lane + step)
                )
                to = n * own.shape[1] + lane
                write(out.at[:, to:to + step], 0, v)


def second(parts, groups, after):
    total, columns = parts[0].shape
    high, every = total // groups // RING, columns * groups
    return list(pl.pallas_call(
        functools.partial(second_body, groups),
        out_shape=[jax.ShapeDtypeStruct((high, every), F32)]
        + [jax.ShapeDtypeStruct((high + TAIL, every), I16)] * 3,
        in_specs=[whole()] * 5,
        out_specs=[whole()] * 4,
        compiler_params=params(24),
        cost_estimate=cost(total * columns * 16, total * columns * 10),
        name="second_sum",
    )(*parts, after))


def bulk_second_body(own, a, b, d, e, after, kept, *outs):
    at = position()
    high = kept.shape[0]
    h = jnp.where(at[1] == 0, at[3], at[2])
    half = own.shape[0] // 2
    step = 256
    for k in range(RING):
        block = lax.rem(h + k, RING)
        out = kept if k == 0 else outs[k - 1]

        def part(upper, arrived, block=block, out=out):
            @pl.when((block < RING // 2) == upper)
            def _():
                row = pl.multiple_of(lax.rem(block, RING // 2) * high, 64)
                first = pl.multiple_of(block * high, 64)
                for lane in range(0, own.shape[1], step):
                    lanes = slice(lane, lane + step)
                    v = own[pl.ds(first, high), lanes]
                    for m in arrived:
                        v = v + plain(m[pl.ds(row, high), lanes]) * scale_of(m[half:, lanes])
                    write(out.at[:, lanes], 0, v)

        part(True, (a, b))
        part(False, (d, e))


def bulk_second(own, upper, lower, after):
    total, columns = own.shape
    high = total // RING
    return list(pl.pallas_call(
        bulk_second_body,
        out_shape=[jax.ShapeDtypeStruct((high, columns), F32)]
        + [jax.ShapeDtypeStruct((high + TAIL, columns), I16)] * 3,
        in_specs=[whole()] * 6,
        out_specs=[whole()] * 4,
        compiler_params=params(24),
        cost_estimate=cost(total * columns * 12, total * columns * 8),
        name="bulk_second_sum",
    )(own, *upper, *lower, after))


def third_body(by_z, own, a, b, d, after, *outs):
    at = position()
    high, step = outs[0].shape
    start = at[0] if by_z else jnp.where(at[1] == 0, at[2], at[3])
    for k in range(RING):
        cut = pl.ds(pl.multiple_of(lax.rem(start + k, RING) * step, 128), step)
        write(outs[k], 0, gathered(own, (a, b, d), (0, 0, high), high, 0, cut))


def third(parts, by_z, after):
    high, every = parts[0].shape
    wide = every // RING
    return list(pl.pallas_call(
        functools.partial(third_body, by_z),
        out_shape=[jax.ShapeDtypeStruct((high, wide), F32)] + [jax.ShapeDtypeStruct((high + TAIL, wide), I16)] * 3,
        in_specs=[whole()] * 5,
        out_specs=[whole()] * 4,
        compiler_params=params(16),
        cost_estimate=cost(high * every * 16, high * every * 10),
        name="third_sum",
    )(*parts, after))


def tick_body(v, out):
    out[...] = v[...]


def tick(v):
    return pl.pallas_call(
        tick_body,
        out_shape=jax.ShapeDtypeStruct(v.shape, v.dtype),
        in_specs=[whole()],
        out_specs=whole(),
        compiler_params=params(1),
        cost_estimate=cost(1000, 32),
        name="tick",
    )(v)


def finish_body(own, a, b, d, rest, ra, rb, rd, out):
    high, wide = own.shape
    for first, v, arrived in ((0, own[...], (a, b, d)), (wide, rest[...], (ra, rb, rd))):
        for m in arrived:
            v = v + plain(m[:high, :]) * scale_of(m[high:, :])
        out[:, first:first + v.shape[1]] = v


def finish(bulk, rest):
    high = bulk[0].shape[0]
    ao = bulk[0].shape[1] + rest[0].shape[1]
    return pl.pallas_call(
        finish_body,
        out_shape=jax.ShapeDtypeStruct((high, ao), F32),
        in_specs=[whole()] * 8,
        out_specs=whole(),
        compiler_params=params(8),
        cost_estimate=cost(high * ao * 8, high * ao * 14),
    )(*bulk, *rest)


def shards(half, metric, survive):
    parts = screen(survive, half)
    here = [parts[0]] + [None] * 3
    for k in ORDER[:3]:
        here[k] = send(parts[k], along_z(k))
    pair = jnp.concatenate([metric, send(metric, other_core)], axis=0)
    metrics = [pair] + [None] * 3
    for k in ORDER[:3]:
        metrics[k] = send(pair, along_z(k))
    mixed = join(metrics)
    there = [send(v, other_core) for v in here]
    bulk_rows, rest_rows, turned = fit([v for both in zip(here, there) for v in both], mixed)

    rest = [None] * 4

    def bulk_step(*blocks, arrived=()):
        return bulk_k(bulk_rows, turned, blocks, arrived)

    def near(up, down):
        up = send(up, first_axis(1))
        down = send(down, first_axis(3))
        return up, down

    def rest_step(first, last):
        out = rest_k(rest_rows, turned, first, last)
        for k, v in zip(ORDER[first:last], out):
            rest[k] = send(v, along_z(k)) if k else v

    def onward(parts, shift):
        for k in ORDER[:3]:
            parts[k] = send(parts[k], shift(k))

    far = near(*bulk_step((2, 0, False), (2, 1, False)))
    rest_step(0, 1)
    lower_up, upper_down = near(*bulk_step((1, 1, False), (3, 0, False)))
    rest_step(1, 3)
    upper_up, lower_down = near(*bulk_step((1, 0, True), (3, 1, True), arrived=far))
    rest_step(3, 4)
    own = bulk_step((0, None, False))[0]
    bulk = bulk_second(own, (upper_up, upper_down), (lower_up, lower_down), metric)
    onward(bulk, second_axis)
    then = tick(metric)
    rest = second(rest, RING, then)
    onward(rest, second_axis)
    then = tick(then)
    bulk = third(bulk, True, then)
    onward(bulk, along_z)
    then = tick(then)
    rest = third(rest, False, then)
    onward(rest, first_axis)
    return finish(bulk, rest)


def solution(mesh):
    finer = Mesh(mesh.devices.reshape(4, 2, 4, 4), AXES)
    placed = (P(("z", "c"), ("x", "y"), None), P(("z", "c"), None), P(("z", "c"), ("x", "y"), None))
    return jax.shard_map(
        shards, mesh=finer, in_specs=placed, out_specs=P(("x", "y"), ("z", "c")), check_vma=False
    )
```

```python
import functools

import jax
import jax.numpy as jnp
from jax import lax
from jax.experimental import pallas as pl
from jax.experimental.pallas import tpu as pltpu
from jax.sharding import Mesh
from jax.sharding import PartitionSpec as P


AXES = ("z", "c", "x", "y")
BF = jnp.bfloat16
F32 = jnp.float32
I16 = jnp.int16
MIB = 1 << 20
RING = 4
ORDER = (2, 0, 1, 3)
TAIL = 16


def whole():
    return pl.BlockSpec(memory_space=pltpu.VMEM)


def scalars():
    return pl.BlockSpec(memory_space=pltpu.SMEM)


def position():
    return [lax.axis_index(a) for a in AXES]


def params(mib):
    return pltpu.CompilerParams(vmem_limit_bytes=mib * MIB)


def cost(flops, moved):
    return pl.CostEstimate(flops=flops, bytes_accessed=moved, transcendentals=0)


def place(z, c, x, y):
    return ((z % 4) * 2 + c) * 16 + (x % 4) * 4 + y % 4


def moves(shift):
    every = [(z, c, x, y) for z in range(4) for c in range(2) for x in range(4) for y in range(4)]
    return [(place(*d), place(*shift(*d))) for d in every]


def send(v, shift):
    return lax.ppermute(v, AXES, moves(shift))


def along_z(k):
    return lambda z, c, x, y: (z + k, c, x, y)


def other_core(z, c, x, y):
    return (z, 1 - c, x, y)


def first_axis(k):
    return lambda z, c, x, y: (z, c, x + k, y) if c == 0 else (z, c, x, y + k)


def second_axis(k):
    return lambda z, c, x, y: (z, c, x, y + k) if c == 0 else (z, c, x + k, y)


def screen_body(survive, half, *rest):
    outs, (held, turned, sems) = rest[:4], rest[4:]
    at = position()
    ao = half.shape[2]
    block = ao // survive.shape[2]
    chunks = sems.shape[0]
    lanes = ao // chunks
    copies = [
        pltpu.make_async_copy(half.at[:, :, cut], held.at[:, :, cut], sems.at[n])
        for n, cut in enumerate(slice(n * lanes, (n + 1) * lanes) for n in range(chunks))
    ]
    for copy in copies:
        copy.start()
    for n in range(chunks):
        copies[n].wait()

        def step(m, carry):
            m = n * (lanes // block) + m
            cut = pl.ds(pl.multiple_of(m * block, block), block)
            keep = survive[0, 0, m].astype(F32)
            turned[:, :, cut] = jnp.swapaxes(held[:, :, cut].astype(F32) * keep, 0, 1).astype(BF)
            return carry

        lax.fori_loop(0, lanes // block, step, 0, unroll=True)
    group = outs[0].shape[0]
    for k in range(RING):
        first = lax.rem(at[0] + k, RING) * group
        outs[k][...] = turned[pl.ds(first, group)]


def screen(survive, half):
    aux, occ, ao = half.shape
    out = jax.ShapeDtypeStruct((occ // RING, aux, ao), BF)
    in_hbm = pl.BlockSpec(memory_space=pltpu.HBM)
    return pl.pallas_call(
        screen_body,
        out_shape=[out] * RING,
        in_specs=[scalars(), in_hbm],
        out_specs=[whole()] * RING,
        scratch_shapes=[
            pltpu.VMEM(half.shape, BF),
            pltpu.VMEM((occ, aux, ao), BF),
            pltpu.SemaphoreType.DMA((4,)),
        ],
        compiler_params=params(50),
        cost_estimate=cost(half.size, half.size * 4),
        name="screen",
    )(survive, half)


def join_body(*refs):
    metrics, mixed = refs[:4], refs[4]
    at = position()
    aux = mixed.shape[0]
    part = aux // 8
    metric = jnp.concatenate([m[...] for m in metrics], axis=0)
    source = lax.broadcasted_iota(jnp.int32, (aux, aux), 0)
    n = lax.broadcasted_iota(jnp.int32, (aux, aux), 1)
    slot = n // part
    up = lax.rem(at[0] - slot // 2 + RING, RING)
    core = jnp.where(slot % 2 == 0, at[1], 1 - at[1])
    wanted = (up * 2 + core) * part + n % part
    pick = jnp.where(source == wanted, 1.0, 0.0).astype(BF)
    mixed[...] = jnp.dot(metric, pick, preferred_element_type=F32).astype(BF)


def join(metrics):
    aux = metrics[0].shape[1]
    return pl.pallas_call(
        join_body,
        out_shape=jax.ShapeDtypeStruct((aux, aux), BF),
        in_specs=[whole()] * 4,
        out_specs=whole(),
        compiler_params=params(4),
        cost_estimate=cost(2 * aux**3, aux * aux * 4),
        name="join",
    )(*metrics)


def fit_body(*refs):
    pieces, mixed, (bulk, rest, turned, fresh) = refs[:8], refs[8], refs[9:]
    at = position()
    step = pl.program_id(0)
    ao = fresh.shape[1]
    aux = mixed.shape[0]
    screened = jnp.concatenate([p[0] for p in pieces], axis=0)
    fitted = jnp.dot(mixed[...], screened, preferred_element_type=F32).astype(BF)
    fresh[...] = fitted
    wide, narrow = bulk.shape[1] // RING, rest.shape[1] // RING
    for n in range(RING):
        column = n * (ao // RING) + at[1] * (wide + narrow)
        bulk[:, n * wide:(n + 1) * wide] = fresh[:, pl.ds(pl.multiple_of(column, 128), wide)]
        column = lax.rem(at[0] + ORDER[n], RING) * (ao // RING) + at[1] * (wide + narrow) + wide
        rest[:, n * narrow:(n + 1) * narrow] = fresh[:, pl.ds(pl.multiple_of(column, 128), narrow)]
    flipped = fitted.T
    cut = pl.ds(pl.multiple_of(step * aux, aux), aux)
    high = ao // (RING * RING)
    for x in range(RING):
        for y in range(RING):
            n = x * RING + y
            to = jnp.where(at[1] == 0, n, y * RING + x) * high
            turned[pl.ds(pl.multiple_of(to, 64), high), cut] = flipped[n * high:(n + 1) * high]


def fit(pieces, mixed):
    group, part, ao = pieces[0].shape
    aux = part * 8
    piece = pl.BlockSpec((1, part, ao), lambda i: (i, 0, 0))
    return pl.pallas_call(
        fit_body,
        grid=(group,),
        out_shape=[jax.ShapeDtypeStruct((group * aux, n), BF) for n in (ao // 3, ao // 6)]
        + [jax.ShapeDtypeStruct((ao, group * aux), BF)],
        in_specs=[piece] * 8 + [whole()],
        out_specs=[pl.BlockSpec((aux, n), lambda i: (i, 0)) for n in (ao // 3, ao // 6)]
        + [pl.BlockSpec((ao, group * aux), lambda i: (0, 0))],
        scratch_shapes=[pltpu.VMEM((aux, ao), BF)],
        compiler_params=params(28),
        cost_estimate=cost(2 * group * aux * aux * ao, group * aux * ao * 6),
        name="fit",
    )(*pieces, mixed)


def exponent(top):
    return jnp.floor(14.9 - jnp.log2(jnp.maximum(top, 1e-30)))


def coded(v, e):
    return jnp.round(v * jnp.exp2(e)).astype(jnp.int32).astype(I16)


def marked(e):
    return jnp.broadcast_to(e, (TAIL, e.shape[1])).astype(jnp.int32).astype(I16)


def scale_of(tail):
    return jnp.exp2(-tail.astype(jnp.int32).astype(F32)[:1])


def plain(q):
    return q.astype(jnp.int32).astype(F32)


def write(out, first, block):
    if out.dtype == F32:
        out[first:first + block.shape[0], :] = block
    else:
        e = exponent(jnp.max(jnp.abs(block), axis=0, keepdims=True))
        end = first + block.shape[0]
        out[first:end, :] = coded(block, e)
        out[end:end + TAIL, :] = marked(e)


def bulk_body(blocks, bulk, turned, *refs):
    at = position()
    total = turned.shape[0] // RING
    own = jnp.where(at[1] == 0, at[2], at[3])
    outs = refs[len(refs) - len(blocks):]
    arrived = iter(refs)
    wide = bulk.shape[1] // 2
    for (shift, half, adds), out in zip(blocks, outs):
        rows = total if half is None else total // 2
        first = lax.rem(own + shift, RING) * total + (0 if half is None else half * rows)
        left = turned[pl.ds(pl.multiple_of(first, 128), rows), :]
        part = next(arrived) if adds else None
        for n in range(2):
            lanes = slice(n * wide, (n + 1) * wide)
            block = jnp.dot(left, bulk[:, lanes], preferred_element_type=F32)
            if adds:
                block = block + plain(part[:rows, lanes]) * scale_of(part[rows:, lanes])
            write(out.at[:, lanes], 0, block)


def bulk_k(bulk, turned, blocks, arrived=()):
    depth, columns = bulk.shape
    total = turned.shape[0] // RING
    sizes = [total if half is None else total // 2 for _, half, _ in blocks]
    return pl.pallas_call(
        functools.partial(bulk_body, blocks),
        out_shape=[
            jax.ShapeDtypeStruct((n + (TAIL if shift else 0), columns), I16 if shift else F32)
            for n, (shift, _, _) in zip(sizes, blocks)
        ],
        in_specs=[whole()] * (2 + len(arrived)),
        out_specs=[whole()] * len(blocks),
        compiler_params=params(28),
        cost_estimate=cost(2 * depth * sum(sizes) * columns, sum(sizes) * columns * 2),
    )(bulk, turned, *arrived)


def rest_body(slot, cut, rest, turned, *outs):
    narrow = rest.shape[1] // RING
    total = turned.shape[0] // RING
    right = rest[:, slot * narrow:(slot + 2) * narrow]
    for g in range(RING):
        block = jnp.dot(turned[g * total:(g + 1) * total, :], right, preferred_element_type=F32)
        for n in range(2):
            out = outs[cut[n][g // 2]]
            size = total if out.dtype == F32 else total + TAIL
            whole_block = out.shape[0] == RING * total
            write(out, (g if whole_block else g % 2) * size, block[:, n * narrow:(n + 1) * narrow])


def rest_k(rest, turned, slot, cut, kinds):
    depth = rest.shape[0]
    ao = turned.shape[0]
    narrow = rest.shape[1] // RING
    shapes = {
        "message": ((ao // 2 + 2 * TAIL, narrow), I16), "half": ((ao // 2, narrow), F32), "all": ((ao, narrow), F32)
    }
    return pl.pallas_call(
        functools.partial(rest_body, slot, cut),
        out_shape=[jax.ShapeDtypeStruct(*shapes[kind]) for kind in kinds],
        in_specs=[whole()] * 2,
        out_specs=[whole()] * len(kinds),
        compiler_params=params(28),
        cost_estimate=cost(4 * depth * ao * narrow, ao * narrow * 4),
    )(rest, turned)


def rest_mid_body(*refs):
    for own, arrived, out in ((refs[0], refs[1], refs[4]), (refs[2], refs[3], refs[5])):
        total = own.shape[0] // 2
        for g in range(2):
            first = g * (total + TAIL)
            v = own[g * total:(g + 1) * total, :] + plain(arrived[first:first + total, :]) * scale_of(
                arrived[first + total:first + total + TAIL, :]
            )
            write(out, first, v)


def rest_mid(up, arrived_up, down, arrived_down):
    shape = jax.ShapeDtypeStruct(arrived_up.shape, I16)
    return pl.pallas_call(
        rest_mid_body,
        out_shape=[shape] * 2,
        in_specs=[whole()] * 4,
        out_specs=[whole()] * 2,
        compiler_params=params(16),
        cost_estimate=cost(up.size * 16, up.size * 16),
        name="rest_mid",
    )(up, arrived_up, down, arrived_down)


def gathered(own, arrived, first, tail, row, lanes):
    v = own[pl.ds(pl.multiple_of(first[0] + row, 64), first[2]), lanes]
    for m in arrived:
        cut = pl.ds(pl.multiple_of(first[1] + row, 16), first[2])
        v = v + plain(m[cut, lanes]) * scale_of(m[tail:tail + TAIL, lanes])
    return v


def rest_second_body(own, a, b, d, e, after, kept, *outs):
    at = position()
    high = kept.shape[0]
    total, step = own.shape[0] // RING, own.shape[1]
    h = jnp.where(at[1] == 0, at[3], at[2])
    for k in range(RING):
        row = lax.rem(h + k, RING) * high
        out = kept if k == 0 else outs[k - 1]
        for n in range(RING):
            start = n % 2 * (total + TAIL)
            v = gathered(
                own, (a, b) if n < 2 else (d, e), (n * total, start, high), start + total, row, slice(0, step)
            )
            write(out.at[:, n * step:(n + 1) * step], 0, v)


def rest_second(own, upper, lower, after):
    total, columns = own.shape
    high, every = total // RING // RING, columns * RING
    return list(pl.pallas_call(
        rest_second_body,
        out_shape=[jax.ShapeDtypeStruct((high, every), F32)]
        + [jax.ShapeDtypeStruct((high + TAIL, every), I16)] * 3,
        in_specs=[whole()] * 6,
        out_specs=[whole()] * 4,
        compiler_params=params(24),
        cost_estimate=cost(total * columns * 12, total * columns * 8),
        name="rest_second_sum",
    )(own, *upper, *lower, after))


def bulk_second_body(own, a, b, d, e, after, kept, *outs):
    at = position()
    high = kept.shape[0]
    h = jnp.where(at[1] == 0, at[3], at[2])
    half = own.shape[0] // 2
    step = 256
    for k in range(RING):
        block = lax.rem(h + k, RING)
        out = kept if k == 0 else outs[k - 1]

        def part(upper, arrived, block=block, out=out):
            @pl.when((block < RING // 2) == upper)
            def _():
                row = pl.multiple_of(lax.rem(block, RING // 2) * high, 64)
                first = pl.multiple_of(block * high, 64)
                for lane in range(0, own.shape[1], step):
                    lanes = slice(lane, lane + step)
                    v = own[pl.ds(first, high), lanes]
                    for m in arrived:
                        v = v + plain(m[pl.ds(row, high), lanes]) * scale_of(m[half:, lanes])
                    write(out.at[:, lanes], 0, v)

        part(True, (a, b))
        part(False, (d, e))


def bulk_second(own, upper, lower, after):
    total, columns = own.shape
    high = total // RING
    return list(pl.pallas_call(
        bulk_second_body,
        out_shape=[jax.ShapeDtypeStruct((high, columns), F32)]
        + [jax.ShapeDtypeStruct((high + TAIL, columns), I16)] * 3,
        in_specs=[whole()] * 6,
        out_specs=[whole()] * 4,
        compiler_params=params(24),
        cost_estimate=cost(total * columns * 12, total * columns * 8),
        name="bulk_second_sum",
    )(own, *upper, *lower, after))


def third_body(by_z, own, a, b, d, after, *outs):
    at = position()
    high, step = outs[0].shape
    start = at[0] if by_z else jnp.where(at[1] == 0, at[2], at[3])
    for k in range(RING):
        cut = pl.ds(pl.multiple_of(lax.rem(start + k, RING) * step, 128), step)
        write(outs[k], 0, gathered(own, (a, b, d), (0, 0, high), high, 0, cut))


def third(parts, by_z, after):
    high, every = parts[0].shape
    wide = every // RING
    return list(pl.pallas_call(
        functools.partial(third_body, by_z),
        out_shape=[jax.ShapeDtypeStruct((high, wide), F32)] + [jax.ShapeDtypeStruct((high + TAIL, wide), I16)] * 3,
        in_specs=[whole()] * 5,
        out_specs=[whole()] * 4,
        compiler_params=params(16),
        cost_estimate=cost(high * every * 16, high * every * 10),
        name="third_sum",
    )(*parts, after))


def tick_body(v, out):
    out[...] = v[...]


def tick(v):
    return pl.pallas_call(
        tick_body,
        out_shape=jax.ShapeDtypeStruct(v.shape, v.dtype),
        in_specs=[whole()],
        out_specs=whole(),
        compiler_params=params(1),
        cost_estimate=cost(1000, 32),
        name="tick",
    )(v)


def finish_body(own, a, b, d, rest, ra, rb, rd, out):
    high, wide = own.shape
    for first, v, arrived in ((0, own[...], (a, b, d)), (wide, rest[...], (ra, rb, rd))):
        for m in arrived:
            v = v + plain(m[:high, :]) * scale_of(m[high:, :])
        out[:, first:first + v.shape[1]] = v


def finish(bulk, rest):
    high = bulk[0].shape[0]
    ao = bulk[0].shape[1] + rest[0].shape[1]
    return pl.pallas_call(
        finish_body,
        out_shape=jax.ShapeDtypeStruct((high, ao), F32),
        in_specs=[whole()] * 8,
        out_specs=whole(),
        compiler_params=params(8),
        cost_estimate=cost(high * ao * 8, high * ao * 14),
    )(*bulk, *rest)


def shards(half, metric, survive):
    parts = screen(survive, half)
    here = [parts[0]] + [None] * 3
    for k in (2, 1, 3):
        here[k] = send(parts[k], along_z(k))
    pair = jnp.concatenate([metric, send(metric, other_core)], axis=0)
    metrics = [pair] + [None] * 3
    for k in (1, 2, 3):
        metrics[k] = send(pair, along_z(k))
    mixed = join(metrics)
    there = [None] * 4
    for k in (0, 2, 1, 3):
        there[k] = send(here[k], other_core)
    bulk_rows, rest_rows, turned = fit([v for both in zip(here, there) for v in both], mixed)

    def bulk_step(*blocks, arrived=()):
        return bulk_k(bulk_rows, turned, blocks, arrived)

    def rest_step(*how):
        return rest_k(rest_rows, turned, *how)

    def near(axis, up, down):
        up = send(up, axis(1))
        down = send(down, axis(3))
        return up, down

    def onward(parts, shift):
        for k in (1, 2, 3):
            parts[k] = send(parts[k], shift(k))

    far = near(first_axis, *bulk_step((2, 0, False), (2, 1, False)))
    lower_up, upper_down = near(first_axis, *bulk_step((1, 1, False), (3, 0, False)))
    upper, lower, rest_own = rest_step(0, ((0, 1), (2, 2)), ("message", "message", "all"))
    rest_far = near(along_z, upper, lower)
    upper_up, lower_down = near(first_axis, *bulk_step((1, 0, True), (3, 1, True), arrived=far))
    keep_up, up, down, keep_down = rest_step(2, ((0, 1), (2, 3)), ("half", "message", "message", "half"))
    rest_near = near(along_z, up, down)
    up, down = rest_mid(keep_up, rest_far[0], keep_down, rest_far[1])
    mid = near(along_z, up, down)
    own = bulk_step((0, None, False))[0]
    bulk = bulk_second(own, (upper_up, upper_down), (lower_up, lower_down), metric)
    onward(bulk, second_axis)
    then = tick(metric)
    rest = rest_second(rest_own, (mid[0], rest_near[1]), (rest_near[0], mid[1]), then)
    onward(rest, second_axis)
    then = tick(then)
    bulk = third(bulk, True, then)
    onward(bulk, along_z)
    then = tick(then)
    rest = third(rest, False, then)
    onward(rest, first_axis)
    return finish(bulk, rest)


def solution(mesh):
    finer = Mesh(mesh.devices.reshape(4, 2, 4, 4), AXES)
    placed = (P(("z", "c"), ("x", "y"), None), P(("z", "c"), None), P(("z", "c"), ("x", "y"), None))
    return jax.shard_map(shards, mesh=finer, in_specs=placed, out_specs=P(("x", "y"), ("z", "c")), check_vma=False)
```

```python
import functools

import jax
import jax.numpy as jnp
from jax import lax
from jax.experimental import pallas as pl
from jax.experimental.pallas import tpu as pltpu
from jax.sharding import Mesh
from jax.sharding import PartitionSpec as P


AXES = ("z", "c", "x", "y")
BF = jnp.bfloat16
F32 = jnp.float32
I16 = jnp.int16
MIB = 1 << 20
RING = 4
TAIL = 8


def whole():
    return pl.BlockSpec(memory_space=pltpu.VMEM)


def scalars():
    return pl.BlockSpec(memory_space=pltpu.SMEM)


def position():
    return [lax.axis_index(a) for a in AXES]


def params(mib):
    return pltpu.CompilerParams(vmem_limit_bytes=mib * MIB)


def cost(flops, moved):
    return pl.CostEstimate(flops=flops, bytes_accessed=moved, transcendentals=0)


def place(z, c, x, y):
    return ((z % 4) * 2 + c) * 16 + (x % 4) * 4 + y % 4


def moves(shift):
    every = [(z, c, x, y) for z in range(4) for c in range(2) for x in range(4) for y in range(4)]
    return [(place(*d), place(*shift(*d))) for d in every]


def send(v, shift):
    return lax.ppermute(v, AXES, moves(shift))


def along_z(k):
    return lambda z, c, x, y: (z + k, c, x, y)


def other_core(z, c, x, y):
    return (z, 1 - c, x, y)


def first_axis(k):
    return lambda z, c, x, y: (z, c, x + k, y) if c == 0 else (z, c, x, y + k)


def second_axis(k):
    return lambda z, c, x, y: (z, c, x, y + k) if c == 0 else (z, c, x + k, y)


def screen_body(survive, half, *rest):
    outs, (held, turned, sems) = rest[:4], rest[4:]
    at = position()
    ao = half.shape[2]
    block = ao // survive.shape[2]
    chunks = sems.shape[0]
    lanes = ao // chunks
    copies = [
        pltpu.make_async_copy(half.at[:, :, cut], held.at[:, :, cut], sems.at[n])
        for n, cut in enumerate(slice(n * lanes, (n + 1) * lanes) for n in range(chunks))
    ]
    for copy in copies:
        copy.start()
    for n in range(chunks):
        copies[n].wait()

        def step(m, carry):
            m = n * (lanes // block) + m
            cut = pl.ds(pl.multiple_of(m * block, block), block)
            keep = survive[0, 0, m].astype(F32)
            turned[:, :, cut] = jnp.swapaxes(held[:, :, cut].astype(F32) * keep, 0, 1).astype(BF)
            return carry

        lax.fori_loop(0, lanes // block, step, 0, unroll=True)
    group = outs[0].shape[0]
    for k in range(RING):
        first = lax.rem(at[0] + k, RING) * group
        outs[k][...] = turned[pl.ds(first, group)]


def screen(survive, half):
    aux, occ, ao = half.shape
    out = jax.ShapeDtypeStruct((occ // RING, aux, ao), BF)
    in_hbm = pl.BlockSpec(memory_space=pltpu.HBM)
    return pl.pallas_call(
        screen_body,
        out_shape=[out] * RING,
        in_specs=[scalars(), in_hbm],
        out_specs=[whole()] * RING,
        scratch_shapes=[
            pltpu.VMEM(half.shape, BF),
            pltpu.VMEM((occ, aux, ao), BF),
            pltpu.SemaphoreType.DMA((4,)),
        ],
        compiler_params=params(50),
        cost_estimate=cost(half.size, half.size * 4),
        name="screen",
    )(survive, half)


def join_body(*refs):
    metrics, mixed = refs[:4], refs[4]
    at = position()
    aux = mixed.shape[0]
    part = aux // 8
    metric = jnp.concatenate([m[...] for m in metrics], axis=0)
    source = lax.broadcasted_iota(jnp.int32, (aux, aux), 0)
    n = lax.broadcasted_iota(jnp.int32, (aux, aux), 1)
    slot = n // part
    up = lax.rem(at[0] - slot // 2 + RING, RING)
    core = jnp.where(slot % 2 == 0, at[1], 1 - at[1])
    wanted = (up * 2 + core) * part + n % part
    pick = jnp.where(source == wanted, 1.0, 0.0).astype(BF)
    mixed[...] = jnp.dot(metric, pick, preferred_element_type=F32).astype(BF)


def join(metrics):
    aux = metrics[0].shape[1]
    return pl.pallas_call(
        join_body,
        out_shape=jax.ShapeDtypeStruct((aux, aux), BF),
        in_specs=[whole()] * 4,
        out_specs=whole(),
        compiler_params=params(4),
        cost_estimate=cost(2 * aux**3, aux * aux * 4),
        name="join",
    )(*metrics)


def fit_body(*refs):
    pieces, mixed, (bulk, rest, turned) = refs[:8], refs[8], refs[9:]
    at = position()
    step = pl.program_id(0)
    ao = turned.shape[0]
    aux = mixed.shape[0]
    screened = jnp.concatenate([p[0] for p in pieces], axis=0)
    fitted = jnp.dot(mixed[...], screened, preferred_element_type=F32).astype(BF)
    wide, narrow = bulk.shape[1] // RING, rest.shape[1] // RING

    def chosen(column, lanes):
        first, second = column, column + wide + narrow
        return jnp.where(at[1] == 0, fitted[:, first:first + lanes], fitted[:, second:second + lanes])

    for n in range(RING):
        bulk[:, n * wide:(n + 1) * wide] = chosen(n * (ao // RING), wide)
        rest[:, n * narrow:(n + 1) * narrow] = chosen(n * (ao // RING) + wide, narrow)
    flipped = fitted.T
    cut = pl.ds(pl.multiple_of(step * aux, aux), aux)
    high = ao // (RING * RING)
    for x in range(RING):
        for y in range(RING):
            n = x * RING + y
            to = jnp.where(at[1] == 0, n, y * RING + x) * high
            turned[pl.ds(pl.multiple_of(to, 64), high), cut] = flipped[n * high:(n + 1) * high]


def fit(pieces, mixed):
    group, part, ao = pieces[0].shape
    aux = part * 8
    piece = pl.BlockSpec((1, part, ao), lambda i: (i, 0, 0))
    return pl.pallas_call(
        fit_body,
        grid=(group,),
        out_shape=[jax.ShapeDtypeStruct((group * aux, n), BF) for n in (ao // 3, ao // 6)]
        + [jax.ShapeDtypeStruct((ao, group * aux), BF)],
        in_specs=[piece] * 8 + [whole()],
        out_specs=[pl.BlockSpec((aux, n), lambda i: (i, 0)) for n in (ao // 3, ao // 6)]
        + [pl.BlockSpec((ao, group * aux), lambda i: (0, 0))],
        compiler_params=params(28),
        cost_estimate=cost(2 * group * aux * aux * ao, group * aux * ao * 6),
        name="fit",
    )(*pieces, mixed)


def exponent(top):
    return jnp.floor(14.9 - jnp.log2(jnp.maximum(top, 1e-30)))


def coded(v, e):
    return jnp.round(v * jnp.exp2(e)).astype(jnp.int32).astype(I16)


def marked(e):
    return jnp.broadcast_to(e, (TAIL, e.shape[1])).astype(jnp.int32).astype(I16)


def scale_of(tail):
    return jnp.exp2(-tail.astype(jnp.int32).astype(F32)[:1])


def plain(q):
    return q.astype(jnp.int32).astype(F32)


def write(out, first, block, tail=None):
    end = first + block.shape[0]
    if out.dtype == F32:
        out[first:end, :] = block
    else:
        e = exponent(jnp.max(jnp.abs(block), axis=0, keepdims=True))
        tail = end if tail is None else tail
        out[first:end, :] = coded(block, e)
        out[tail:tail + TAIL, :] = marked(e)


def bulk_body(blocks, bulk, turned, *refs):
    at = position()
    total = turned.shape[0] // RING
    own = jnp.where(at[1] == 0, at[2], at[3])
    outs = refs[len(refs) - len(blocks):]
    arrived = iter(refs)
    wide = bulk.shape[1] // 2
    for (shift, half, adds), out in zip(blocks, outs):
        rows = total if half is None else total // 2
        first = lax.rem(own + shift, RING) * total + (0 if half is None else half * rows)
        left = turned[pl.ds(pl.multiple_of(first, 128), rows), :]
        part = next(arrived) if adds else None
        for n in range(2):
            lanes = slice(n * wide, (n + 1) * wide)
            block = jnp.dot(left, bulk[:, lanes], preferred_element_type=F32)
            if adds:
                block = block + plain(part[:rows, lanes]) * scale_of(part[rows:, lanes])
            write(out.at[:, lanes], 0, block)


def bulk_k(bulk, turned, blocks, arrived=()):
    depth, columns = bulk.shape
    total = turned.shape[0] // RING
    sizes = [total if half is None else total // 2 for _, half, _ in blocks]
    return pl.pallas_call(
        functools.partial(bulk_body, blocks),
        out_shape=[
            jax.ShapeDtypeStruct((n + (TAIL if shift else 0), columns), I16 if shift else F32)
            for n, (shift, _, _) in zip(sizes, blocks)
        ],
        in_specs=[whole()] * (2 + len(arrived)),
        out_specs=[whole()] * len(blocks),
        compiler_params=params(28),
        cost_estimate=cost(2 * depth * sum(sizes) * columns, sum(sizes) * columns * 2),
    )(bulk, turned, *arrived)


def rest_body(steps, cut, rest, turned, *outs):
    at = position()
    narrow = rest.shape[1] // RING
    total = turned.shape[0] // RING
    right = jnp.concatenate(
        [rest[:, pl.ds(pl.multiple_of(lax.rem(at[0] + k, RING) * narrow, 128), narrow)] for k in steps], axis=1
    )
    for g in range(RING):
        block = jnp.dot(turned[g * total:(g + 1) * total, :], right, preferred_element_type=F32)
        for n in range(2):
            out = outs[cut[n][g // 2]]
            row = g if out.shape[0] == RING * total else g % 2
            write(out, row * total, block[:, n * narrow:(n + 1) * narrow], 2 * total + g % 2 * TAIL)


def rest_k(rest, turned, steps, cut, kinds):
    depth = rest.shape[0]
    ao = turned.shape[0]
    narrow = rest.shape[1] // RING
    shapes = {
        "message": ((ao // 2 + 2 * TAIL, narrow), I16), "half": ((ao // 2, narrow), F32), "all": ((ao, narrow), F32)
    }
    return pl.pallas_call(
        functools.partial(rest_body, steps, cut),
        out_shape=[jax.ShapeDtypeStruct(*shapes[kind]) for kind in kinds],
        in_specs=[whole()] * 2,
        out_specs=[whole()] * len(kinds),
        compiler_params=params(28),
        cost_estimate=cost(4 * depth * ao * narrow, ao * narrow * 4),
    )(rest, turned)


def rest_mid_body(*refs):
    for own, arrived, out in ((refs[0], refs[1], refs[4]), (refs[2], refs[3], refs[5])):
        total = own.shape[0] // 2
        for g in range(2):
            first, tail = g * total, 2 * total + g * TAIL
            v = own[first:first + total, :] + plain(arrived[first:first + total, :]) * scale_of(
                arrived[tail:tail + TAIL, :]
            )
            write(out, first, v, tail)


def rest_mid(up, arrived_up, down, arrived_down):
    shape = jax.ShapeDtypeStruct(arrived_up.shape, I16)
    return pl.pallas_call(
        rest_mid_body,
        out_shape=[shape] * 2,
        in_specs=[whole()] * 4,
        out_specs=[whole()] * 2,
        compiler_params=params(16),
        cost_estimate=cost(up.size * 16, up.size * 16),
        name="rest_mid",
    )(up, arrived_up, down, arrived_down)


def gathered(own, arrived, first, tail, row, lanes):
    v = own[pl.ds(pl.multiple_of(first[0] + row, 64), first[2]), lanes]
    for m in arrived:
        cut = pl.ds(pl.multiple_of(first[1] + row, 16), first[2])
        v = v + plain(m[cut, lanes]) * scale_of(m[tail:tail + TAIL, lanes])
    return v


def rest_second_body(own, a, b, d, e, after, kept, *outs):
    at = position()
    high = kept.shape[0]
    total, step = own.shape[0] // RING, own.shape[1]
    h = jnp.where(at[1] == 0, at[3], at[2])
    for k in range(RING):
        row = lax.rem(h + k, RING) * high
        out = kept if k == 0 else outs[k - 1]
        for n in range(RING):
            start, tail = n % 2 * total, 2 * total + n % 2 * TAIL
            v = gathered(own, (a, b) if n < 2 else (d, e), (n * total, start, high), tail, row, slice(0, step))
            write(out.at[:, n * step:(n + 1) * step], 0, v)


def rest_second(own, upper, lower, after):
    total, columns = own.shape
    high, every = total // RING // RING, columns * RING
    return list(pl.pallas_call(
        rest_second_body,
        out_shape=[jax.ShapeDtypeStruct((high, every), F32)]
        + [jax.ShapeDtypeStruct((high + TAIL, every), I16)] * 3,
        in_specs=[whole()] * 6,
        out_specs=[whole()] * 4,
        compiler_params=params(24),
        cost_estimate=cost(total * columns * 12, total * columns * 8),
        name="rest_second_sum",
    )(own, *upper, *lower, after))


def bulk_second_body(own, a, b, d, e, after, kept, *outs):
    at = position()
    high = kept.shape[0]
    h = jnp.where(at[1] == 0, at[3], at[2])
    half = own.shape[0] // 2
    step = 256
    for k in range(RING):
        block = lax.rem(h + k, RING)
        out = kept if k == 0 else outs[k - 1]

        def part(upper, arrived, block=block, out=out):
            @pl.when((block < RING // 2) == upper)
            def _():
                row = pl.multiple_of(lax.rem(block, RING // 2) * high, 64)
                first = pl.multiple_of(block * high, 64)
                for lane in range(0, own.shape[1], step):
                    lanes = slice(lane, lane + step)
                    v = own[pl.ds(first, high), lanes]
                    for m in arrived:
                        v = v + plain(m[pl.ds(row, high), lanes]) * scale_of(m[half:, lanes])
                    write(out.at[:, lanes], 0, v)

        part(True, (a, b))
        part(False, (d, e))


def bulk_second(own, upper, lower, after):
    total, columns = own.shape
    high = total // RING
    return list(pl.pallas_call(
        bulk_second_body,
        out_shape=[jax.ShapeDtypeStruct((high, columns), F32)]
        + [jax.ShapeDtypeStruct((high + TAIL, columns), I16)] * 3,
        in_specs=[whole()] * 6,
        out_specs=[whole()] * 4,
        compiler_params=params(24),
        cost_estimate=cost(total * columns * 12, total * columns * 8),
        name="bulk_second_sum",
    )(own, *upper, *lower, after))


def third_body(by_z, own, a, b, d, after, *outs):
    at = position()
    high, step = outs[0].shape
    start = at[0] if by_z else jnp.where(at[1] == 0, at[2], at[3])
    for k in range(RING):
        cut = pl.ds(pl.multiple_of(lax.rem(start + k, RING) * step, 128), step)
        write(outs[k], 0, gathered(own, (a, b, d), (0, 0, high), high, 0, cut))


def third(parts, by_z, after):
    high, every = parts[0].shape
    wide = every // RING
    return list(pl.pallas_call(
        functools.partial(third_body, by_z),
        out_shape=[jax.ShapeDtypeStruct((high, wide), F32)] + [jax.ShapeDtypeStruct((high + TAIL, wide), I16)] * 3,
        in_specs=[whole()] * 5,
        out_specs=[whole()] * 4,
        compiler_params=params(16),
        cost_estimate=cost(high * every * 16, high * every * 10),
        name="third_sum",
    )(*parts, after))


def tick_body(v, out):
    out[...] = v[...]


def tick(v):
    return pl.pallas_call(
        tick_body,
        out_shape=jax.ShapeDtypeStruct(v.shape, v.dtype),
        in_specs=[whole()],
        out_specs=whole(),
        compiler_params=params(1),
        cost_estimate=cost(1000, 32),
        name="tick",
    )(v)


def finish_body(own, a, b, d, rest, ra, rb, rd, out):
    high, wide = own.shape
    for first, v, arrived in ((0, own[...], (a, b, d)), (wide, rest[...], (ra, rb, rd))):
        for m in arrived:
            v = v + plain(m[:high, :]) * scale_of(m[high:, :])
        out[:, first:first + v.shape[1]] = v


def finish(bulk, rest):
    high = bulk[0].shape[0]
    ao = bulk[0].shape[1] + rest[0].shape[1]
    return pl.pallas_call(
        finish_body,
        out_shape=jax.ShapeDtypeStruct((high, ao), F32),
        in_specs=[whole()] * 8,
        out_specs=whole(),
        compiler_params=params(8),
        cost_estimate=cost(high * ao * 8, high * ao * 14),
    )(*bulk, *rest)


def shards(half, metric, survive):
    parts = screen(survive, half)
    here = [parts[0]] + [None] * 3
    for k in (2, 1, 3):
        here[k] = send(parts[k], along_z(k))
    pair = jnp.concatenate([metric, send(metric, other_core)], axis=0)
    metrics = [pair] + [None] * 3
    for k in (1, 2, 3):
        metrics[k] = send(pair, along_z(k))
    mixed = join(metrics)
    there = [None] * 4
    for k in (0, 2, 1, 3):
        there[k] = send(here[k], other_core)
    bulk_rows, rest_rows, turned = fit([v for both in zip(here, there) for v in both], mixed)

    def bulk_step(*blocks, arrived=()):
        return bulk_k(bulk_rows, turned, blocks, arrived)

    def rest_step(*how):
        return rest_k(rest_rows, turned, *how)

    def near(axis, up, down):
        up = send(up, axis(1))
        down = send(down, axis(3))
        return up, down

    def onward(parts, shift):
        for k in (1, 2, 3):
            parts[k] = send(parts[k], shift(k))

    far = near(first_axis, *bulk_step((2, 0, False), (2, 1, False)))
    upper, lower, rest_own = rest_step((2, 0), ((0, 1), (2, 2)), ("message", "message", "all"))
    rest_far = near(along_z, upper, lower)
    lower_up, upper_down = near(first_axis, *bulk_step((1, 1, False), (3, 0, False)))
    keep_up, up, down, keep_down = rest_step((1, 3), ((0, 1), (2, 3)), ("half", "message", "message", "half"))
    rest_near = near(along_z, up, down)
    upper_up, lower_down = near(first_axis, *bulk_step((1, 0, True), (3, 1, True), arrived=far))
    up, down = rest_mid(keep_up, rest_far[0], keep_down, rest_far[1])
    mid = near(along_z, up, down)
    own = bulk_step((0, None, False))[0]
    bulk = bulk_second(own, (upper_up, upper_down), (lower_up, lower_down), metric)
    onward(bulk, second_axis)
    then = tick(metric)
    rest = rest_second(rest_own, (mid[0], rest_near[1]), (rest_near[0], mid[1]), then)
    onward(rest, second_axis)
    then = tick(then)
    bulk = third(bulk, True, then)
    onward(bulk, along_z)
    then = tick(then)
    rest = third(rest, False, then)
    onward(rest, first_axis)
    return finish(bulk, rest)


def solution(mesh):
    finer = Mesh(mesh.devices.reshape(4, 2, 4, 4), AXES)
    placed = (P(("z", "c"), ("x", "y"), None), P(("z", "c"), None), P(("z", "c"), ("x", "y"), None))
    return jax.shard_map(shards, mesh=finer, in_specs=placed, out_specs=P(("x", "y"), ("z", "c")), check_vma=False)
```

```python
import functools

import jax
import jax.numpy as jnp
from jax import lax
from jax.experimental import pallas as pl
from jax.experimental.pallas import tpu as pltpu
from jax.sharding import Mesh
from jax.sharding import PartitionSpec as P


AXES = ("z", "c", "x", "y")
BF = jnp.bfloat16
F32 = jnp.float32
I16 = jnp.int16
MIB = 1 << 20
RING = 4
TAIL = 8


def whole():
    return pl.BlockSpec(memory_space=pltpu.VMEM)


def scalars():
    return pl.BlockSpec(memory_space=pltpu.SMEM)


def position():
    return [lax.axis_index(a) for a in AXES]


def params(mib):
    return pltpu.CompilerParams(vmem_limit_bytes=mib * MIB)


def cost(flops, moved):
    return pl.CostEstimate(flops=flops, bytes_accessed=moved, transcendentals=0)


def place(z, c, x, y):
    return ((z % 4) * 2 + c) * 16 + (x % 4) * 4 + y % 4


def moves(shift):
    every = [(z, c, x, y) for z in range(4) for c in range(2) for x in range(4) for y in range(4)]
    return [(place(*d), place(*shift(*d))) for d in every]


def send(v, shift):
    return lax.ppermute(v, AXES, moves(shift))


def along_z(k):
    return lambda z, c, x, y: (z + k, c, x, y)


def other_core(z, c, x, y):
    return (z, 1 - c, x, y)


def first_axis(k):
    return lambda z, c, x, y: (z, c, x + k, y) if c == 0 else (z, c, x, y + k)


def second_axis(k):
    return lambda z, c, x, y: (z, c, x, y + k) if c == 0 else (z, c, x + k, y)


def screen_body(survive, half, *rest):
    outs, (held, turned, sems) = rest[:4], rest[4:]
    at = position()
    ao = half.shape[2]
    block = ao // survive.shape[2]
    chunks = sems.shape[0]
    lanes = ao // chunks
    copies = [
        pltpu.make_async_copy(half.at[:, :, cut], held.at[:, :, cut], sems.at[n])
        for n, cut in enumerate(slice(n * lanes, (n + 1) * lanes) for n in range(chunks))
    ]
    for copy in copies:
        copy.start()
    group = outs[0].shape[0]
    for n in range(chunks):
        copies[n].wait()
        for m in range(n * (lanes // block), (n + 1) * (lanes // block)):
            cut = slice(m * block, (m + 1) * block)
            keep = survive[0, 0, m].astype(F32)
            turned[:, :, cut] = jnp.swapaxes(held[:, :, cut].astype(F32) * keep, 0, 1).astype(BF)
        cut = slice(n * lanes, (n + 1) * lanes)
        for k in range(RING):
            outs[k][:, :, cut] = turned[pl.ds(lax.rem(at[0] + k, RING) * group, group), :, cut]


def screen(survive, half):
    aux, occ, ao = half.shape
    out = jax.ShapeDtypeStruct((occ // RING, aux, ao), BF)
    in_hbm = pl.BlockSpec(memory_space=pltpu.HBM)
    return pl.pallas_call(
        screen_body,
        out_shape=[out] * RING,
        in_specs=[scalars(), in_hbm],
        out_specs=[whole()] * RING,
        scratch_shapes=[
            pltpu.VMEM(half.shape, BF),
            pltpu.VMEM((occ, aux, ao), BF),
            pltpu.SemaphoreType.DMA((6,)),
        ],
        compiler_params=params(50),
        cost_estimate=cost(half.size, half.size * 4),
        name="screen",
    )(survive, half)


def join_body(*refs):
    metrics, mixed = refs[:4], refs[4]
    at = position()
    aux = metrics[0].shape[1]
    part = aux // 8
    metric = jnp.concatenate([m[...] for m in metrics], axis=0)
    source = lax.broadcasted_iota(jnp.int32, (aux, aux), 0)
    n = lax.broadcasted_iota(jnp.int32, (aux, aux), 1)
    slot = n // part
    up = lax.rem(at[0] - slot // 2 + RING, RING)
    core = jnp.where(slot % 2 == 0, at[1], 1 - at[1])
    wanted = (up * 2 + core) * part + n % part
    pick = jnp.where(source == wanted, 1.0, 0.0).astype(BF)
    mixed[...] = jnp.zeros_like(mixed)
    for n in range(2):
        cut = slice(n * aux, (n + 1) * aux)
        mixed[cut, cut] = jnp.dot(metric, pick, preferred_element_type=F32).astype(BF)


def join(metrics):
    aux = metrics[0].shape[1]
    return pl.pallas_call(
        join_body,
        out_shape=jax.ShapeDtypeStruct((2 * aux, 2 * aux), BF),
        in_specs=[whole()] * 4,
        out_specs=whole(),
        compiler_params=params(4),
        cost_estimate=cost(2 * aux**3, aux * aux * 4),
        name="join",
    )(*metrics)


def fit_body(*refs):
    pieces, mixed, (bulk, rest, turned) = refs[:8], refs[8], refs[9:]
    at = position()
    step = pl.program_id(0)
    ao = turned.shape[0]
    aux = mixed.shape[0]
    screened = jnp.concatenate([p[n] for n in range(2) for p in pieces], axis=0)
    fitted = jnp.dot(mixed[...], screened, preferred_element_type=F32).astype(BF)
    wide, narrow = bulk.shape[1] // RING, rest.shape[1] // RING

    def chosen(column, lanes):
        first, second = column, column + wide + narrow
        return jnp.where(at[1] == 0, fitted[:, first:first + lanes], fitted[:, second:second + lanes])

    for n in range(RING):
        bulk[:, n * wide:(n + 1) * wide] = chosen(n * (ao // RING), wide)
        rest[:, n * narrow:(n + 1) * narrow] = chosen(n * (ao // RING) + wide, narrow)
    flipped = fitted.T
    cut = pl.ds(pl.multiple_of(step * aux, aux), aux)
    high = ao // (RING * RING)
    for x in range(RING):
        for y in range(RING):
            n = x * RING + y
            to = jnp.where(at[1] == 0, n, y * RING + x) * high
            turned[pl.ds(pl.multiple_of(to, 64), high), cut] = flipped[n * high:(n + 1) * high]


def fit(pieces, mixed):
    group, part, ao = pieces[0].shape
    aux, steps = 2 * part * 8, group // 2
    piece = pl.BlockSpec((2, part, ao), lambda i: (i, 0, 0))
    return pl.pallas_call(
        fit_body,
        grid=(steps,),
        out_shape=[jax.ShapeDtypeStruct((steps * aux, n), BF) for n in (ao // 3, ao // 6)]
        + [jax.ShapeDtypeStruct((ao, steps * aux), BF)],
        in_specs=[piece] * 8 + [whole()],
        out_specs=[pl.BlockSpec((aux, n), lambda i: (i, 0)) for n in (ao // 3, ao // 6)]
        + [pl.BlockSpec((ao, steps * aux), lambda i: (0, 0))],
        compiler_params=params(28),
        cost_estimate=cost(2 * steps * aux * aux * ao, steps * aux * ao * 6),
        name="fit",
    )(*pieces, mixed)


def exponent(top):
    return jnp.floor(14.9 - jnp.log2(jnp.maximum(top, 1e-30)))


def coded(v, e):
    return jnp.round(v * jnp.exp2(e)).astype(jnp.int32).astype(I16)


def marked(e):
    return jnp.broadcast_to(e, (TAIL, e.shape[1])).astype(jnp.int32).astype(I16)


def scale_of(tail):
    return jnp.exp2(-tail.astype(jnp.int32).astype(F32)[:1])


def plain(q):
    return q.astype(jnp.int32).astype(F32)


def write(out, first, block, tail=None):
    end = first + block.shape[0]
    if out.dtype == F32:
        out[first:end, :] = block
    else:
        e = exponent(jnp.max(jnp.abs(block), axis=0, keepdims=True))
        tail = end if tail is None else tail
        out[first:end, :] = coded(block, e)
        out[tail:tail + TAIL, :] = marked(e)


def bulk_body(blocks, bulk, turned, *refs):
    at = position()
    total = turned.shape[0] // RING
    own = jnp.where(at[1] == 0, at[2], at[3])
    outs = refs[len(refs) - len(blocks):]
    arrived = iter(refs)
    wide = bulk.shape[1] // 2
    for (shift, half, adds), out in zip(blocks, outs):
        rows = total if half is None else total // 2
        first = lax.rem(own + shift, RING) * total + (0 if half is None else half * rows)
        left = turned[pl.ds(pl.multiple_of(first, 128), rows), :]
        part = next(arrived) if adds else None
        for n in range(2):
            lanes = slice(n * wide, (n + 1) * wide)
            block = jnp.dot(left, bulk[:, lanes], preferred_element_type=F32)
            if adds:
                block = block + plain(part[:rows, lanes]) * scale_of(part[rows:, lanes])
            write(out.at[:, lanes], 0, block)


def bulk_k(bulk, turned, blocks, arrived=()):
    depth, columns = bulk.shape
    total = turned.shape[0] // RING
    sizes = [total if half is None else total // 2 for _, half, _ in blocks]
    return pl.pallas_call(
        functools.partial(bulk_body, blocks),
        out_shape=[
            jax.ShapeDtypeStruct((n + (TAIL if shift else 0), columns), I16 if shift else F32)
            for n, (shift, _, _) in zip(sizes, blocks)
        ],
        in_specs=[whole()] * (2 + len(arrived)),
        out_specs=[whole()] * len(blocks),
        compiler_params=params(28),
        cost_estimate=cost(2 * depth * sum(sizes) * columns, sum(sizes) * columns * 2),
    )(bulk, turned, *arrived)


def rest_body(steps, cut, rest, turned, *outs):
    at = position()
    narrow = rest.shape[1] // RING
    total = turned.shape[0] // RING
    right = jnp.concatenate(
        [rest[:, pl.ds(pl.multiple_of(lax.rem(at[0] + k, RING) * narrow, 128), narrow)] for k in steps], axis=1
    )
    for g in range(RING):
        block = jnp.dot(turned[g * total:(g + 1) * total, :], right, preferred_element_type=F32)
        for n in range(2):
            out = outs[cut[n][g // 2]]
            row = g if out.shape[0] == RING * total else g % 2
            write(out, row * total, block[:, n * narrow:(n + 1) * narrow], 2 * total + g % 2 * TAIL)


def rest_k(rest, turned, steps, cut, kinds):
    depth = rest.shape[0]
    ao = turned.shape[0]
    narrow = rest.shape[1] // RING
    shapes = {
        "message": ((ao // 2 + 2 * TAIL, narrow), I16), "half": ((ao // 2, narrow), F32), "all": ((ao, narrow), F32)
    }
    return pl.pallas_call(
        functools.partial(rest_body, steps, cut),
        out_shape=[jax.ShapeDtypeStruct(*shapes[kind]) for kind in kinds],
        in_specs=[whole()] * 2,
        out_specs=[whole()] * len(kinds),
        compiler_params=params(28),
        cost_estimate=cost(4 * depth * ao * narrow, ao * narrow * 4),
    )(rest, turned)


def rest_mid_body(*refs):
    for own, arrived, out in ((refs[0], refs[1], refs[4]), (refs[2], refs[3], refs[5])):
        total = own.shape[0] // 2
        for g in range(2):
            first, tail = g * total, 2 * total + g * TAIL
            v = own[first:first + total, :] + plain(arrived[first:first + total, :]) * scale_of(
                arrived[tail:tail + TAIL, :]
            )
            write(out, first, v, tail)


def rest_mid(up, arrived_up, down, arrived_down):
    shape = jax.ShapeDtypeStruct(arrived_up.shape, I16)
    return pl.pallas_call(
        rest_mid_body,
        out_shape=[shape] * 2,
        in_specs=[whole()] * 4,
        out_specs=[whole()] * 2,
        compiler_params=params(16),
        cost_estimate=cost(up.size * 16, up.size * 16),
        name="rest_mid",
    )(up, arrived_up, down, arrived_down)


def gathered(own, arrived, first, tail, row, lanes):
    v = own[pl.ds(pl.multiple_of(first[0] + row, 64), first[2]), lanes]
    for m in arrived:
        cut = pl.ds(pl.multiple_of(first[1] + row, 16), first[2])
        v = v + plain(m[cut, lanes]) * scale_of(m[tail:tail + TAIL, lanes])
    return v


def rest_second_body(own, a, b, d, e, after, kept, *outs):
    at = position()
    high = kept.shape[0]
    total, step = own.shape[0] // RING, own.shape[1]
    h = jnp.where(at[1] == 0, at[3], at[2])
    for k in range(RING):
        row = lax.rem(h + k, RING) * high
        out = kept if k == 0 else outs[k - 1]
        for n in range(RING):
            start, tail = n % 2 * total, 2 * total + n % 2 * TAIL
            v = gathered(own, (a, b) if n < 2 else (d, e), (n * total, start, high), tail, row, slice(0, step))
            write(out.at[:, n * step:(n + 1) * step], 0, v)


def rest_second(own, upper, lower, after):
    total, columns = own.shape
    high, every = total // RING // RING, columns * RING
    return list(pl.pallas_call(
        rest_second_body,
        out_shape=[jax.ShapeDtypeStruct((high, every), F32)]
        + [jax.ShapeDtypeStruct((high + TAIL, every), I16)] * 3,
        in_specs=[whole()] * 6,
        out_specs=[whole()] * 4,
        compiler_params=params(24),
        cost_estimate=cost(total * columns * 12, total * columns * 8),
        name="rest_second_sum",
    )(own, *upper, *lower, after))


def bulk_second_body(own, a, b, d, e, after, kept, *outs):
    at = position()
    high = kept.shape[0]
    h = jnp.where(at[1] == 0, at[3], at[2])
    half = own.shape[0] // 2
    step = 256
    for k in range(RING):
        block = lax.rem(h + k, RING)
        out = kept if k == 0 else outs[k - 1]

        def part(upper, arrived, block=block, out=out):
            @pl.when((block < RING // 2) == upper)
            def _():
                row = pl.multiple_of(lax.rem(block, RING // 2) * high, 64)
                first = pl.multiple_of(block * high, 64)
                for lane in range(0, own.shape[1], step):
                    lanes = slice(lane, lane + step)
                    v = own[pl.ds(first, high), lanes]
                    for m in arrived:
                        v = v + plain(m[pl.ds(row, high), lanes]) * scale_of(m[half:, lanes])
                    write(out.at[:, lanes], 0, v)

        part(True, (a, b))
        part(False, (d, e))


def bulk_second(own, upper, lower, after):
    total, columns = own.shape
    high = total // RING
    return list(pl.pallas_call(
        bulk_second_body,
        out_shape=[jax.ShapeDtypeStruct((high, columns), F32)]
        + [jax.ShapeDtypeStruct((high + TAIL, columns), I16)] * 3,
        in_specs=[whole()] * 6,
        out_specs=[whole()] * 4,
        compiler_params=params(24),
        cost_estimate=cost(total * columns * 12, total * columns * 8),
        name="bulk_second_sum",
    )(own, *upper, *lower, after))


def third_body(by_z, own, a, b, d, after, *outs):
    at = position()
    high, step = outs[0].shape
    start = at[0] if by_z else jnp.where(at[1] == 0, at[2], at[3])
    for k in range(RING):
        cut = pl.ds(pl.multiple_of(lax.rem(start + k, RING) * step, 128), step)
        write(outs[k], 0, gathered(own, (a, b, d), (0, 0, high), high, 0, cut))


def third(parts, by_z, after):
    high, every = parts[0].shape
    wide = every // RING
    return list(pl.pallas_call(
        functools.partial(third_body, by_z),
        out_shape=[jax.ShapeDtypeStruct((high, wide), F32)] + [jax.ShapeDtypeStruct((high + TAIL, wide), I16)] * 3,
        in_specs=[whole()] * 5,
        out_specs=[whole()] * 4,
        compiler_params=params(16),
        cost_estimate=cost(high * every * 16, high * every * 10),
        name="third_sum",
    )(*parts, after))


def tick_body(v, out):
    out[...] = v[...]


def tick(v):
    return pl.pallas_call(
        tick_body,
        out_shape=jax.ShapeDtypeStruct(v.shape, v.dtype),
        in_specs=[whole()],
        out_specs=whole(),
        compiler_params=params(1),
        cost_estimate=cost(1000, 32),
        name="tick",
    )(v)


def finish_body(own, a, b, d, rest, ra, rb, rd, out):
    high, wide = own.shape
    for first, v, arrived in ((0, own[...], (a, b, d)), (wide, rest[...], (ra, rb, rd))):
        for m in arrived:
            v = v + plain(m[:high, :]) * scale_of(m[high:, :])
        out[:, first:first + v.shape[1]] = v


def finish(bulk, rest):
    high = bulk[0].shape[0]
    ao = bulk[0].shape[1] + rest[0].shape[1]
    return pl.pallas_call(
        finish_body,
        out_shape=jax.ShapeDtypeStruct((high, ao), F32),
        in_specs=[whole()] * 8,
        out_specs=whole(),
        compiler_params=params(8),
        cost_estimate=cost(high * ao * 8, high * ao * 14),
    )(*bulk, *rest)


def shards(half, metric, survive):
    parts = screen(survive, half)
    here = [parts[0]] + [None] * 3
    for k in (1, 3, 2):
        here[k] = send(parts[k], along_z(k))
    pair = jnp.concatenate([metric, send(metric, other_core)], axis=0)
    metrics = [pair] + [None] * 3
    for k in (1, 2, 3):
        metrics[k] = send(pair, along_z(k))
    mixed = join(metrics)
    there = [None] * 4
    for k in (0, 1, 3, 2):
        there[k] = send(here[k], other_core)
    bulk_rows, rest_rows, turned = fit([v for both in zip(here, there) for v in both], mixed)

    def bulk_step(*blocks, arrived=()):
        return bulk_k(bulk_rows, turned, blocks, arrived)

    def rest_step(*how):
        return rest_k(rest_rows, turned, *how)

    def near(axis, up, down):
        up = send(up, axis(1))
        down = send(down, axis(3))
        return up, down

    def onward(parts, shift):
        for k in (1, 2, 3):
            parts[k] = send(parts[k], shift(k))

    far = near(first_axis, *bulk_step((2, 0, False), (2, 1, False)))
    upper, lower, rest_own = rest_step((2, 0), ((0, 1), (2, 2)), ("message", "message", "all"))
    rest_far = near(along_z, upper, lower)
    lower_up, upper_down = near(first_axis, *bulk_step((1, 1, False), (3, 0, False)))
    keep_up, up, down, keep_down = rest_step((1, 3), ((0, 1), (2, 3)), ("half", "message", "message", "half"))
    rest_near = near(along_z, up, down)
    upper_up, lower_down = near(first_axis, *bulk_step((1, 0, True), (3, 1, True), arrived=far))
    up, down = rest_mid(keep_up, rest_far[0], keep_down, rest_far[1])
    mid = near(along_z, up, down)
    own = bulk_step((0, None, False))[0]
    bulk = bulk_second(own, (upper_up, upper_down), (lower_up, lower_down), metric)
    onward(bulk, second_axis)
    then = tick(metric)
    rest = rest_second(rest_own, (mid[0], rest_near[1]), (rest_near[0], mid[1]), then)
    onward(rest, second_axis)
    then = tick(then)
    bulk = third(bulk, True, then)
    onward(bulk, along_z)
    then = tick(then)
    rest = third(rest, False, then)
    onward(rest, first_axis)
    return finish(bulk, rest)


def solution(mesh):
    finer = Mesh(mesh.devices.reshape(4, 2, 4, 4), AXES)
    placed = (P(("z", "c"), ("x", "y"), None), P(("z", "c"), None), P(("z", "c"), ("x", "y"), None))
    return jax.shard_map(shards, mesh=finer, in_specs=placed, out_specs=P(("x", "y"), ("z", "c")), check_vma=False)
```

```python
import functools

import jax
import jax.numpy as jnp
from jax import lax
from jax.experimental import pallas as pl
from jax.experimental.pallas import tpu as pltpu
from jax.sharding import Mesh
from jax.sharding import PartitionSpec as P


AXES = ("z", "c", "x", "y")
BF = jnp.bfloat16
F32 = jnp.float32
I16 = jnp.int16
MIB = 1 << 20
RING = 4
TAIL = 8


def whole():
    return pl.BlockSpec(memory_space=pltpu.VMEM)


def scalars():
    return pl.BlockSpec(memory_space=pltpu.SMEM)


def position():
    return [lax.axis_index(a) for a in AXES]


def params(mib):
    return pltpu.CompilerParams(vmem_limit_bytes=mib * MIB)


def cost(flops, moved):
    return pl.CostEstimate(flops=flops, bytes_accessed=moved, transcendentals=0)


def place(z, c, x, y):
    return ((z % 4) * 2 + c) * 16 + (x % 4) * 4 + y % 4


def moves(shift):
    every = [(z, c, x, y) for z in range(4) for c in range(2) for x in range(4) for y in range(4)]
    return [(place(*d), place(*shift(*d))) for d in every]


def send(v, shift):
    return lax.ppermute(v, AXES, moves(shift))


def along_z(k):
    return lambda z, c, x, y: (z + k, c, x, y)


def other_core(z, c, x, y):
    return (z, 1 - c, x, y)


def first_axis(k):
    return lambda z, c, x, y: (z, c, x + k, y) if c == 0 else (z, c, x, y + k)


def second_axis(k):
    return lambda z, c, x, y: (z, c, x, y + k) if c == 0 else (z, c, x + k, y)


def screen_body(survive, half, *rest):
    outs, (held, turned, sems) = rest[:4], rest[4:]
    at = position()
    ao = half.shape[2]
    block = ao // survive.shape[2]
    chunks = sems.shape[0]
    lanes = ao // chunks
    copies = [
        pltpu.make_async_copy(half.at[:, :, cut], held.at[:, :, cut], sems.at[n])
        for n, cut in enumerate(slice(n * lanes, (n + 1) * lanes) for n in range(chunks))
    ]
    for copy in copies:
        copy.start()
    group = outs[0].shape[0]
    for n in range(chunks):
        copies[n].wait()
        for m in range(n * (lanes // block), (n + 1) * (lanes // block)):
            cut = slice(m * block, (m + 1) * block)
            keep = survive[0, 0, m].astype(F32)
            turned[:, :, cut] = jnp.swapaxes(held[:, :, cut].astype(F32) * keep, 0, 1).astype(BF)
        cut = slice(n * lanes, (n + 1) * lanes)
        for k in range(RING):
            outs[k][:, :, cut] = turned[pl.ds(lax.rem(at[0] + k, RING) * group, group), :, cut]


def screen(survive, half):
    aux, occ, ao = half.shape
    out = jax.ShapeDtypeStruct((occ // RING, aux, ao), BF)
    in_hbm = pl.BlockSpec(memory_space=pltpu.HBM)
    return pl.pallas_call(
        screen_body,
        out_shape=[out] * RING,
        in_specs=[scalars(), in_hbm],
        out_specs=[whole()] * RING,
        scratch_shapes=[
            pltpu.VMEM(half.shape, BF),
            pltpu.VMEM((occ, aux, ao), BF),
            pltpu.SemaphoreType.DMA((4,)),
        ],
        compiler_params=params(50),
        cost_estimate=cost(half.size, half.size * 4),
        name="screen",
    )(survive, half)


def join_body(*refs):
    metrics, mixed = refs[:4], refs[4]
    at = position()
    aux = metrics[0].shape[1]
    part = aux // 8
    metric = jnp.concatenate([m[...] for m in metrics], axis=0)
    source = lax.broadcasted_iota(jnp.int32, (aux, aux), 0)
    n = lax.broadcasted_iota(jnp.int32, (aux, aux), 1)
    slot = n // part
    up = lax.rem(at[0] - slot // 2 + RING, RING)
    core = jnp.where(slot % 2 == 0, at[1], 1 - at[1])
    wanted = (up * 2 + core) * part + n % part
    pick = jnp.where(source == wanted, 1.0, 0.0).astype(BF)
    mixed[...] = jnp.zeros_like(mixed)
    for n in range(2):
        cut = slice(n * aux, (n + 1) * aux)
        mixed[cut, cut] = jnp.dot(metric, pick, preferred_element_type=F32).astype(BF)


def join(metrics):
    aux = metrics[0].shape[1]
    return pl.pallas_call(
        join_body,
        out_shape=jax.ShapeDtypeStruct((2 * aux, 2 * aux), BF),
        in_specs=[whole()] * 4,
        out_specs=whole(),
        compiler_params=params(4),
        cost_estimate=cost(2 * aux**3, aux * aux * 4),
        name="join",
    )(*metrics)


def fit_body(*refs):
    pieces, mixed, (bulk, rest, turned, *far) = refs[:8], refs[8], refs[9:]
    at = position()
    step = pl.program_id(0)
    ao = turned.shape[0]
    aux = mixed.shape[0]
    screened = jnp.concatenate([p[n] for n in range(2) for p in pieces], axis=0)
    fitted = jnp.dot(mixed[...], screened, preferred_element_type=F32).astype(BF)
    wide, narrow = bulk.shape[1] // RING, rest.shape[1] // RING
    rows = pl.ds(pl.multiple_of(step * aux, aux), aux)

    def chosen(column, lanes):
        first, second = column, column + wide + narrow
        return jnp.where(at[1] == 0, fitted[:, first:first + lanes], fitted[:, second:second + lanes])

    for n in range(RING):
        bulk[rows, n * wide:(n + 1) * wide] = chosen(n * (ao // RING), wide)
        rest[rows, n * narrow:(n + 1) * narrow] = chosen(n * (ao // RING) + wide, narrow)
    flipped = fitted.T
    cut = pl.ds(pl.multiple_of(step * aux, aux), aux)
    high = ao // (RING * RING)
    for x in range(RING):
        for y in range(RING):
            n = x * RING + y
            to = jnp.where(at[1] == 0, n, y * RING + x) * high
            turned[pl.ds(pl.multiple_of(to, 64), high), cut] = flipped[n * high:(n + 1) * high]

    @pl.when(step == pl.num_programs(0) - 1)
    def _():
        bulk_body(FAR, bulk, turned, *far)


def fit(pieces, mixed):
    group, part, ao = pieces[0].shape
    aux, steps = 2 * part * 8, group // 2
    shapes = [((steps * aux, ao // 3), BF), ((steps * aux, ao // 6), BF), ((ao, steps * aux), BF)]
    shapes += [((ao // RING // 2 + TAIL, ao // 3), I16)] * 2
    return pl.pallas_call(
        fit_body,
        grid=(steps,),
        out_shape=[jax.ShapeDtypeStruct(*shape) for shape in shapes],
        in_specs=[pl.BlockSpec((2, part, ao), lambda i: (i, 0, 0))] * 8 + [whole()],
        out_specs=[pl.BlockSpec(shape, lambda i: (0, 0)) for shape, _ in shapes],
        compiler_params=params(36),
        cost_estimate=cost(2 * steps * aux * aux * ao + steps * aux * ao * ao // 6, steps * aux * ao * 6),
        name="fit",
    )(*pieces, mixed)


def exponent(top):
    return jnp.floor(14.9 - jnp.log2(jnp.maximum(top, 1e-30)))


def coded(v, e):
    return jnp.round(v * jnp.exp2(e)).astype(jnp.int32).astype(I16)


def marked(e):
    return jnp.broadcast_to(e, (TAIL, e.shape[1])).astype(jnp.int32).astype(I16)


def scale_of(tail):
    return jnp.exp2(-tail.astype(jnp.int32).astype(F32)[:1])


def plain(q):
    return q.astype(jnp.int32).astype(F32)


def write(out, first, block, tail=None):
    end = first + block.shape[0]
    if out.dtype == F32:
        out[first:end, :] = block
    else:
        e = exponent(jnp.max(jnp.abs(block), axis=0, keepdims=True))
        tail = end if tail is None else tail
        out[first:end, :] = coded(block, e)
        out[tail:tail + TAIL, :] = marked(e)


FAR = ((2, 0, False), (2, 1, False))


def bulk_body(blocks, bulk, turned, *refs):
    at = position()
    total = turned.shape[0] // RING
    own = jnp.where(at[1] == 0, at[2], at[3])
    outs = refs[len(refs) - len(blocks):]
    arrived = iter(refs)
    wide = bulk.shape[1] // 2
    for (shift, half, adds), out in zip(blocks, outs):
        rows = total if half is None else total // 2
        first = lax.rem(own + shift, RING) * total + (0 if half is None else half * rows)
        left = turned[pl.ds(pl.multiple_of(first, 128), rows), :]
        part = next(arrived) if adds else None
        for n in range(2):
            lanes = slice(n * wide, (n + 1) * wide)
            block = jnp.dot(left, bulk[:, lanes], preferred_element_type=F32)
            if adds:
                block = block + plain(part[:rows, lanes]) * scale_of(part[rows:, lanes])
            write(out.at[:, lanes], 0, block)


def bulk_k(bulk, turned, blocks, arrived=()):
    depth, columns = bulk.shape
    total = turned.shape[0] // RING
    sizes = [total if half is None else total // 2 for _, half, _ in blocks]
    return pl.pallas_call(
        functools.partial(bulk_body, blocks),
        out_shape=[
            jax.ShapeDtypeStruct((n + (TAIL if shift else 0), columns), I16 if shift else F32)
            for n, (shift, _, _) in zip(sizes, blocks)
        ],
        in_specs=[whole()] * (2 + len(arrived)),
        out_specs=[whole()] * len(blocks),
        compiler_params=params(28),
        cost_estimate=cost(2 * depth * sum(sizes) * columns, sum(sizes) * columns * 2),
    )(bulk, turned, *arrived)


def rest_body(steps, cut, rest, turned, *outs):
    at = position()
    narrow = rest.shape[1] // RING
    total = turned.shape[0] // RING
    right = jnp.concatenate(
        [rest[:, pl.ds(pl.multiple_of(lax.rem(at[0] + k, RING) * narrow, 128), narrow)] for k in steps], axis=1
    )
    for g in range(RING):
        block = jnp.dot(turned[g * total:(g + 1) * total, :], right, preferred_element_type=F32)
        for n in range(2):
            out = outs[cut[n][g // 2]]
            row = g if out.shape[0] == RING * total else g % 2
            write(out, row * total, block[:, n * narrow:(n + 1) * narrow], 2 * total + g % 2 * TAIL)


def rest_k(rest, turned, steps, cut, kinds):
    depth = rest.shape[0]
    ao = turned.shape[0]
    narrow = rest.shape[1] // RING
    shapes = {
        "message": ((ao // 2 + 2 * TAIL, narrow), I16), "half": ((ao // 2, narrow), F32), "all": ((ao, narrow), F32)
    }
    return pl.pallas_call(
        functools.partial(rest_body, steps, cut),
        out_shape=[jax.ShapeDtypeStruct(*shapes[kind]) for kind in kinds],
        in_specs=[whole()] * 2,
        out_specs=[whole()] * len(kinds),
        compiler_params=params(28),
        cost_estimate=cost(4 * depth * ao * narrow, ao * narrow * 4),
    )(rest, turned)


def rest_mid_body(*refs):
    for own, arrived, out in ((refs[0], refs[1], refs[4]), (refs[2], refs[3], refs[5])):
        total = own.shape[0] // 2
        for g in range(2):
            first, tail = g * total, 2 * total + g * TAIL
            v = own[first:first + total, :] + plain(arrived[first:first + total, :]) * scale_of(
                arrived[tail:tail + TAIL, :]
            )
            write(out, first, v, tail)


def rest_mid(up, arrived_up, down, arrived_down):
    shape = jax.ShapeDtypeStruct(arrived_up.shape, I16)
    return pl.pallas_call(
        rest_mid_body,
        out_shape=[shape] * 2,
        in_specs=[whole()] * 4,
        out_specs=[whole()] * 2,
        compiler_params=params(16),
        cost_estimate=cost(up.size * 16, up.size * 16),
        name="rest_mid",
    )(up, arrived_up, down, arrived_down)


def gathered(own, arrived, first, tail, row, lanes):
    v = own[pl.ds(pl.multiple_of(first[0] + row, 64), first[2]), lanes]
    for m in arrived:
        cut = pl.ds(pl.multiple_of(first[1] + row, 16), first[2])
        v = v + plain(m[cut, lanes]) * scale_of(m[tail:tail + TAIL, lanes])
    return v


def rest_second_body(own, a, b, d, e, after, kept, *outs):
    at = position()
    high = kept.shape[0]
    total, step = own.shape[0] // RING, own.shape[1]
    h = jnp.where(at[1] == 0, at[3], at[2])
    for k in range(RING):
        row = lax.rem(h + k, RING) * high
        out = kept if k == 0 else outs[k - 1]
        for n in range(RING):
            start, tail = n % 2 * total, 2 * total + n % 2 * TAIL
            v = gathered(own, (a, b) if n < 2 else (d, e), (n * total, start, high), tail, row, slice(0, step))
            write(out.at[:, n * step:(n + 1) * step], 0, v)


def rest_second(own, upper, lower, after):
    total, columns = own.shape
    high, every = total // RING // RING, columns * RING
    return list(pl.pallas_call(
        rest_second_body,
        out_shape=[jax.ShapeDtypeStruct((high, every), F32)]
        + [jax.ShapeDtypeStruct((high + TAIL, every), I16)] * 3,
        in_specs=[whole()] * 6,
        out_specs=[whole()] * 4,
        compiler_params=params(24),
        cost_estimate=cost(total * columns * 12, total * columns * 8),
        name="rest_second_sum",
    )(own, *upper, *lower, after))


def bulk_second_body(steps, own, a, b, d, e, after, *outs):
    at = position()
    high = own.shape[0] // RING
    h = jnp.where(at[1] == 0, at[3], at[2])
    half = own.shape[0] // 2
    step = 256
    for k, out in zip(steps, outs):
        block = lax.rem(h + k, RING)

        def part(upper, arrived, block=block, out=out):
            @pl.when((block < RING // 2) == upper)
            def _():
                row = pl.multiple_of(lax.rem(block, RING // 2) * high, 64)
                first = pl.multiple_of(block * high, 64)
                for lane in range(0, own.shape[1], step):
                    lanes = slice(lane, lane + step)
                    v = own[pl.ds(first, high), lanes]
                    for m in arrived:
                        v = v + plain(m[pl.ds(row, high), lanes]) * scale_of(m[half:, lanes])
                    write(out.at[:, lanes], 0, v)

        part(True, (a, b))
        part(False, (d, e))


def bulk_second(steps, own, upper, lower, after):
    total, columns = own.shape
    high = total // RING
    return list(pl.pallas_call(
        functools.partial(bulk_second_body, steps),
        out_shape=[
            jax.ShapeDtypeStruct((high + TAIL, columns), I16) if k else jax.ShapeDtypeStruct((high, columns), F32)
            for k in steps
        ],
        in_specs=[whole()] * 6,
        out_specs=[whole()] * len(steps),
        compiler_params=params(24),
        cost_estimate=cost(high * columns * 12 * len(steps), high * columns * 8 * len(steps)),
        name="bulk_second_sum",
    )(own, *upper, *lower, after))


def third_body(by_z, own, a, b, d, after, *outs):
    at = position()
    high, step = outs[0].shape
    start = at[0] if by_z else jnp.where(at[1] == 0, at[2], at[3])
    for k in range(RING):
        cut = pl.ds(pl.multiple_of(lax.rem(start + k, RING) * step, 128), step)
        write(outs[k], 0, gathered(own, (a, b, d), (0, 0, high), high, 0, cut))


def third(parts, by_z, after):
    high, every = parts[0].shape
    wide = every // RING
    return list(pl.pallas_call(
        functools.partial(third_body, by_z),
        out_shape=[jax.ShapeDtypeStruct((high, wide), F32)] + [jax.ShapeDtypeStruct((high + TAIL, wide), I16)] * 3,
        in_specs=[whole()] * 5,
        out_specs=[whole()] * 4,
        compiler_params=params(16),
        cost_estimate=cost(high * every * 16, high * every * 10),
        name="third_sum",
    )(*parts, after))


def tick_body(v, out):
    out[...] = v[...]


def tick(v):
    return pl.pallas_call(
        tick_body,
        out_shape=jax.ShapeDtypeStruct(v.shape, v.dtype),
        in_specs=[whole()],
        out_specs=whole(),
        compiler_params=params(1),
        cost_estimate=cost(1000, 32),
        name="tick",
    )(v)


def finish_body(own, a, b, d, rest, ra, rb, rd, out):
    high, wide = own.shape
    for first, v, arrived in ((0, own[...], (a, b, d)), (wide, rest[...], (ra, rb, rd))):
        for m in arrived:
            v = v + plain(m[:high, :]) * scale_of(m[high:, :])
        out[:, first:first + v.shape[1]] = v


def finish(bulk, rest):
    high = bulk[0].shape[0]
    ao = bulk[0].shape[1] + rest[0].shape[1]
    return pl.pallas_call(
        finish_body,
        out_shape=jax.ShapeDtypeStruct((high, ao), F32),
        in_specs=[whole()] * 8,
        out_specs=whole(),
        compiler_params=params(8),
        cost_estimate=cost(high * ao * 8, high * ao * 14),
    )(*bulk, *rest)


def shards(half, metric, survive):
    parts = screen(survive, half)
    here = [parts[0]] + [None] * 3
    for k in (2, 1, 3):
        here[k] = send(parts[k], along_z(k))
    pair = jnp.concatenate([metric, send(metric, other_core)], axis=0)
    metrics = [pair] + [None] * 3
    for k in (1, 2, 3):
        metrics[k] = send(pair, along_z(k))
    mixed = join(metrics)
    there = [None] * 4
    for k in (0, 2, 1, 3):
        there[k] = send(here[k], other_core)
    bulk_rows, rest_rows, turned, *far = fit([v for both in zip(here, there) for v in both], mixed)

    def bulk_step(*blocks, arrived=()):
        return bulk_k(bulk_rows, turned, blocks, arrived)

    def rest_step(*how):
        return rest_k(rest_rows, turned, *how)

    def near(axis, up, down):
        up = send(up, axis(1))
        down = send(down, axis(3))
        return up, down

    def onward(parts, shift):
        for k in (1, 2, 3):
            parts[k] = send(parts[k], shift(k))

    far = near(first_axis, *far)
    upper, lower, rest_own = rest_step((2, 0), ((0, 1), (2, 2)), ("message", "message", "all"))
    rest_far = near(along_z, upper, lower)
    lower_up, upper_down = near(first_axis, *bulk_step((1, 1, False), (3, 0, False)))
    keep_up, up, down, keep_down = rest_step((1, 3), ((0, 1), (2, 3)), ("half", "message", "message", "half"))
    rest_near = near(along_z, up, down)
    upper_up, lower_down = near(first_axis, *bulk_step((1, 0, True), (3, 1, True), arrived=far))
    up, down = rest_mid(keep_up, rest_far[0], keep_down, rest_far[1])
    mid = near(along_z, up, down)
    own = bulk_step((0, None, False))[0]
    arrived = own, (upper_up, upper_down), (lower_up, lower_down), metric
    bulk = [None] * 4
    (bulk[2],) = bulk_second((2,), *arrived)
    bulk[0], bulk[1], bulk[3] = bulk_second((0, 1, 3), *arrived)
    onward(bulk, second_axis)
    then = tick(metric)
    rest = rest_second(rest_own, (mid[0], rest_near[1]), (rest_near[0], mid[1]), then)
    onward(rest, second_axis)
    then = tick(then)
    bulk = third(bulk, True, then)
    onward(bulk, along_z)
    then = tick(then)
    rest = third(rest, False, then)
    onward(rest, first_axis)
    return finish(bulk, rest)


def solution(mesh):
    finer = Mesh(mesh.devices.reshape(4, 2, 4, 4), AXES)
    placed = (P(("z", "c"), ("x", "y"), None), P(("z", "c"), None), P(("z", "c"), ("x", "y"), None))
    return jax.shard_map(shards, mesh=finer, in_specs=placed, out_specs=P(("x", "y"), ("z", "c")), check_vma=False)
```

```python
import functools

import jax
import jax.numpy as jnp
from jax import lax
from jax.experimental import pallas as pl
from jax.experimental.pallas import tpu as pltpu
from jax.sharding import Mesh
from jax.sharding import PartitionSpec as P


AXES = ("z", "c", "x", "y")
BF = jnp.bfloat16
F32 = jnp.float32
I16 = jnp.int16
MIB = 1 << 20
RING = 4
TAIL = 8


def whole():
    return pl.BlockSpec(memory_space=pltpu.VMEM)


def scalars():
    return pl.BlockSpec(memory_space=pltpu.SMEM)


def position():
    return [lax.axis_index(a) for a in AXES]


def params(mib):
    return pltpu.CompilerParams(vmem_limit_bytes=mib * MIB)


def cost(flops, moved):
    return pl.CostEstimate(flops=flops, bytes_accessed=moved, transcendentals=0)


def place(z, c, x, y):
    return ((z % 4) * 2 + c) * 16 + (x % 4) * 4 + y % 4


def moves(shift):
    every = [(z, c, x, y) for z in range(4) for c in range(2) for x in range(4) for y in range(4)]
    return [(place(*d), place(*shift(*d))) for d in every]


def send(v, shift):
    return lax.ppermute(v, AXES, moves(shift))


def along_z(k):
    return lambda z, c, x, y: (z + k, c, x, y)


def other_core(z, c, x, y):
    return (z, 1 - c, x, y)


def first_axis(k):
    return lambda z, c, x, y: (z, c, x + k, y) if c == 0 else (z, c, x, y + k)


def second_axis(k):
    return lambda z, c, x, y: (z, c, x, y + k) if c == 0 else (z, c, x + k, y)


def screen_body(survive, half, *rest):
    outs, (held, turned, sems) = rest[:4], rest[4:]
    at = position()
    ao = half.shape[2]
    block = ao // survive.shape[2]
    chunks = sems.shape[0]
    lanes = ao // chunks
    copies = [
        pltpu.make_async_copy(half.at[:, :, cut], held.at[:, :, cut], sems.at[n])
        for n, cut in enumerate(slice(n * lanes, (n + 1) * lanes) for n in range(chunks))
    ]
    for copy in copies:
        copy.start()
    for n in range(chunks):
        copies[n].wait()

        def step(m, carry):
            m = n * (lanes // block) + m
            cut = pl.ds(pl.multiple_of(m * block, block), block)
            keep = survive[0, 0, m].astype(F32)
            turned[:, :, cut] = jnp.swapaxes(held[:, :, cut].astype(F32) * keep, 0, 1).astype(BF)
            return carry

        lax.fori_loop(0, lanes // block, step, 0, unroll=True)
    group = outs[0].shape[0]
    for k in range(RING):
        first = lax.rem(at[0] + k, RING) * group
        outs[k][...] = turned[pl.ds(first, group)]


def screen(survive, half):
    aux, occ, ao = half.shape
    out = jax.ShapeDtypeStruct((occ // RING, aux, ao), BF)
    in_hbm = pl.BlockSpec(memory_space=pltpu.HBM)
    return pl.pallas_call(
        screen_body,
        out_shape=[out] * RING,
        in_specs=[scalars(), in_hbm],
        out_specs=[whole()] * RING,
        scratch_shapes=[
            pltpu.VMEM(half.shape, BF),
            pltpu.VMEM((occ, aux, ao), BF),
            pltpu.SemaphoreType.DMA((4,)),
        ],
        compiler_params=params(50),
        cost_estimate=cost(half.size, half.size * 4),
        name="screen",
    )(survive, half)


def join_body(*refs):
    metrics, mixed = refs[:4], refs[4]
    at = position()
    aux = metrics[0].shape[1]
    part = aux // 8
    metric = jnp.concatenate([m[...] for m in metrics], axis=0)
    source = lax.broadcasted_iota(jnp.int32, (aux, aux), 0)
    n = lax.broadcasted_iota(jnp.int32, (aux, aux), 1)
    slot = n // part
    up = lax.rem(at[0] - slot // 2 + RING, RING)
    core = jnp.where(slot % 2 == 0, at[1], 1 - at[1])
    wanted = (up * 2 + core) * part + n % part
    pick = jnp.where(source == wanted, 1.0, 0.0).astype(BF)
    mixed[...] = jnp.zeros_like(mixed)
    for n in range(2):
        cut = slice(n * aux, (n + 1) * aux)
        mixed[cut, cut] = jnp.dot(metric, pick, preferred_element_type=F32).astype(BF)


def join(metrics):
    aux = metrics[0].shape[1]
    return pl.pallas_call(
        join_body,
        out_shape=jax.ShapeDtypeStruct((2 * aux, 2 * aux), BF),
        in_specs=[whole()] * 4,
        out_specs=whole(),
        compiler_params=params(4),
        cost_estimate=cost(2 * aux**3, aux * aux * 4),
        name="join",
    )(*metrics)


def fit_body(*refs):
    pieces, mixed, (bulk, rest, turned, *far) = refs[:8], refs[8], refs[9:]
    at = position()
    step = pl.program_id(0)
    ao = turned.shape[0]
    aux = mixed.shape[0]
    screened = jnp.concatenate([p[n] for n in range(2) for p in pieces], axis=0)
    fitted = jnp.dot(mixed[...], screened, preferred_element_type=F32).astype(BF)
    wide, narrow = bulk.shape[1] // RING, rest.shape[1] // RING
    rows = pl.ds(pl.multiple_of(step * aux, aux), aux)

    def chosen(column, lanes):
        first, second = column, column + wide + narrow
        return jnp.where(at[1] == 0, fitted[:, first:first + lanes], fitted[:, second:second + lanes])

    for n in range(RING):
        bulk[rows, n * wide:(n + 1) * wide] = chosen(n * (ao // RING), wide)
        rest[rows, n * narrow:(n + 1) * narrow] = chosen(n * (ao // RING) + wide, narrow)
    flipped = fitted.T
    cut = pl.ds(pl.multiple_of(step * aux, aux), aux)
    high = ao // (RING * RING)
    for x in range(RING):
        for y in range(RING):
            n = x * RING + y
            to = jnp.where(at[1] == 0, n, y * RING + x) * high
            turned[pl.ds(pl.multiple_of(to, 64), high), cut] = flipped[n * high:(n + 1) * high]

    @pl.when(step == pl.num_programs(0) - 1)
    def _():
        bulk_body(FAR, bulk, turned, *far)


def fit(pieces, mixed):
    group, part, ao = pieces[0].shape
    aux, steps = 2 * part * 8, group // 2
    shapes = [((steps * aux, ao // 3), BF), ((steps * aux, ao // 6), BF), ((ao, steps * aux), BF)]
    shapes += [((ao // RING // 2 + TAIL, ao // 3), I16)] * 2
    return pl.pallas_call(
        fit_body,
        grid=(steps,),
        out_shape=[jax.ShapeDtypeStruct(*shape) for shape in shapes],
        in_specs=[pl.BlockSpec((2, part, ao), lambda i: (i, 0, 0))] * 8 + [whole()],
        out_specs=[pl.BlockSpec(shape, lambda i: (0, 0)) for shape, _ in shapes],
        compiler_params=params(36),
        cost_estimate=cost(2 * steps * aux * aux * ao + steps * aux * ao * ao // 6, steps * aux * ao * 6),
        name="fit",
    )(*pieces, mixed)


def exponent(top):
    return jnp.floor(14.9 - jnp.log2(jnp.maximum(top, 1e-33)))


def coded(v, e):
    return jnp.round(v * jnp.exp2(e)).astype(jnp.int32).astype(I16)


def marked(e):
    return jnp.broadcast_to(e, (TAIL, e.shape[1])).astype(jnp.int32).astype(I16)


def scale_of(tail):
    return jnp.exp2(-tail.astype(jnp.int32).astype(F32)[:1])


def plain(q):
    return q.astype(jnp.int32).astype(F32)


def write(out, first, block, tail=None):
    end = first + block.shape[0]
    if out.dtype == F32:
        out[first:end, :] = block
    else:
        e = exponent(jnp.max(jnp.abs(block), axis=0, keepdims=True))
        tail = end if tail is None else tail
        out[first:end, :] = coded(block, e)
        out[tail:tail + TAIL, :] = marked(e)


FAR = ((2, 0, False), (2, 1, False))


def bulk_body(blocks, bulk, turned, *refs):
    at = position()
    total = turned.shape[0] // RING
    own = jnp.where(at[1] == 0, at[2], at[3])
    outs = refs[len(refs) - len(blocks):]
    arrived = iter(refs)
    wide = bulk.shape[1] // 2
    for (shift, half, adds), out in zip(blocks, outs):
        rows = total if half is None else total // 2
        first = lax.rem(own + shift, RING) * total + (0 if half is None else half * rows)
        left = turned[pl.ds(pl.multiple_of(first, 128), rows), :]
        part = next(arrived) if adds else None
        for n in range(2):
            lanes = slice(n * wide, (n + 1) * wide)
            block = jnp.dot(left, bulk[:, lanes], preferred_element_type=F32)
            if adds:
                block = block + plain(part[:rows, lanes]) * scale_of(part[rows:, lanes])
            write(out.at[:, lanes], 0, block)


def bulk_k(bulk, turned, blocks, arrived=()):
    depth, columns = bulk.shape
    total = turned.shape[0] // RING
    sizes = [total if half is None else total // 2 for _, half, _ in blocks]
    return pl.pallas_call(
        functools.partial(bulk_body, blocks),
        out_shape=[
            jax.ShapeDtypeStruct((n + (TAIL if shift else 0), columns), I16 if shift else F32)
            for n, (shift, _, _) in zip(sizes, blocks)
        ],
        in_specs=[whole()] * (2 + len(arrived)),
        out_specs=[whole()] * len(blocks),
        compiler_params=params(28),
        cost_estimate=cost(2 * depth * sum(sizes) * columns, sum(sizes) * columns * 2),
    )(bulk, turned, *arrived)


def rest_body(steps, cut, rest, turned, *outs):
    at = position()
    narrow = rest.shape[1] // RING
    total = turned.shape[0] // RING
    right = jnp.concatenate(
        [rest[:, pl.ds(pl.multiple_of(lax.rem(at[0] + k, RING) * narrow, 128), narrow)] for k in steps], axis=1
    )
    for g in range(RING):
        block = jnp.dot(turned[g * total:(g + 1) * total, :], right, preferred_element_type=F32)
        for n in range(2):
            out = outs[cut[n][g // 2]]
            row = g if out.shape[0] == RING * total else g % 2
            write(out, row * total, block[:, n * narrow:(n + 1) * narrow], 2 * total + g % 2 * TAIL)


def rest_k(rest, turned, steps, cut, kinds):
    depth = rest.shape[0]
    ao = turned.shape[0]
    narrow = rest.shape[1] // RING
    shapes = {
        "message": ((ao // 2 + 2 * TAIL, narrow), I16), "half": ((ao // 2, narrow), F32), "all": ((ao, narrow), F32)
    }
    return pl.pallas_call(
        functools.partial(rest_body, steps, cut),
        out_shape=[jax.ShapeDtypeStruct(*shapes[kind]) for kind in kinds],
        in_specs=[whole()] * 2,
        out_specs=[whole()] * len(kinds),
        compiler_params=params(28),
        cost_estimate=cost(4 * depth * ao * narrow, ao * narrow * 4),
    )(rest, turned)


def rest_mid_body(*refs):
    for own, arrived, out in ((refs[0], refs[1], refs[4]), (refs[2], refs[3], refs[5])):
        total = own.shape[0] // 2
        for g in range(2):
            first, tail = g * total, 2 * total + g * TAIL
            v = own[first:first + total, :] + plain(arrived[first:first + total, :]) * scale_of(
                arrived[tail:tail + TAIL, :]
            )
            write(out, first, v, tail)


def rest_mid(up, arrived_up, down, arrived_down):
    shape = jax.ShapeDtypeStruct(arrived_up.shape, I16)
    return pl.pallas_call(
        rest_mid_body,
        out_shape=[shape] * 2,
        in_specs=[whole()] * 4,
        out_specs=[whole()] * 2,
        compiler_params=params(16),
        cost_estimate=cost(up.size * 16, up.size * 16),
        name="rest_mid",
    )(up, arrived_up, down, arrived_down)


def gathered(own, arrived, first, tail, row, lanes):
    v = own[pl.ds(pl.multiple_of(first[0] + row, 64), first[2]), lanes]
    for m in arrived:
        cut = pl.ds(pl.multiple_of(first[1] + row, 16), first[2])
        v = v + plain(m[cut, lanes]) * scale_of(m[tail:tail + TAIL, lanes])
    return v


def rest_second_body(own, a, b, d, e, after, kept, *outs):
    at = position()
    high = kept.shape[0]
    total, step = own.shape[0] // RING, own.shape[1]
    h = jnp.where(at[1] == 0, at[3], at[2])
    for k in range(RING):
        row = lax.rem(h + k, RING) * high
        out = kept if k == 0 else outs[k - 1]
        for n in range(RING):
            start, tail = n % 2 * total, 2 * total + n % 2 * TAIL
            v = gathered(own, (a, b) if n < 2 else (d, e), (n * total, start, high), tail, row, slice(0, step))
            write(out.at[:, n * step:(n + 1) * step], 0, v)


def rest_second(own, upper, lower, after):
    total, columns = own.shape
    high, every = total // RING // RING, columns * RING
    return list(pl.pallas_call(
        rest_second_body,
        out_shape=[jax.ShapeDtypeStruct((high, every), F32)]
        + [jax.ShapeDtypeStruct((high + TAIL, every), I16)] * 3,
        in_specs=[whole()] * 6,
        out_specs=[whole()] * 4,
        compiler_params=params(24),
        cost_estimate=cost(total * columns * 12, total * columns * 8),
        name="rest_second_sum",
    )(own, *upper, *lower, after))


def bulk_second_body(steps, own, a, b, d, e, after, *outs):
    at = position()
    high = own.shape[0] // RING
    h = jnp.where(at[1] == 0, at[3], at[2])
    half = own.shape[0] // 2
    step = 256
    for k, out in zip(steps, outs):
        block = lax.rem(h + k, RING)

        def part(upper, arrived, block=block, out=out):
            @pl.when((block < RING // 2) == upper)
            def _():
                row = pl.multiple_of(lax.rem(block, RING // 2) * high, 64)
                first = pl.multiple_of(block * high, 64)
                for lane in range(0, own.shape[1], step):
                    lanes = slice(lane, lane + step)
                    v = own[pl.ds(first, high), lanes]
                    for m in arrived:
                        v = v + plain(m[pl.ds(row, high), lanes]) * scale_of(m[half:, lanes])
                    write(out.at[:, lanes], 0, v)

        part(True, (a, b))
        part(False, (d, e))


def bulk_second(steps, own, upper, lower, after):
    total, columns = own.shape
    high = total // RING
    return list(pl.pallas_call(
        functools.partial(bulk_second_body, steps),
        out_shape=[
            jax.ShapeDtypeStruct((high + TAIL, columns), I16) if k else jax.ShapeDtypeStruct((high, columns), F32)
            for k in steps
        ],
        in_specs=[whole()] * 6,
        out_specs=[whole()] * len(steps),
        compiler_params=params(24),
        cost_estimate=cost(high * columns * 12 * len(steps), high * columns * 8 * len(steps)),
        name="bulk_second_sum",
    )(own, *upper, *lower, after))


def third_body(by_z, own, a, b, d, after, *outs):
    at = position()
    high, step = outs[0].shape
    start = at[0] if by_z else jnp.where(at[1] == 0, at[2], at[3])
    for k in range(RING):
        cut = pl.ds(pl.multiple_of(lax.rem(start + k, RING) * step, 128), step)
        write(outs[k], 0, gathered(own, (a, b, d), (0, 0, high), high, 0, cut))


def third(parts, by_z, after):
    high, every = parts[0].shape
    wide = every // RING
    return list(pl.pallas_call(
        functools.partial(third_body, by_z),
        out_shape=[jax.ShapeDtypeStruct((high, wide), F32)] + [jax.ShapeDtypeStruct((high + TAIL, wide), I16)] * 3,
        in_specs=[whole()] * 5,
        out_specs=[whole()] * 4,
        compiler_params=params(16),
        cost_estimate=cost(high * every * 16, high * every * 10),
        name="third_sum",
    )(*parts, after))


def tick_body(v, out):
    out[...] = v[...]


def tick(v):
    return pl.pallas_call(
        tick_body,
        out_shape=jax.ShapeDtypeStruct(v.shape, v.dtype),
        in_specs=[whole()],
        out_specs=whole(),
        compiler_params=params(1),
        cost_estimate=cost(1000, 32),
        name="tick",
    )(v)


def finish_body(own, a, b, d, rest, ra, rb, rd, out):
    high, wide = own.shape
    for first, v, arrived in ((0, own[...], (a, b, d)), (wide, rest[...], (ra, rb, rd))):
        for m in arrived:
            v = v + plain(m[:high, :]) * scale_of(m[high:, :])
        out[:, first:first + v.shape[1]] = v


def finish(bulk, rest):
    high = bulk[0].shape[0]
    ao = bulk[0].shape[1] + rest[0].shape[1]
    return pl.pallas_call(
        finish_body,
        out_shape=jax.ShapeDtypeStruct((high, ao), F32),
        in_specs=[whole()] * 8,
        out_specs=whole(),
        compiler_params=params(8),
        cost_estimate=cost(high * ao * 8, high * ao * 14),
    )(*bulk, *rest)


def shards(half, metric, survive):
    parts = screen(survive, half)
    here = [parts[0]] + [None] * 3
    for k in (2, 1, 3):
        here[k] = send(parts[k], along_z(k))
    pair = jnp.concatenate([metric, send(metric, other_core)], axis=0)
    metrics = [pair] + [None] * 3
    for k in (1, 2, 3):
        metrics[k] = send(pair, along_z(k))
    mixed = join(metrics)
    there = [None] * 4
    for k in (0, 2, 1, 3):
        there[k] = send(here[k], other_core)
    bulk_rows, rest_rows, turned, *far = fit([v for both in zip(here, there) for v in both], mixed)

    def bulk_step(*blocks, arrived=()):
        return bulk_k(bulk_rows, turned, blocks, arrived)

    def rest_step(*how):
        return rest_k(rest_rows, turned, *how)

    def near(axis, up, down):
        up = send(up, axis(1))
        down = send(down, axis(3))
        return up, down

    def onward(parts, shift):
        for k in (1, 2, 3):
            parts[k] = send(parts[k], shift(k))

    far = near(first_axis, *far)
    upper, lower, rest_own = rest_step((2, 0), ((0, 1), (2, 2)), ("message", "message", "all"))
    rest_far = near(along_z, upper, lower)
    lower_up, upper_down = near(first_axis, *bulk_step((1, 1, False), (3, 0, False)))
    keep_up, up, down, keep_down = rest_step((1, 3), ((0, 1), (2, 3)), ("half", "message", "message", "half"))
    rest_near = near(along_z, up, down)
    upper_up, lower_down = near(first_axis, *bulk_step((1, 0, True), (3, 1, True), arrived=far))
    up, down = rest_mid(keep_up, rest_far[0], keep_down, rest_far[1])
    mid = near(along_z, up, down)
    own = bulk_step((0, None, False))[0]
    arrived = own, (upper_up, upper_down), (lower_up, lower_down), metric
    bulk = [None] * 4
    (bulk[2],) = bulk_second((2,), *arrived)
    bulk[0], bulk[1], bulk[3] = bulk_second((0, 1, 3), *arrived)
    onward(bulk, second_axis)
    then = tick(metric)
    rest = rest_second(rest_own, (mid[0], rest_near[1]), (rest_near[0], mid[1]), then)
    onward(rest, second_axis)
    then = tick(then)
    bulk = third(bulk, True, then)
    onward(bulk, along_z)
    then = tick(then)
    rest = third(rest, False, then)
    onward(rest, first_axis)
    return finish(bulk, rest)


def solution(mesh):
    finer = Mesh(mesh.devices.reshape(4, 2, 4, 4), AXES)
    placed = (P(("z", "c"), ("x", "y"), None), P(("z", "c"), None), P(("z", "c"), ("x", "y"), None))
    return jax.shard_map(shards, mesh=finer, in_specs=placed, out_specs=P(("x", "y"), ("z", "c")), check_vma=False)
```

```python
import functools

import jax
import jax.numpy as jnp
from jax import lax
from jax.experimental import pallas as pl
from jax.experimental.pallas import tpu as pltpu
from jax.sharding import Mesh
from jax.sharding import PartitionSpec as P


AXES = ("z", "c", "x", "y")
BF = jnp.bfloat16
F32 = jnp.float32
I16 = jnp.int16
MIB = 1 << 20
RING = 4
TAIL = 8


def whole():
    return pl.BlockSpec(memory_space=pltpu.VMEM)


def scalars():
    return pl.BlockSpec(memory_space=pltpu.SMEM)


def position():
    return [lax.axis_index(a) for a in AXES]


def params(mib):
    return pltpu.CompilerParams(vmem_limit_bytes=mib * MIB)


def cost(flops, moved):
    return pl.CostEstimate(flops=flops, bytes_accessed=moved, transcendentals=0)


def place(z, c, x, y):
    return ((z % 4) * 2 + c) * 16 + (x % 4) * 4 + y % 4


def moves(shift):
    every = [(z, c, x, y) for z in range(4) for c in range(2) for x in range(4) for y in range(4)]
    return [(place(*d), place(*shift(*d))) for d in every]


def send(v, shift):
    return lax.ppermute(v, AXES, moves(shift))


def along_z(k):
    return lambda z, c, x, y: (z + k, c, x, y)


def other_core(z, c, x, y):
    return (z, 1 - c, x, y)


def first_axis(k):
    return lambda z, c, x, y: (z, c, x + k, y) if c == 1 else (z, c, x, y + k)


def second_axis(k):
    return lambda z, c, x, y: (z, c, x, y + k) if c == 1 else (z, c, x + k, y)


def screen_body(survive, half, *rest):
    outs, (held, turned, sems) = rest[:4], rest[4:]
    at = position()
    ao = half.shape[2]
    block = ao // survive.shape[2]
    chunks = sems.shape[0]
    lanes = ao // chunks
    copies = [
        pltpu.make_async_copy(half.at[:, :, cut], held.at[:, :, cut], sems.at[n])
        for n, cut in enumerate(slice(n * lanes, (n + 1) * lanes) for n in range(chunks))
    ]
    for copy in copies:
        copy.start()
    for n in range(chunks):
        copies[n].wait()

        def step(m, carry):
            m = n * (lanes // block) + m
            cut = pl.ds(pl.multiple_of(m * block, block), block)
            keep = survive[0, 0, m].astype(F32)
            turned[:, :, cut] = jnp.swapaxes(held[:, :, cut].astype(F32) * keep, 0, 1).astype(BF)
            return carry

        lax.fori_loop(0, lanes // block, step, 0, unroll=True)
    group = outs[0].shape[0]
    for k in range(RING):
        first = lax.rem(at[0] + k, RING) * group
        outs[k][...] = turned[pl.ds(first, group)]


def screen(survive, half):
    aux, occ, ao = half.shape
    out = jax.ShapeDtypeStruct((occ // RING, aux, ao), BF)
    in_hbm = pl.BlockSpec(memory_space=pltpu.HBM)
    return pl.pallas_call(
        screen_body,
        out_shape=[out] * RING,
        in_specs=[scalars(), in_hbm],
        out_specs=[whole()] * RING,
        scratch_shapes=[
            pltpu.VMEM(half.shape, BF),
            pltpu.VMEM((occ, aux, ao), BF),
            pltpu.SemaphoreType.DMA((8,)),
        ],
        compiler_params=params(50),
        cost_estimate=cost(half.size, half.size * 4),
        name="screen",
    )(survive, half)


def join_body(*refs):
    metrics, mixed = refs[:4], refs[4]
    at = position()
    aux = metrics[0].shape[1]
    part = aux // 8
    metric = jnp.concatenate([m[...] for m in metrics], axis=0)
    source = lax.broadcasted_iota(jnp.int32, (aux, aux), 0)
    n = lax.broadcasted_iota(jnp.int32, (aux, aux), 1)
    slot = n // part
    up = lax.rem(at[0] - slot // 2 + RING, RING)
    core = jnp.where(slot % 2 == 0, at[1], 1 - at[1])
    wanted = (up * 2 + core) * part + n % part
    pick = jnp.where(source == wanted, 1.0, 0.0).astype(BF)
    mixed[...] = jnp.zeros_like(mixed)
    for n in range(2):
        cut = slice(n * aux, (n + 1) * aux)
        mixed[cut, cut] = jnp.dot(metric, pick, preferred_element_type=F32).astype(BF)


def join(metrics):
    aux = metrics[0].shape[1]
    return pl.pallas_call(
        join_body,
        out_shape=jax.ShapeDtypeStruct((2 * aux, 2 * aux), BF),
        in_specs=[whole()] * 4,
        out_specs=whole(),
        compiler_params=params(4),
        cost_estimate=cost(2 * aux**3, aux * aux * 4),
        name="join",
    )(*metrics)


def fit_body(*refs):
    pieces, mixed, (bulk, rest, turned, *far) = refs[:8], refs[8], refs[9:]
    at = position()
    step = pl.program_id(0)
    ao = turned.shape[0]
    aux = mixed.shape[0]
    screened = jnp.concatenate([p[n] for n in range(2) for p in pieces], axis=0)
    fitted = jnp.dot(mixed[...], screened, preferred_element_type=F32).astype(BF)
    wide, narrow = bulk.shape[1] // RING, rest.shape[1] // RING
    rows = pl.ds(pl.multiple_of(step * aux, aux), aux)

    def chosen(column, lanes):
        first, second = column, column + wide + narrow
        return jnp.where(at[1] == 0, fitted[:, first:first + lanes], fitted[:, second:second + lanes])

    for n in range(RING):
        bulk[rows, n * wide:(n + 1) * wide] = chosen(n * (ao // RING), wide)
        rest[rows, n * narrow:(n + 1) * narrow] = chosen(n * (ao // RING) + wide, narrow)
    flipped = fitted.T
    cut = pl.ds(pl.multiple_of(step * aux, aux), aux)
    high = ao // (RING * RING)
    for x in range(RING):
        for y in range(RING):
            n = x * RING + y
            to = jnp.where(at[1] == 1, n, y * RING + x) * high
            turned[pl.ds(pl.multiple_of(to, 64), high), cut] = flipped[n * high:(n + 1) * high]

    @pl.when(step == pl.num_programs(0) - 1)
    def _():
        bulk_body(FAR, bulk, turned, *far)


def fit(pieces, mixed):
    group, part, ao = pieces[0].shape
    aux, steps = 2 * part * 8, group // 2
    shapes = [((steps * aux, ao // 3), BF), ((steps * aux, ao // 6), BF), ((ao, steps * aux), BF)]
    shapes += [((ao // RING // 2 + TAIL, ao // 3), I16)] * 2
    return pl.pallas_call(
        fit_body,
        grid=(steps,),
        out_shape=[jax.ShapeDtypeStruct(*shape) for shape in shapes],
        in_specs=[pl.BlockSpec((2, part, ao), lambda i: (i, 0, 0))] * 8 + [whole()],
        out_specs=[pl.BlockSpec(shape, lambda i: (0, 0)) for shape, _ in shapes],
        compiler_params=params(36),
        cost_estimate=cost(2 * steps * aux * aux * ao + steps * aux * ao * ao // 6, steps * aux * ao * 6),
        name="fit",
    )(*pieces, mixed)


def exponent(top):
    return jnp.floor(14.9 - jnp.log2(jnp.maximum(top, 1e-33)))


def coded(v, e):
    return jnp.round(v * jnp.exp2(e)).astype(jnp.int32).astype(I16)


def marked(e):
    return jnp.broadcast_to(e, (TAIL, e.shape[1])).astype(jnp.int32).astype(I16)


def scale_of(tail):
    return jnp.exp2(-tail.astype(jnp.int32).astype(F32)[:1])


def plain(q):
    return q.astype(jnp.int32).astype(F32)


def write(out, first, block, tail=None):
    end = first + block.shape[0]
    if out.dtype == F32:
        out[first:end, :] = block
    else:
        e = exponent(jnp.max(jnp.abs(block), axis=0, keepdims=True))
        tail = end if tail is None else tail
        out[first:end, :] = coded(block, e)
        out[tail:tail + TAIL, :] = marked(e)


FAR = ((2, 0, False), (2, 1, False))


def bulk_body(blocks, bulk, turned, *refs):
    at = position()
    total = turned.shape[0] // RING
    own = jnp.where(at[1] == 1, at[2], at[3])
    outs = refs[len(refs) - len(blocks):]
    arrived = iter(refs)
    wide = bulk.shape[1] // 2
    for (shift, half, adds), out in zip(blocks, outs):
        rows = total if half is None else total // 2
        first = lax.rem(own + shift, RING) * total + (0 if half is None else half * rows)
        left = turned[pl.ds(pl.multiple_of(first, 128), rows), :]
        part = next(arrived) if adds else None
        for n in range(2):
            lanes = slice(n * wide, (n + 1) * wide)
            block = jnp.dot(left, bulk[:, lanes], preferred_element_type=F32)
            if adds:
                block = block + plain(part[:rows, lanes]) * scale_of(part[rows:, lanes])
            write(out.at[:, lanes], 0, block)


def bulk_k(bulk, turned, blocks, arrived=()):
    depth, columns = bulk.shape
    total = turned.shape[0] // RING
    sizes = [total if half is None else total // 2 for _, half, _ in blocks]
    return pl.pallas_call(
        functools.partial(bulk_body, blocks),
        out_shape=[
            jax.ShapeDtypeStruct((n + (TAIL if shift else 0), columns), I16 if shift else F32)
            for n, (shift, _, _) in zip(sizes, blocks)
        ],
        in_specs=[whole()] * (2 + len(arrived)),
        out_specs=[whole()] * len(blocks),
        compiler_params=params(28),
        cost_estimate=cost(2 * depth * sum(sizes) * columns, sum(sizes) * columns * 2),
    )(bulk, turned, *arrived)


def rest_body(steps, cut, rest, turned, *outs):
    at = position()
    narrow = rest.shape[1] // RING
    total = turned.shape[0] // RING
    right = jnp.concatenate(
        [rest[:, pl.ds(pl.multiple_of(lax.rem(at[0] + k, RING) * narrow, 128), narrow)] for k in steps], axis=1
    )
    for g in range(RING):
        block = jnp.dot(turned[g * total:(g + 1) * total, :], right, preferred_element_type=F32)
        for n in range(2):
            out = outs[cut[n][g // 2]]
            row = g if out.shape[0] == RING * total else g % 2
            write(out, row * total, block[:, n * narrow:(n + 1) * narrow], 2 * total + g % 2 * TAIL)


def rest_k(rest, turned, steps, cut, kinds):
    depth = rest.shape[0]
    ao = turned.shape[0]
    narrow = rest.shape[1] // RING
    shapes = {
        "message": ((ao // 2 + 2 * TAIL, narrow), I16), "half": ((ao // 2, narrow), F32), "all": ((ao, narrow), F32)
    }
    return pl.pallas_call(
        functools.partial(rest_body, steps, cut),
        out_shape=[jax.ShapeDtypeStruct(*shapes[kind]) for kind in kinds],
        in_specs=[whole()] * 2,
        out_specs=[whole()] * len(kinds),
        compiler_params=params(28),
        cost_estimate=cost(4 * depth * ao * narrow, ao * narrow * 4),
    )(rest, turned)


def rest_mid_body(*refs):
    for own, arrived, out in ((refs[0], refs[1], refs[4]), (refs[2], refs[3], refs[5])):
        total = own.shape[0] // 2
        for g in range(2):
            first, tail = g * total, 2 * total + g * TAIL
            v = own[first:first + total, :] + plain(arrived[first:first + total, :]) * scale_of(
                arrived[tail:tail + TAIL, :]
            )
            write(out, first, v, tail)


def rest_mid(up, arrived_up, down, arrived_down):
    shape = jax.ShapeDtypeStruct(arrived_up.shape, I16)
    return pl.pallas_call(
        rest_mid_body,
        out_shape=[shape] * 2,
        in_specs=[whole()] * 4,
        out_specs=[whole()] * 2,
        compiler_params=params(16),
        cost_estimate=cost(up.size * 16, up.size * 16),
        name="rest_mid",
    )(up, arrived_up, down, arrived_down)


def gathered(own, arrived, first, tail, row, lanes):
    v = own[pl.ds(pl.multiple_of(first[0] + row, 64), first[2]), lanes]
    for m in arrived:
        cut = pl.ds(pl.multiple_of(first[1] + row, 16), first[2])
        v = v + plain(m[cut, lanes]) * scale_of(m[tail:tail + TAIL, lanes])
    return v


def rest_second_body(own, a, b, d, e, after, kept, *outs):
    at = position()
    high = kept.shape[0]
    total, step = own.shape[0] // RING, own.shape[1]
    h = jnp.where(at[1] == 1, at[3], at[2])
    for k in range(RING):
        row = lax.rem(h + k, RING) * high
        out = kept if k == 0 else outs[k - 1]
        for n in range(RING):
            start, tail = n % 2 * total, 2 * total + n % 2 * TAIL
            v = gathered(own, (a, b) if n < 2 else (d, e), (n * total, start, high), tail, row, slice(0, step))
            write(out.at[:, n * step:(n + 1) * step], 0, v)


def rest_second(own, upper, lower, after):
    total, columns = own.shape
    high, every = total // RING // RING, columns * RING
    return list(pl.pallas_call(
        rest_second_body,
        out_shape=[jax.ShapeDtypeStruct((high, every), F32)]
        + [jax.ShapeDtypeStruct((high + TAIL, every), I16)] * 3,
        in_specs=[whole()] * 6,
        out_specs=[whole()] * 4,
        compiler_params=params(24),
        cost_estimate=cost(total * columns * 12, total * columns * 8),
        name="rest_second_sum",
    )(own, *upper, *lower, after))


def bulk_second_body(steps, own, a, b, d, e, after, *outs):
    at = position()
    high = own.shape[0] // RING
    h = jnp.where(at[1] == 1, at[3], at[2])
    half = own.shape[0] // 2
    step = 256
    for k, out in zip(steps, outs):
        block = lax.rem(h + k, RING)

        def part(upper, arrived, block=block, out=out):
            @pl.when((block < RING // 2) == upper)
            def _():
                row = pl.multiple_of(lax.rem(block, RING // 2) * high, 64)
                first = pl.multiple_of(block * high, 64)
                for lane in range(0, own.shape[1], step):
                    lanes = slice(lane, lane + step)
                    v = own[pl.ds(first, high), lanes]
                    for m in arrived:
                        v = v + plain(m[pl.ds(row, high), lanes]) * scale_of(m[half:, lanes])
                    write(out.at[:, lanes], 0, v)

        part(True, (a, b))
        part(False, (d, e))


def bulk_second(steps, own, upper, lower, after):
    total, columns = own.shape
    high = total // RING
    return list(pl.pallas_call(
        functools.partial(bulk_second_body, steps),
        out_shape=[
            jax.ShapeDtypeStruct((high + TAIL, columns), I16) if k else jax.ShapeDtypeStruct((high, columns), F32)
            for k in steps
        ],
        in_specs=[whole()] * 6,
        out_specs=[whole()] * len(steps),
        compiler_params=params(24),
        cost_estimate=cost(high * columns * 12 * len(steps), high * columns * 8 * len(steps)),
        name="bulk_second_sum",
    )(own, *upper, *lower, after))


def third_body(by_z, own, a, b, d, after, *outs):
    at = position()
    high, step = outs[0].shape
    start = at[0] if by_z else jnp.where(at[1] == 1, at[2], at[3])
    for k in range(RING):
        cut = pl.ds(pl.multiple_of(lax.rem(start + k, RING) * step, 128), step)
        write(outs[k], 0, gathered(own, (a, b, d), (0, 0, high), high, 0, cut))


def third(parts, by_z, after):
    high, every = parts[0].shape
    wide = every // RING
    return list(pl.pallas_call(
        functools.partial(third_body, by_z),
        out_shape=[jax.ShapeDtypeStruct((high, wide), F32)] + [jax.ShapeDtypeStruct((high + TAIL, wide), I16)] * 3,
        in_specs=[whole()] * 5,
        out_specs=[whole()] * 4,
        compiler_params=params(16),
        cost_estimate=cost(high * every * 16, high * every * 10),
        name="third_sum",
    )(*parts, after))


def tick_body(v, out):
    out[...] = v[...]


def tick(v):
    return pl.pallas_call(
        tick_body,
        out_shape=jax.ShapeDtypeStruct(v.shape, v.dtype),
        in_specs=[whole()],
        out_specs=whole(),
        compiler_params=params(1),
        cost_estimate=cost(1000, 32),
        name="tick",
    )(v)


def finish_body(own, a, b, d, rest, ra, rb, rd, out):
    high, wide = own.shape
    for first, v, arrived in ((0, own[...], (a, b, d)), (wide, rest[...], (ra, rb, rd))):
        for m in arrived:
            v = v + plain(m[:high, :]) * scale_of(m[high:, :])
        out[:, first:first + v.shape[1]] = v


def finish(bulk, rest):
    high = bulk[0].shape[0]
    ao = bulk[0].shape[1] + rest[0].shape[1]
    return pl.pallas_call(
        finish_body,
        out_shape=jax.ShapeDtypeStruct((high, ao), F32),
        in_specs=[whole()] * 8,
        out_specs=whole(),
        compiler_params=params(8),
        cost_estimate=cost(high * ao * 8, high * ao * 14),
    )(*bulk, *rest)


def shards(half, metric, survive):
    parts = screen(survive, half)
    here = [parts[0]] + [None] * 3
    for k in (2, 1, 3):
        here[k] = send(parts[k], along_z(k))
    pair = jnp.concatenate([metric, send(metric, other_core)], axis=0)
    metrics = [pair] + [None] * 3
    for k in (1, 2, 3):
        metrics[k] = send(pair, along_z(k))
    mixed = join(metrics)
    there = [None] * 4
    for k in (0, 2, 1, 3):
        there[k] = send(here[k], other_core)
    bulk_rows, rest_rows, turned, *far = fit([v for both in zip(here, there) for v in both], mixed)

    def bulk_step(*blocks, arrived=()):
        return bulk_k(bulk_rows, turned, blocks, arrived)

    def rest_step(*how):
        return rest_k(rest_rows, turned, *how)

    def near(axis, up, down):
        up = send(up, axis(1))
        down = send(down, axis(3))
        return up, down

    def onward(parts, shift):
        for k in (1, 2, 3):
            parts[k] = send(parts[k], shift(k))

    far = near(first_axis, *far)
    upper, lower, rest_own = rest_step((2, 0), ((0, 1), (2, 2)), ("message", "message", "all"))
    rest_far = near(along_z, upper, lower)
    lower_up, upper_down = near(first_axis, *bulk_step((1, 1, False), (3, 0, False)))
    keep_up, up, down, keep_down = rest_step((1, 3), ((0, 1), (2, 3)), ("half", "message", "message", "half"))
    rest_near = near(along_z, up, down)
    upper_up, lower_down = near(first_axis, *bulk_step((1, 0, True), (3, 1, True), arrived=far))
    up, down = rest_mid(keep_up, rest_far[0], keep_down, rest_far[1])
    mid = near(along_z, up, down)
    own = bulk_step((0, None, False))[0]
    arrived = own, (upper_up, upper_down), (lower_up, lower_down), metric
    bulk = [None] * 4
    (bulk[2],) = bulk_second((2,), *arrived)
    bulk[0], bulk[1], bulk[3] = bulk_second((0, 1, 3), *arrived)
    onward(bulk, second_axis)
    then = tick(metric)
    rest = rest_second(rest_own, (mid[0], rest_near[1]), (rest_near[0], mid[1]), then)
    onward(rest, second_axis)
    then = tick(then)
    bulk = third(bulk, True, then)
    onward(bulk, along_z)
    then = tick(then)
    rest = third(rest, False, then)
    onward(rest, first_axis)
    return finish(bulk, rest)


def solution(mesh):
    finer = Mesh(mesh.devices.reshape(4, 2, 4, 4), AXES)
    placed = (P(("z", "c"), ("x", "y"), None), P(("z", "c"), None), P(("z", "c"), ("x", "y"), None))
    return jax.shard_map(shards, mesh=finer, in_specs=placed, out_specs=P(("x", "y"), ("z", "c")), check_vma=False)
```
